16 devices in a mesh: dp: 2 (over y, z), sp: 8 (over x, core).
Axes of the slice: x: 4, y: 2, z: 1, core: 2. Of those that a mesh axis runs over, the one named last changes fastest.
The devices are a block of a 4x4x8 slice.
Arguments:
- tok_in: bfloat16 [4096, 6144], P(('dp', 'sp')), parts along dimension 0
- tok_pos: int32 [4096], P(('dp', 'sp')), parts along dimension 0
- w_dq: bfloat16 [6144, 1536], replicated
- g_q: float32 [1536], replicated
- w_uq: bfloat16 [1536, 64, 192], replicated
- w_dkv: bfloat16 [6144, 576], replicated
- g_kv: float32 [512], replicated
- w_uk: bfloat16 [512, 64, 128], replicated
- w_uv: bfloat16 [512, 64, 128], replicated
- w_o: bfloat16 [64, 128, 6144], replicated
Outputs:
- output 1: bfloat16 [4096, 6144], P(('dp', 'sp')), parts along dimension 0
- output 2: bfloat16 [4096, 512], P(('dp', 'sp')), parts along dimension 0
- output 3: bfloat16 [4096, 64], P(('dp', 'sp')), parts along dimension 0
There are 2 independent parts. The reference program is written for one: setup_inputs(seed, part) draws one part's arguments, and reference() takes and returns one part's arrays. A program takes and returns all parts, laid end to end along the dimension named above; an argument that names none is the same for every part.
All inputs are finite; a program needn't handle non-finite values.
Results may differ from the reference program's by a relative error of at most 0.00605.
Values are sent between devices in bfloat16 or wider.
A program may use at most 768 MiB of HBM per device.

```python
import math
import jax
import jax.numpy as jnp
from jax import lax

SEQ_LEN = 2048
ROW_BLOCK = 256
MODEL_DIM = 6144
NUM_HEADS = 64
Q_RANK = 1536
KV_RANK = 512
NOPE_DIM = 128
ROPE_DIM = 64
V_DIM = 128

ROPE_THETA = 10000.0
YARN_FACTOR = 40.0
ORIG_CTX = 4096.0
BETA_FAST = 32.0
BETA_SLOW = 1.0
NORM_EPS = 1e-6


def rope_freqs(rot_dim):
    half_dim = rot_dim // 2
    log_base = 2.0 * math.log(ROPE_THETA)
    low_idx = max(math.floor(rot_dim * math.log(ORIG_CTX / (BETA_FAST * 2.0 * math.pi)) / log_base), 0)
    high_idx = min(math.ceil(rot_dim * math.log(ORIG_CTX / (BETA_SLOW * 2.0 * math.pi)) / log_base), half_dim - 1)
    spread = max(high_idx - low_idx, 0.001)
    freq_list = []
    for freq_idx in range(half_dim):
        base_freq = ROPE_THETA ** (-2.0 * freq_idx / rot_dim)
        ramp_val = min(max((freq_idx - low_idx) / spread, 0.0), 1.0)
        freq_list.append(base_freq / YARN_FACTOR * ramp_val + base_freq * (1.0 - ramp_val))
    return jnp.asarray(freq_list, dtype=jnp.float32)


def rotate_half(act_in, cos_t, sin_t):
    half_dim = act_in.shape[-1] // 2
    first = act_in[..., :half_dim]
    second = act_in[..., half_dim:]
    return jnp.concatenate([first * cos_t - second * sin_t, second * cos_t + first * sin_t], axis=-1)


def rms_norm(act_in, gain):
    mean_sq = jnp.mean(act_in * act_in, axis=-1, keepdims=True)
    return act_in * lax.rsqrt(mean_sq + NORM_EPS) * gain


def setup_inputs(seed: int = 0, part: int = 0) -> dict:
    root_key = jax.random.key(seed)
    part_key = jax.random.fold_in(root_key, part)
    key_x, key_pos = jax.random.split(part_key)
    weight_keys = jax.random.split(root_key, 8)

    def draw_weight(sub_key, arr_shape, fan_in):
        return (jax.random.normal(sub_key, arr_shape, jnp.float32) * fan_in ** -0.5).astype(jnp.bfloat16)

    tok_in = jax.random.normal(key_x, (SEQ_LEN, MODEL_DIM), jnp.float32).astype(jnp.bfloat16)
    pos_steps = jax.random.randint(key_pos, (SEQ_LEN,), 1, 5, dtype=jnp.int32)
    tok_pos = (jnp.cumsum(pos_steps) - pos_steps[0]).astype(jnp.int32)
    w_dq = draw_weight(weight_keys[0], (MODEL_DIM, Q_RANK), MODEL_DIM)
    g_q = jax.random.uniform(weight_keys[1], (Q_RANK,), jnp.float32, 0.5, 1.5)
    w_uq = draw_weight(weight_keys[2], (Q_RANK, NUM_HEADS, NOPE_DIM + ROPE_DIM), Q_RANK)
    w_dkv = draw_weight(weight_keys[3], (MODEL_DIM, KV_RANK + ROPE_DIM), MODEL_DIM)
    g_kv = jax.random.uniform(weight_keys[4], (KV_RANK,), jnp.float32, 0.5, 1.5)
    w_uk = draw_weight(weight_keys[5], (KV_RANK, NUM_HEADS, NOPE_DIM), KV_RANK)
    w_uv = draw_weight(weight_keys[6], (KV_RANK, NUM_HEADS, V_DIM), KV_RANK)
    w_o = draw_weight(weight_keys[7], (NUM_HEADS, V_DIM, MODEL_DIM), NUM_HEADS * V_DIM)
    return dict(tok_in=tok_in, tok_pos=tok_pos, w_dq=w_dq, g_q=g_q, w_uq=w_uq, w_dkv=w_dkv, g_kv=g_kv, w_uk=w_uk, w_uv=w_uv, w_o=w_o)


def reference(tok_in, tok_pos, w_dq, g_q, w_uq, w_dkv, g_kv, w_uk, w_uv, w_o):
    qk_dim = NOPE_DIM + ROPE_DIM
    attn_scale = (0.1 * math.log(YARN_FACTOR) + 1.0) ** 2 / math.sqrt(qk_dim)
    angles = tok_pos.astype(jnp.float32)[:, None] * rope_freqs(ROPE_DIM)[None, :]
    cos_t = jnp.cos(angles)
    sin_t = jnp.sin(angles)
    q_lat = rms_norm(jnp.dot(tok_in, w_dq, preferred_element_type=jnp.float32), g_q).astype(jnp.bfloat16)
    q_full = jnp.dot(q_lat, w_uq.reshape(Q_RANK, NUM_HEADS * qk_dim), preferred_element_type=jnp.float32).reshape(SEQ_LEN, NUM_HEADS, qk_dim)
    q_nope = q_full[:, :, :NOPE_DIM].astype(jnp.bfloat16)
    q_rot = rotate_half(q_full[:, :, NOPE_DIM:], cos_t[:, None, :], sin_t[:, None, :]).astype(jnp.bfloat16)
    kv_lat = jnp.dot(tok_in, w_dkv, preferred_element_type=jnp.float32)
    cache_kv = rms_norm(kv_lat[:, :KV_RANK], g_kv).astype(jnp.bfloat16)
    cache_pe = rotate_half(kv_lat[:, KV_RANK:], cos_t, sin_t).astype(jnp.bfloat16)
    k_nope = jnp.dot(cache_kv, w_uk.reshape(KV_RANK, NUM_HEADS * NOPE_DIM), preferred_element_type=jnp.float32).reshape(SEQ_LEN, NUM_HEADS, NOPE_DIM).astype(jnp.bfloat16)
    values = jnp.dot(cache_kv, w_uv.reshape(KV_RANK, NUM_HEADS * V_DIM), preferred_element_type=jnp.float32).reshape(SEQ_LEN, NUM_HEADS, V_DIM).astype(jnp.bfloat16)
    key_idx = jnp.arange(SEQ_LEN)
    num_blocks = SEQ_LEN // ROW_BLOCK

    def head_attention(head_in):
        qn_head, qr_head, kn_head, v_head = head_in

        def block_attention(blk_idx):
            start = blk_idx * ROW_BLOCK
            qn_blk = lax.dynamic_slice_in_dim(qn_head, start, ROW_BLOCK, axis=0)
            qr_blk = lax.dynamic_slice_in_dim(qr_head, start, ROW_BLOCK, axis=0)
            logits = jnp.dot(qn_blk, kn_head.T, preferred_element_type=jnp.float32) + jnp.dot(qr_blk, cache_pe.T, preferred_element_type=jnp.float32)
            logits = logits * attn_scale
            row_idx = start + jnp.arange(ROW_BLOCK)
            logits = jnp.where(key_idx[None, :] <= row_idx[:, None], logits, -jnp.inf)
            attn_prob = jax.nn.softmax(logits, axis=-1).astype(jnp.bfloat16)
            return jnp.dot(attn_prob, v_head, preferred_element_type=jnp.float32).astype(jnp.bfloat16)

        return lax.map(block_attention, jnp.arange(num_blocks)).reshape(SEQ_LEN, V_DIM)

    head_outs = lax.map(head_attention, (jnp.swapaxes(q_nope, 0, 1), jnp.swapaxes(q_rot, 0, 1), jnp.swapaxes(k_nope, 0, 1), jnp.swapaxes(values, 0, 1)))
    attn_cat = jnp.swapaxes(head_outs, 0, 1).reshape(SEQ_LEN, NUM_HEADS * V_DIM)
    attn_out = jnp.dot(attn_cat, w_o.reshape(NUM_HEADS * V_DIM, MODEL_DIM), preferred_element_type=jnp.float32).astype(jnp.bfloat16)
    return attn_out, cache_kv, cache_pe
```

```python
import functools
import math

import jax
import jax.numpy as jnp
from jax import lax
from jax.experimental import pallas as pl
from jax.experimental.pallas import tpu as pltpu
from jax.sharding import PartitionSpec as P

ROPE_THETA = 10000.0
YARN_FACTOR = 40.0
ORIG_CTX = 4096.0
BETA_FAST = 32.0
BETA_SLOW = 1.0
NORM_EPS = 1e-6

MESH = pl.DeviceIdType.MESH
F32 = jnp.float32
BF16 = jnp.bfloat16
NT = (((1,), (1,)), ((), ()))
TT = (((0,), (1,)), ((), ()))


def rope_freqs(rot_dim):
    half_dim = rot_dim // 2
    log_base = 2.0 * math.log(ROPE_THETA)
    low_idx = max(math.floor(rot_dim * math.log(ORIG_CTX / (BETA_FAST * 2.0 * math.pi)) / log_base), 0)
    high_idx = min(math.ceil(rot_dim * math.log(ORIG_CTX / (BETA_SLOW * 2.0 * math.pi)) / log_base), half_dim - 1)
    spread = max(high_idx - low_idx, 0.001)
    freq_list = []
    for freq_idx in range(half_dim):
        base_freq = ROPE_THETA ** (-2.0 * freq_idx / rot_dim)
        ramp_val = min(max((freq_idx - low_idx) / spread, 0.0), 1.0)
        freq_list.append(base_freq / YARN_FACTOR * ramp_val + base_freq * (1.0 - ramp_val))
    return jnp.asarray(freq_list, dtype=jnp.float32)


def front_kernel(ranks, x_hbm, wkv_hbm, wq_hbm, gq_ref, gkv_ref, tab_ref,
                 kv_all, pe_all, cq_all, tab_all, ckv_out, cpe_out,
                 x_v, wkv_v, wq_v, cq_f, kv_v, pe_v, cq_v,
                 w_sem, own_sem, kv_send, kv_recv, pe_send, pe_recv, cq_send, cq_recv, tab_send, tab_recv):
    me = lax.axis_index("sp")
    core = lax.rem(me, 2)
    sib = me + 1 - 2 * core
    chips = ranks // 2
    rows = x_v.shape[0]
    kv_rank = kv_v.shape[1]
    half = (wkv_v.shape[1] - kv_rank) // 2
    far = [lax.rem(me + 2 * d, ranks) for d in range(1, chips)]

    kchunks, nq = wkv_v.shape[0], wq_v.shape[0]
    kc = wkv_v.shape[2]
    nc = wq_v.shape[2]
    x_copy = pltpu.make_async_copy(x_hbm, x_v, w_sem.at[0])
    wkv_copies = [pltpu.make_async_copy(wkv_hbm.at[:, pl.ds(k * kc, kc)], wkv_v.at[k], w_sem.at[1 + k]) for k in range(kchunks)]
    wq_copies = [pltpu.make_async_copy(wq_hbm.at[:, pl.ds(k * nc, nc)], wq_v.at[k], w_sem.at[1 + kchunks + k]) for k in range(nq)]
    x_copy.start()
    for c in wkv_copies + wq_copies:
        c.start()

    barrier = pltpu.get_barrier_semaphore()
    for peer in [sib] + far:
        pl.semaphore_signal(barrier, inc=1, device_id={"sp": peer}, device_id_type=MESH)
    pl.semaphore_wait(barrier, chips)

    def block(ref, idx):
        return ref.at[pl.ds(idx * rows, rows)]

    def remote(src, ref, idx, send, recv, dev):
        return pltpu.make_async_remote_copy(src_ref=src, dst_ref=block(ref, idx), send_sem=send, recv_sem=recv,
                                            device_id={"sp": dev}, device_id_type=MESH)

    tab_copy = remote(tab_ref, tab_all, core, tab_send.at[0], tab_recv.at[0], sib)
    tab_copy.start()
    tab_own = pltpu.make_async_copy(tab_ref, block(tab_all, core), own_sem.at[0])
    tab_own.start()

    x_copy.wait()
    acc = None
    for k in range(kchunks):
        wkv_copies[k].wait()
        part = lax.dot_general(x_v[:, k * kc:(k + 1) * kc], wkv_v[k], NT, preferred_element_type=F32)
        acc = part if acc is None else acc + part
    a = acc[:, :kv_rank]
    inv = lax.rsqrt(jnp.mean(a * a, axis=-1, keepdims=True) + NORM_EPS)
    kv_v[...] = (a * inv * gkv_ref[...]).astype(BF16)
    z1 = acc[:, kv_rank:kv_rank + half]
    z2 = acc[:, kv_rank + half:]
    cos_t = tab_ref[:, :half]
    sin_t = tab_ref[:, half:2 * half]
    pe = jnp.concatenate([z1 * cos_t - z2 * sin_t, z2 * cos_t + z1 * sin_t], axis=-1).astype(BF16)
    pe_v[...] = jnp.zeros_like(pe_v)
    pe_v[:, :2 * half] = pe
    ckv_out[...] = kv_v[...]
    cpe_out[...] = pe

    sends = []
    for n, dev in enumerate([sib] + far):
        slot = 0 if n == 0 else n
        c1 = remote(kv_v, kv_all, me, kv_send.at[n], kv_recv.at[slot], dev)
        c2 = remote(pe_v, pe_all, me, pe_send.at[n], pe_recv.at[slot], dev)
        c1.start()
        c2.start()
        sends += [c1, c2]
    own = [pltpu.make_async_copy(kv_v, block(kv_all, me), own_sem.at[1]),
           pltpu.make_async_copy(pe_v, block(pe_all, me), own_sem.at[2])]
    for c in own:
        c.start()

    ssq = jnp.zeros((rows, 1), F32)
    for k in range(nq):
        wq_copies[k].wait()
        q = jnp.dot(x_v[...], wq_v[k], preferred_element_type=F32)
        cq_f[:, k * nc:(k + 1) * nc] = q
        ssq = ssq + jnp.sum(q * q, axis=-1, keepdims=True)
    inv_q = lax.rsqrt(ssq / cq_f.shape[1] + NORM_EPS)
    cq_v[...] = (cq_f[...] * inv_q * gq_ref[...]).astype(BF16)
    cq_copy = remote(cq_v, cq_all, core, cq_send.at[0], cq_recv.at[0], sib)
    cq_copy.start()
    cq_own = pltpu.make_async_copy(cq_v, block(cq_all, core), own_sem.at[3])
    cq_own.start()

    fwd = []
    for n in range(1, chips):
        src = lax.rem(me + ranks - 2 * n, ranks)
        g1 = remote(block(kv_all, src), kv_all, src, kv_send.at[chips + n - 1], kv_recv.at[chips + n - 1], sib)
        g2 = remote(block(pe_all, src), pe_all, src, pe_send.at[chips + n - 1], pe_recv.at[chips + n - 1], sib)
        sends[2 * n].wait_recv()
        g1.start()
        sends[2 * n + 1].wait_recv()
        g2.start()
        fwd += [g1, g2]
    sends[0].wait_recv()
    sends[1].wait_recv()
    for c in sends:
        c.wait_send()
    for c in fwd:
        c.wait()
    tab_copy.wait()
    cq_copy.wait()
    tab_own.wait()
    cq_own.wait()
    for c in own:
        c.wait()


def attn_kernel(scale2, heads, idx_ref, cq_ref, kv_ref, pe_ref, cosq_ref, sinq_ref,
                wqa_ref, wqb_ref, wka_ref, wkb_ref, wva_ref, wvb_ref, oa_ref, ob_ref,
                k_a, k_b, v_a, v_b, v_p, q_a, q_b, s_a, s_b, m_a, m_b, l_ref, o_ref):
    step = pl.program_id(0)
    full = idx_ref[0]
    blk = k_a.shape[1]
    nope = wka_ref.shape[1]
    half = cosq_ref.shape[0]
    rot = 2 * half
    sub = blk // 2

    @pl.when(step == 0)
    def _():
        for kb in range(k_a.shape[0]):
            pe = pe_ref[kb * blk:(kb + 1) * blk, :]
            k_a[kb, :, nope:] = pe
            k_b[kb, :, nope:] = pe
        q_a[nope + rot:, :] = jnp.zeros((q_a.shape[0] - nope - rot, q_a.shape[1]), BF16)
        q_b[nope + rot:, :] = jnp.zeros((q_b.shape[0] - nope - rot, q_b.shape[1]), BF16)
        v_p[...] = jnp.zeros_like(v_p)
        s_b[...] = jnp.zeros_like(s_b)
        m_b[...] = jnp.zeros_like(m_b)

    def q_proj(w_ref, q_ref):
        u = lax.dot_general(w_ref[0], cq_ref[...], NT, preferred_element_type=F32)
        q_ref[:nope, :] = u[:nope].astype(BF16)
        z1 = u[nope:nope + half]
        z2 = u[nope + half:]
        q_ref[nope:nope + half, :] = (z1 * cosq_ref[...] - z2 * sinq_ref[...]).astype(BF16)
        q_ref[nope + half:nope + rot, :] = (z2 * cosq_ref[...] + z1 * sinq_ref[...]).astype(BF16)

    def kv_proj(kb, wk, wv):
        c = kv_ref[pl.ds(pl.multiple_of(kb * blk, blk), blk), :]
        k = jnp.dot(c, wk, preferred_element_type=F32).astype(BF16)
        k_a[kb, :, :nope] = k[:, :nope]
        k_b[kb, :, :nope] = k[:, nope:]
        v = lax.dot_general(wv, c, NT, preferred_element_type=F32).astype(BF16)
        v_a[kb] = v[:nope]
        v_b[kb] = v[nope:]

    def fold_max(m_ref, s, cols):
        t = jnp.max(s.reshape(s.shape[0] // 8, 8, s.shape[1]), axis=0)
        m_ref[:, cols] = jnp.maximum(m_ref[:, cols], t)

    everything = slice(None)

    def qk(kb, k_ref, q_ref, s_ref, m_ref):
        s = jnp.dot(k_ref[kb], q_ref[...], preferred_element_type=F32)
        s_ref[kb] = s
        fold_max(m_ref, s, everything)

    def qk_diag(kb, k_ref, q_ref, s_ref, m_ref):
        s0 = jnp.dot(k_ref[kb, :sub, :], q_ref[...], preferred_element_type=F32)
        s1 = jnp.dot(k_ref[kb, sub:, :], q_ref[:, sub:], preferred_element_type=F32)
        keep = lax.broadcasted_iota(jnp.int32, (sub, sub), 0) <= lax.broadcasted_iota(jnp.int32, (sub, sub), 1)
        s00 = jnp.where(keep, s0[:, :sub], -jnp.inf)
        s1 = jnp.where(keep, s1, -jnp.inf)
        s01 = s0[:, sub:]
        s_ref[kb, :sub, :sub] = s00
        s_ref[kb, :sub, sub:] = s01
        s_ref[kb, sub:, sub:] = s1
        fold_max(m_ref, s00, slice(0, sub))
        fold_max(m_ref, s01, slice(sub, blk))
        fold_max(m_ref, s1, slice(sub, blk))

    def fold_sum(p, cols):
        l_ref[:, cols] += jnp.sum(p.reshape(p.shape[0] // 8, 8, p.shape[1]), axis=0)

    def top(m_ref):
        return jnp.max(m_ref[...], axis=0, keepdims=True)

    def pv(kb, v_ref, s_ref, m):
        p = jnp.exp2((s_ref[kb] - m) * scale2)
        fold_sum(p, everything)
        o_ref[...] += jnp.dot(v_ref[kb], p.astype(BF16), preferred_element_type=F32)

    def pv_diag(kb, v_ref, s_ref, m):
        p0 = jnp.exp2((s_ref[kb, :sub, :] - m) * scale2)
        p1 = jnp.exp2((s_ref[kb, sub:, sub:] - m[:, sub:]) * scale2)
        fold_sum(p0, everything)
        fold_sum(p1, slice(sub, blk))
        p0 = p0.astype(BF16)
        o_ref[...] += jnp.dot(v_ref[kb, :, :sub], p0, preferred_element_type=F32)
        o_ref[:, sub:] += jnp.dot(v_ref[kb, :, sub:], p1.astype(BF16), preferred_element_type=F32)

    def finish(out_ref):
        l = jnp.sum(l_ref[...], axis=0, keepdims=True)
        out_ref[...] = (o_ref[...] / l).T.astype(BF16)

    def clear():
        l_ref[...] = jnp.zeros_like(l_ref)
        o_ref[...] = jnp.zeros_like(o_ref)

    @pl.when(step < heads)
    def _():
        q_proj(wqa_ref, q_a)
        q_proj(wqb_ref, q_b)
        wk = jnp.concatenate([wka_ref[...], wkb_ref[...]], axis=1)
        wv = jnp.concatenate([wva_ref[...].T, wvb_ref[...].T], axis=0)
        m = top(m_b)
        clear()
        m_a[...] = jnp.full_like(m_a, -jnp.inf)

        def body1(kb, _):
            kv_proj(kb, wk, wv)
            qk(kb, k_a, q_a, s_a, m_a)
            pv(kb, v_p, s_b, m)
            return _

        lax.fori_loop(0, full, body1, 0)
        kv_proj(full, wk, wv)
        qk_diag(full, k_a, q_a, s_a, m_a)
        pv_diag(full, v_p, s_b, m)
        finish(ob_ref)
        m2 = top(m_a)
        clear()
        m_b[...] = jnp.full_like(m_b, -jnp.inf)

        def body2(kb, _):
            qk(kb, k_b, q_b, s_b, m_b)
            pv(kb, v_a, s_a, m2)
            v_p[kb] = v_b[kb]
            return _

        lax.fori_loop(0, full, body2, 0)
        qk_diag(full, k_b, q_b, s_b, m_b)
        pv_diag(full, v_a, s_a, m2)
        v_p[full] = v_b[full]
        finish(oa_ref)

    @pl.when(step == heads)
    def _():
        m = top(m_b)
        clear()

        def body(kb, _):
            pv(kb, v_p, s_b, m)
            return _

        lax.fori_loop(0, full, body, 0)
        pv_diag(full, v_p, s_b, m)
        finish(ob_ref)


def solution(mesh):
    ranks = mesh.shape["sp"]
    tok_spec = P(("dp", "sp"))
    rows_spec = P(("dp", "sp"), None)
    replicated = P()

    def local_step(tok_in, tok_pos, w_dq, g_q, w_uq, w_dkv, g_kv, w_uk, w_uv, w_o):
        rows, model = tok_in.shape
        num_heads = w_uq.shape[1]
        qk_dim = w_uq.shape[2]
        q_rank = w_dq.shape[1]
        kv_rank = g_kv.shape[0]
        rot = w_dkv.shape[1] - kv_rank
        nope = qk_dim - rot
        v_dim = w_uv.shape[2]
        seq = rows * ranks
        half = rot // 2
        chips = ranks // 2
        mine = num_heads // 2
        pairs = mine // 2
        pe_w = 128
        attn_scale = (0.1 * math.log(YARN_FACTOR) + 1.0) ** 2 / math.sqrt(qk_dim)
        me = lax.axis_index("sp")
        core = lax.rem(me, 2)

        angles = tok_pos.astype(F32)[:, None] * rope_freqs(rot)[None, :]
        tab = jnp.concatenate([jnp.cos(angles), jnp.sin(angles), jnp.zeros((rows, 128 - rot), F32)], axis=1)

        kchunks, nq = 2, 3
        any_spec = pl.BlockSpec(memory_space=pl.ANY)
        vmem_spec = pl.BlockSpec(memory_space=pltpu.VMEM)
        dma = pltpu.SemaphoreType.DMA
        kv_all, pe_all, cq_all, tab_all, cache_kv, cache_pe = pl.pallas_call(
            functools.partial(front_kernel, ranks),
            out_shape=(
                jax.ShapeDtypeStruct((seq, kv_rank), BF16),
                jax.ShapeDtypeStruct((seq, pe_w), BF16),
                jax.ShapeDtypeStruct((2 * rows, q_rank), BF16),
                jax.ShapeDtypeStruct((2 * rows, 128), F32),
                jax.ShapeDtypeStruct((rows, kv_rank), BF16),
                jax.ShapeDtypeStruct((rows, rot), BF16),
            ),
            in_specs=[any_spec, any_spec, any_spec, vmem_spec, vmem_spec, vmem_spec],
            out_specs=(any_spec, any_spec, any_spec, any_spec, vmem_spec, vmem_spec),
            scratch_shapes=[
                pltpu.VMEM((rows, model), BF16),
                pltpu.VMEM((kchunks, kv_rank + rot, model // kchunks), BF16),
                pltpu.VMEM((nq, model, q_rank // nq), BF16),
                pltpu.VMEM((rows, q_rank), F32),
                pltpu.VMEM((rows, kv_rank), BF16),
                pltpu.VMEM((rows, pe_w), BF16),
                pltpu.VMEM((rows, q_rank), BF16),
                dma((1 + kchunks + nq,)),
                dma((4,)),
                dma((2 * chips - 1,)),
                dma((2 * chips - 1,)),
                dma((2 * chips - 1,)),
                dma((2 * chips - 1,)),
                dma((1,)),
                dma((1,)),
                dma((1,)),
                dma((1,)),
            ],
            compiler_params=pltpu.CompilerParams(collective_id=0, has_side_effects=True, vmem_limit_bytes=60 << 20),
            cost_estimate=pl.CostEstimate(flops=2 * rows * model * (q_rank + kv_rank + rot), bytes_accessed=2 * model * (q_rank + kv_rank + rot), transcendentals=0),
        )(tok_in, w_dkv.T, w_dq, g_q[None, :], g_kv[None, :], tab)

        wuk_h = lax.dynamic_slice_in_dim(w_uk, core * mine, mine, axis=1).reshape(kv_rank, mine * nope)
        wuv_h = lax.dynamic_slice_in_dim(w_uv, core * mine, mine, axis=1).reshape(kv_rank, mine * v_dim)
        wuq_t = jnp.transpose(w_uq, (1, 2, 0))
        tab_t = tab_all.T
        cos_q, sin_q = tab_t[:half], tab_t[half:2 * half]
        qn = 2 * rows
        nblk = seq // qn
        idx = jnp.stack([me // 2, core * mine]).astype(jnp.int32)

        def whole(shape):
            return pl.BlockSpec(shape, lambda i, s: (0,) * len(shape))

        last = pairs - 1
        o_a, o_b = pl.pallas_call(
            functools.partial(attn_kernel, attn_scale * math.log2(math.e), pairs),
            out_shape=(jax.ShapeDtypeStruct((qn, pairs * v_dim), BF16),) * 2,
            grid_spec=pltpu.PrefetchScalarGridSpec(
                num_scalar_prefetch=1,
                grid=(pairs + 1,),
                in_specs=[
                    whole((qn, q_rank)),
                    whole((seq, kv_rank)),
                    whole((seq, pe_w)),
                    whole((half, qn)),
                    whole((half, qn)),
                    pl.BlockSpec((1, qk_dim, q_rank), lambda i, s: (s[1] + jnp.minimum(i, last), 0, 0)),
                    pl.BlockSpec((1, qk_dim, q_rank), lambda i, s: (s[1] + pairs + jnp.minimum(i, last), 0, 0)),
                    pl.BlockSpec((kv_rank, nope), lambda i, s: (0, jnp.minimum(i, last))),
                    pl.BlockSpec((kv_rank, nope), lambda i, s: (0, pairs + jnp.minimum(i, last))),
                    pl.BlockSpec((kv_rank, v_dim), lambda i, s: (0, jnp.minimum(i, last))),
                    pl.BlockSpec((kv_rank, v_dim), lambda i, s: (0, pairs + jnp.minimum(i, last))),
                ],
                out_specs=(
                    pl.BlockSpec((qn, v_dim), lambda i, s: (0, jnp.minimum(i, last))),
                    pl.BlockSpec((qn, v_dim), lambda i, s: (0, jnp.maximum(i - 1, 0))),
                ),
                scratch_shapes=[
                    pltpu.VMEM((nblk, qn, nope + pe_w), BF16),
                    pltpu.VMEM((nblk, qn, nope + pe_w), BF16),
                    pltpu.VMEM((nblk, v_dim, qn), BF16),
                    pltpu.VMEM((nblk, v_dim, qn), BF16),
                    pltpu.VMEM((nblk, v_dim, qn), BF16),
                    pltpu.VMEM((nope + pe_w, qn), BF16),
                    pltpu.VMEM((nope + pe_w, qn), BF16),
                    pltpu.VMEM((nblk, qn, qn), F32),
                    pltpu.VMEM((nblk, qn, qn), F32),
                    pltpu.VMEM((8, qn), F32),
                    pltpu.VMEM((8, qn), F32),
                    pltpu.VMEM((8, qn), F32),
                    pltpu.VMEM((v_dim, qn), F32),
                ],
            ),
            compiler_params=pltpu.CompilerParams(dimension_semantics=("arbitrary",), vmem_limit_bytes=60 << 20),
        )(idx, cq_all, kv_all, pe_all, cos_q, sin_q, wuq_t, wuq_t, wuk_h, wuk_h, wuv_h, wuv_h)

        o_mine = jnp.concatenate([o_a, o_b], axis=1)
        keep = lax.dynamic_slice_in_dim(o_mine, core * rows, rows, axis=0)
        give = lax.dynamic_slice_in_dim(o_mine, (1 - core) * rows, rows, axis=0)
        swap = [(d, d + 1 - 2 * (d % 2)) for d in range(ranks)]
        got = lax.ppermute(give, "sp", swap)
        first = core == 0
        o_full = jnp.concatenate([jnp.where(first, keep, got), jnp.where(first, got, keep)], axis=1)
        attn_out = jnp.dot(o_full, w_o.reshape(num_heads * v_dim, model), preferred_element_type=F32).astype(BF16)
        return attn_out, cache_kv, cache_pe

    return jax.shard_map(local_step, mesh=mesh,
                         in_specs=(rows_spec, tok_spec) + (replicated,) * 8,
                         out_specs=(rows_spec, rows_spec, rows_spec), check_vma=False)
```

```python
import functools
import math

import jax
import jax.numpy as jnp
from jax import lax
from jax.experimental import pallas as pl
from jax.experimental.pallas import tpu as pltpu
from jax.sharding import PartitionSpec as P

ROPE_THETA = 10000.0
YARN_FACTOR = 40.0
ORIG_CTX = 4096.0
BETA_FAST = 32.0
BETA_SLOW = 1.0
NORM_EPS = 1e-6

MESH = pl.DeviceIdType.MESH
F32 = jnp.float32
BF16 = jnp.bfloat16
NT = (((1,), (1,)), ((), ()))
TT = (((0,), (1,)), ((), ()))


def rope_freqs(rot_dim):
    half_dim = rot_dim // 2
    log_base = 2.0 * math.log(ROPE_THETA)
    low_idx = max(math.floor(rot_dim * math.log(ORIG_CTX / (BETA_FAST * 2.0 * math.pi)) / log_base), 0)
    high_idx = min(math.ceil(rot_dim * math.log(ORIG_CTX / (BETA_SLOW * 2.0 * math.pi)) / log_base), half_dim - 1)
    spread = max(high_idx - low_idx, 0.001)
    freq_list = []
    for freq_idx in range(half_dim):
        base_freq = ROPE_THETA ** (-2.0 * freq_idx / rot_dim)
        ramp_val = min(max((freq_idx - low_idx) / spread, 0.0), 1.0)
        freq_list.append(base_freq / YARN_FACTOR * ramp_val + base_freq * (1.0 - ramp_val))
    return jnp.asarray(freq_list, dtype=jnp.float32)


def front_kernel(ranks, heads, x_hbm, wkv_hbm, wq_hbm, wuk_hbm, wuv_hbm, gq_ref, gkv_ref, cos_ref, sin_ref,
                 kv_all, cq_all, tab_all, wk_out, wv_out, ckv_out, cpe_out,
                 x_v, wkv_v, wq_v, wu_v, wo_v, wide_v, cq_f, kv_v, cq_v, tab_v,
                 w_sem, own_sem, kv_send, kv_recv, pair_send, pair_recv):
    me = lax.axis_index("sp")
    core = lax.rem(me, 2)
    sib = me + 1 - 2 * core
    rows = x_v.shape[0]
    half = cos_ref.shape[0]
    kv_rank = gkv_ref.shape[1]
    right = lax.rem(me + 2, ranks)
    left = lax.rem(me + ranks - 2, ranks)
    across = lax.rem(me + 4, ranks)

    kchunks, nq = wkv_v.shape[0], wq_v.shape[0]
    kc = wkv_v.shape[2]
    nc = wq_v.shape[2]
    first = core * heads
    loads = [pltpu.make_async_copy(x_hbm, x_v, w_sem.at[0])]
    loads += [pltpu.make_async_copy(wkv_hbm.at[:, pl.ds(k * kc, kc)], wkv_v.at[k], w_sem.at[1 + k]) for k in range(kchunks)]
    loads += [pltpu.make_async_copy(wq_hbm.at[:, pl.ds(k * nc, nc)], wq_v.at[k], w_sem.at[1 + kchunks + k]) for k in range(nq)]
    loads += [pltpu.make_async_copy(h.at[:, pl.ds(first, heads), :], wu_v.at[k], w_sem.at[1 + kchunks + nq + k])
              for k, h in enumerate((wuk_hbm, wuv_hbm))]
    for c in loads:
        c.start()

    barrier = pltpu.get_barrier_semaphore()
    for peer in (sib, right, left):
        pl.semaphore_signal(barrier, inc=1, device_id={"sp": peer}, device_id_type=MESH)
    pl.semaphore_wait(barrier, 3)

    def block(idx, start=0, size=None):
        return kv_all.at[pl.ds(idx * rows + start, size or rows)]

    def remote(src, dst, send, recv, dev):
        return pltpu.make_async_remote_copy(src_ref=src, dst_ref=dst, send_sem=send, recv_sem=recv,
                                            device_id={"sp": dev}, device_id_type=MESH)

    loads[0].wait()
    acc = None
    for k in range(kchunks):
        loads[1 + k].wait()
        part = lax.dot_general(x_v[:, k * kc:(k + 1) * kc], wkv_v[k], NT, preferred_element_type=F32)
        acc = part if acc is None else acc + part
    a = acc[:, :kv_rank]
    inv = lax.rsqrt(jnp.mean(a * a, axis=-1, keepdims=True) + NORM_EPS)
    ckv = (a * inv * gkv_ref[...]).astype(BF16)
    tab_v[:half, :] = cos_ref[...]
    tab_v[half:, :] = sin_ref[...]
    tab = tab_v[...].T
    cos_t, sin_t = tab[:, :half], tab[:, half:]
    z1 = acc[:, kv_rank:kv_rank + half]
    z2 = acc[:, kv_rank + half:]
    pe = jnp.concatenate([z1 * cos_t - z2 * sin_t, z2 * cos_t + z1 * sin_t], axis=-1).astype(BF16)
    kv_v[:, :kv_rank] = ckv
    kv_v[:, kv_rank:] = jnp.concatenate([pe, jnp.zeros((rows, kv_v.shape[1] - kv_rank - 2 * half), BF16)], axis=-1)
    ckv_out[...] = ckv
    cpe_out[...] = pe

    to_sib = remote(kv_v, block(me), kv_send.at[0], kv_recv.at[0], sib)
    to_right = remote(kv_v, block(me), kv_send.at[1], kv_recv.at[1], right)
    to_left = remote(kv_v, block(me), kv_send.at[2], kv_recv.at[2], left)
    tab_copy = remote(tab_v, tab_all.at[core], pair_send.at[0], pair_recv.at[0], sib)
    for c in (to_right, to_left, to_sib, tab_copy):
        c.start()
    own = [pltpu.make_async_copy(kv_v, block(me), own_sem.at[0]),
           pltpu.make_async_copy(tab_v, tab_all.at[core], own_sem.at[1])]
    for c in own:
        c.start()

    ssq = jnp.zeros((rows, 1), F32)
    for k in range(nq):
        loads[1 + kchunks + k].wait()
        q = jnp.dot(x_v[...], wq_v[k], preferred_element_type=F32)
        cq_f[:, k * nc:(k + 1) * nc] = q
        ssq = ssq + jnp.sum(q * q, axis=-1, keepdims=True)
    inv_q = lax.rsqrt(ssq / cq_f.shape[1] + NORM_EPS)
    cq_v[...] = (cq_f[...] * inv_q * gq_ref[...]).astype(BF16)
    cq_copy = remote(cq_v, cq_all.at[pl.ds(core * rows, rows)], pair_send.at[1], pair_recv.at[1], sib)
    cq_copy.start()
    own.append(pltpu.make_async_copy(cq_v, cq_all.at[pl.ds(core * rows, rows)], own_sem.at[2]))
    own[-1].start()

    mid = rows // 2
    to_right.wait_recv()
    half_right = remote(block(left, 0, mid), block(left, 0, mid), kv_send.at[3], kv_recv.at[3], right)
    half_right.start()
    sib_left = remote(block(left), block(left), kv_send.at[5], kv_recv.at[5], sib)
    sib_left.start()
    to_left.wait_recv()
    half_left = remote(block(right, mid, mid), block(right, mid, mid), kv_send.at[4], kv_recv.at[4], left)
    half_left.start()
    sib_right = remote(block(right), block(right), kv_send.at[6], kv_recv.at[6], sib)
    sib_right.start()

    depth = wide_v.shape[1] // 8
    groups = wide_v.shape[0]
    width = wide_v.shape[2]
    for t, out in enumerate((wk_out, wv_out)):
        loads[1 + kchunks + nq + t].wait()

        def relayout(i, _, t=t):
            base = pl.multiple_of(i * depth, depth)
            for g in range(groups):
                wide_v[g] = wu_v[t, pl.ds(base, depth), g * 8:(g + 1) * 8, :].astype(F32).reshape(depth * 8, width)
            for g in range(groups):
                for h in range(8):
                    col = (g * 8 + h) * width
                    wo_v[t, pl.ds(base, depth), col:col + width] = wide_v[g, pl.ds(h, depth, stride=8), :].astype(BF16)
            return _

        lax.fori_loop(0, wu_v.shape[1] // depth, relayout, 0)
        own.append(pltpu.make_async_copy(wo_v.at[t], out, own_sem.at[3 + t]))
        own[-1].start()

    half_right.wait_recv()
    half_left.wait_recv()
    sib_across = remote(block(across), block(across), kv_send.at[7], kv_recv.at[7], sib)
    sib_across.start()
    to_sib.wait()
    to_right.wait_send()
    to_left.wait_send()
    half_right.wait_send()
    half_left.wait_send()
    for c in (sib_left, sib_right, sib_across, tab_copy, cq_copy):
        c.wait()
    for c in own:
        c.wait()


def attn_kernel(scale2, heads, idx_ref, cq_ref, kv_ref, tab_ref,
                wqa_ref, wqb_ref, wka_ref, wkb_ref, wva_ref, wvb_ref, oa_ref, ob_ref,
                k_a, k_b, v_a, v_b, v_p, q_a, q_b, s_a, s_b, m_a, m_b, l_a, l_b, o_a, o_b, cosq_ref, sinq_ref):
    step = pl.program_id(0)
    full = idx_ref[0]
    blk = k_a.shape[1]
    nope = wka_ref.shape[1]
    kv_rank = wka_ref.shape[0]
    half = cosq_ref.shape[0]
    rot = 2 * half
    sub = blk // 2

    @pl.when(step == 0)
    def _():
        for kb in range(k_a.shape[0]):
            pe = kv_ref[kb * blk:(kb + 1) * blk, kv_rank:]
            k_a[kb, :, nope:] = pe
            k_b[kb, :, nope:] = pe
        q_a[nope + rot:, :] = jnp.zeros((q_a.shape[0] - nope - rot, q_a.shape[1]), BF16)
        q_b[nope + rot:, :] = jnp.zeros((q_b.shape[0] - nope - rot, q_b.shape[1]), BF16)
        for c in range(2):
            cosq_ref[:, c * sub:(c + 1) * sub] = tab_ref[c, :half, :]
            sinq_ref[:, c * sub:(c + 1) * sub] = tab_ref[c, half:, :]
        v_p[...] = jnp.zeros_like(v_p)
        o_a[...] = jnp.zeros_like(o_a)
        l_a[...] = jnp.ones_like(l_a)
        s_b[...] = jnp.zeros_like(s_b)
        m_b[...] = jnp.zeros_like(m_b)

    def q_proj(w_ref, q_ref):
        u = lax.dot_general(w_ref[0], cq_ref[...], NT, preferred_element_type=F32)
        q_ref[:nope, :] = u[:nope].astype(BF16)
        z1 = u[nope:nope + half]
        z2 = u[nope + half:]
        q_ref[nope:nope + half, :] = (z1 * cosq_ref[...] - z2 * sinq_ref[...]).astype(BF16)
        q_ref[nope + half:nope + rot, :] = (z2 * cosq_ref[...] + z1 * sinq_ref[...]).astype(BF16)

    def kv_proj(kb, wk, wv):
        c = kv_ref[pl.ds(pl.multiple_of(kb * blk, blk), blk), :kv_rank]
        k = jnp.dot(c, wk, preferred_element_type=F32).astype(BF16)
        k_a[kb, :, :nope] = k[:, :nope]
        k_b[kb, :, :nope] = k[:, nope:]
        v = lax.dot_general(wv, c, NT, preferred_element_type=F32).astype(BF16)
        v_a[kb] = v[:nope]
        v_b[kb] = v[nope:]

    def fold_max(m_ref, s, cols):
        t = jnp.max(s.reshape(s.shape[0] // 8, 8, s.shape[1]), axis=0)
        m_ref[:, cols] = jnp.maximum(m_ref[:, cols], t)

    everything = slice(None)

    def qk(kb, k_ref, q_ref, s_ref, m_ref):
        s = jnp.dot(k_ref[kb], q_ref[...], preferred_element_type=F32)
        s_ref[kb] = s
        fold_max(m_ref, s, everything)

    def qk_diag(kb, k_ref, q_ref, s_ref, m_ref):
        s0 = jnp.dot(k_ref[kb, :sub, :], q_ref[...], preferred_element_type=F32)
        s1 = jnp.dot(k_ref[kb, sub:, :], q_ref[:, sub:], preferred_element_type=F32)
        keep = lax.broadcasted_iota(jnp.int32, (sub, sub), 0) <= lax.broadcasted_iota(jnp.int32, (sub, sub), 1)
        s00 = jnp.where(keep, s0[:, :sub], -jnp.inf)
        s1 = jnp.where(keep, s1, -jnp.inf)
        s01 = s0[:, sub:]
        s_ref[kb, :sub, :sub] = s00
        s_ref[kb, :sub, sub:] = s01
        s_ref[kb, sub:, sub:] = s1
        fold_max(m_ref, s00, slice(0, sub))
        fold_max(m_ref, s01, slice(sub, blk))
        fold_max(m_ref, s1, slice(sub, blk))

    def fold_sum(l_ref, p, cols):
        l_ref[:, cols] += jnp.sum(p.reshape(p.shape[0] // 8, 8, p.shape[1]), axis=0)

    def top(m_ref):
        return jnp.max(m_ref[...], axis=0, keepdims=True)

    def pv(kb, v_ref, s_ref, m, l_ref, o_ref):
        p = jnp.exp2((s_ref[kb] - m) * scale2)
        fold_sum(l_ref, p, everything)
        o_ref[...] += jnp.dot(v_ref[kb], p.astype(BF16), preferred_element_type=F32)

    def pv_diag(kb, v_ref, s_ref, m, l_ref, o_ref):
        p0 = jnp.exp2((s_ref[kb, :sub, :] - m) * scale2)
        p1 = jnp.exp2((s_ref[kb, sub:, sub:] - m[:, sub:]) * scale2)
        fold_sum(l_ref, p0, everything)
        fold_sum(l_ref, p1, slice(sub, blk))
        p0 = p0.astype(BF16)
        o_ref[...] += jnp.dot(v_ref[kb, :, :sub], p0, preferred_element_type=F32)
        o_ref[:, sub:] += jnp.dot(v_ref[kb, :, sub:], p1.astype(BF16), preferred_element_type=F32)

    def finish(l_ref, o_ref, out_ref):
        l = jnp.sum(l_ref[...], axis=0, keepdims=True)
        out_ref[...] = (o_ref[...] / l).T.astype(BF16)

    def clear(l_ref, o_ref):
        l_ref[...] = jnp.zeros_like(l_ref)
        o_ref[...] = jnp.zeros_like(o_ref)

    @pl.when(step < heads)
    def _():
        m = top(m_b)
        clear(l_b, o_b)
        m_a[...] = jnp.full_like(m_a, -jnp.inf)
        finish(l_a, o_a, oa_ref)
        q_proj(wqa_ref, q_a)
        q_proj(wqb_ref, q_b)
        wk = jnp.concatenate([wka_ref[...], wkb_ref[...]], axis=1)
        wv = jnp.concatenate([wva_ref[...].T, wvb_ref[...].T], axis=0)

        def body1(kb, _):
            kv_proj(kb, wk, wv)
            qk(kb, k_a, q_a, s_a, m_a)
            pv(kb, v_p, s_b, m, l_b, o_b)
            return _

        lax.fori_loop(0, full, body1, 0)
        clear(l_a, o_a)
        kv_proj(full, wk, wv)
        qk_diag(full, k_a, q_a, s_a, m_a)
        pv_diag(full, v_p, s_b, m, l_b, o_b)
        m2 = top(m_a)
        m_b[...] = jnp.full_like(m_b, -jnp.inf)

        def body2(kb, _):
            qk(kb, k_b, q_b, s_b, m_b)
            pv(kb, v_a, s_a, m2, l_a, o_a)
            v_p[kb] = v_b[kb]
            return _

        lax.fori_loop(0, full, body2, 0)
        finish(l_b, o_b, ob_ref)
        qk_diag(full, k_b, q_b, s_b, m_b)
        pv_diag(full, v_a, s_a, m2, l_a, o_a)
        v_p[full] = v_b[full]

    @pl.when(step == heads)
    def _():
        m = top(m_b)
        clear(l_b, o_b)
        finish(l_a, o_a, oa_ref)

        def body(kb, _):
            pv(kb, v_p, s_b, m, l_b, o_b)
            return _

        lax.fori_loop(0, full, body, 0)
        pv_diag(full, v_p, s_b, m, l_b, o_b)
        finish(l_b, o_b, ob_ref)


def out_kernel(oa_hbm, ob_hbm, wo_hbm, out_hbm, own_v, sib_v, w_v, out_v,
               o_sem, w_sem, out_sem, send_sem, recv_sem):
    me = lax.axis_index("sp")
    core = lax.rem(me, 2)
    sib = me + 1 - 2 * core
    rows, span = own_v.shape
    wide = oa_hbm.shape[1]
    bufs, _, _, nc = w_v.shape
    steps = out_hbm.shape[1] // nc

    def fetch(n, slot, part):
        owner = core if part == 0 else 1 - core
        return pltpu.make_async_copy(
            wo_hbm.at[pl.ds(pl.multiple_of(owner * span, span), span), pl.ds(pl.multiple_of(n * nc, nc), nc)],
            w_v.at[slot, part], w_sem.at[slot, part])

    fetch(0, 0, 0).start()
    own = [pltpu.make_async_copy(h.at[pl.ds(core * rows, rows)], own_v.at[:, pl.ds(k * wide, wide)], o_sem.at[k])
           for k, h in enumerate((oa_hbm, ob_hbm))]
    for c in own:
        c.start()
    fetch(0, 0, 1).start()
    for n in range(1, bufs):
        for part in range(2):
            fetch(n, n, part).start()

    barrier = pltpu.get_barrier_semaphore()
    pl.semaphore_signal(barrier, inc=1, device_id={"sp": sib}, device_id_type=MESH)
    pl.semaphore_wait(barrier, 1)
    swap = [pltpu.make_async_remote_copy(
        src_ref=h.at[pl.ds((1 - core) * rows, rows)], dst_ref=sib_v.at[:, pl.ds(k * wide, wide)],
        send_sem=send_sem.at[k], recv_sem=recv_sem.at[k], device_id={"sp": sib}, device_id_type=MESH)
        for k, h in enumerate((oa_hbm, ob_hbm))]
    for c in swap:
        c.start()
    for c in own:
        c.wait()

    def store(n, slot):
        return pltpu.make_async_copy(out_v.at[slot], out_hbm.at[:, pl.ds(pl.multiple_of(n * nc, nc), nc)], out_sem.at[slot])

    def body(n, carry):
        slot = lax.rem(n, bufs)
        oslot = lax.rem(n, 2)
        fetch(n, slot, 0).wait()
        acc = jnp.dot(own_v[...], w_v[slot, 0], preferred_element_type=F32)

        @pl.when(n == 0)
        def _():
            for c in swap:
                c.wait()

        @pl.when(n >= 2)
        def _():
            store(n - 2, oslot).wait()

        fetch(n, slot, 1).wait()
        acc = acc + jnp.dot(sib_v[...], w_v[slot, 1], preferred_element_type=F32)
        out_v[oslot] = acc.astype(BF16)
        store(n, oslot).start()

        @pl.when(n + bufs < steps)
        def _():
            fetch(n + bufs, slot, 0).start()
            fetch(n + bufs, slot, 1).start()

        return carry

    lax.fori_loop(0, steps, body, 0)
    for n in range(steps - 2, steps):
        store(n, n % 2).wait()


def solution(mesh):
    ranks = mesh.shape["sp"]
    tok_spec = P(("dp", "sp"))
    rows_spec = P(("dp", "sp"), None)
    replicated = P()

    def local_step(tok_in, tok_pos, w_dq, g_q, w_uq, w_dkv, g_kv, w_uk, w_uv, w_o):
        rows, model = tok_in.shape
        num_heads = w_uq.shape[1]
        qk_dim = w_uq.shape[2]
        q_rank = w_dq.shape[1]
        kv_rank = g_kv.shape[0]
        rot = w_dkv.shape[1] - kv_rank
        nope = qk_dim - rot
        v_dim = w_uv.shape[2]
        seq = rows * ranks
        half = rot // 2
        chips = ranks // 2
        mine = num_heads // 2
        pairs = mine // 2
        pe_w = 128
        attn_scale = (0.1 * math.log(YARN_FACTOR) + 1.0) ** 2 / math.sqrt(qk_dim)
        me = lax.axis_index("sp")
        core = lax.rem(me, 2)

        angles = rope_freqs(rot)[:, None] * tok_pos.astype(F32)[None, :]
        cos_t, sin_t = jnp.cos(angles), jnp.sin(angles)

        kchunks, nq, depth = 2, 3, 64
        kv_w = kv_rank + pe_w
        any_spec = pl.BlockSpec(memory_space=pl.ANY)
        vmem_spec = pl.BlockSpec(memory_space=pltpu.VMEM)
        dma = pltpu.SemaphoreType.DMA
        kv_all, cq_all, tab_all, wk2, wv2, cache_kv, cache_pe = pl.pallas_call(
            functools.partial(front_kernel, ranks, mine),
            out_shape=(
                jax.ShapeDtypeStruct((seq, kv_w), BF16),
                jax.ShapeDtypeStruct((2 * rows, q_rank), BF16),
                jax.ShapeDtypeStruct((2, rot, rows), F32),
                jax.ShapeDtypeStruct((kv_rank, mine * nope), BF16),
                jax.ShapeDtypeStruct((kv_rank, mine * v_dim), BF16),
                jax.ShapeDtypeStruct((rows, kv_rank), BF16),
                jax.ShapeDtypeStruct((rows, rot), BF16),
            ),
            in_specs=[any_spec] * 5 + [vmem_spec] * 4,
            out_specs=(any_spec,) * 5 + (vmem_spec, vmem_spec),
            scratch_shapes=[
                pltpu.VMEM((rows, model), BF16),
                pltpu.VMEM((kchunks, kv_rank + rot, model // kchunks), BF16),
                pltpu.VMEM((nq, model, q_rank // nq), BF16),
                pltpu.VMEM((2, kv_rank, mine, nope), BF16),
                pltpu.VMEM((2, kv_rank, mine * nope), BF16),
                pltpu.VMEM((mine // 8, depth * 8, nope), F32),
                pltpu.VMEM((rows, q_rank), F32),
                pltpu.VMEM((rows, kv_w), BF16),
                pltpu.VMEM((rows, q_rank), BF16),
                pltpu.VMEM((rot, rows), F32),
                dma((1 + kchunks + nq + 2,)),
                dma((5,)),
                dma((8,)),
                dma((8,)),
                dma((2,)),
                dma((2,)),
            ],
            compiler_params=pltpu.CompilerParams(collective_id=0, has_side_effects=True, vmem_limit_bytes=60 << 20),
            cost_estimate=pl.CostEstimate(flops=2 * rows * model * (q_rank + kv_rank + rot), bytes_accessed=2 * model * (q_rank + kv_rank + rot), transcendentals=0),
        )(tok_in, w_dkv.T, w_dq, w_uk, w_uv, g_q[None, :], g_kv[None, :], cos_t, sin_t)

        wuq_t = jnp.transpose(w_uq, (1, 2, 0))
        qn = 2 * rows
        nblk = seq // qn
        idx = jnp.stack([me // 2, core * mine]).astype(jnp.int32)

        def whole(shape):
            return pl.BlockSpec(shape, lambda i, s: (0,) * len(shape))

        last = pairs - 1
        head_v = pltpu.VMEM((nblk, v_dim, qn), BF16)
        head_k = pltpu.VMEM((nblk, qn, nope + pe_w), BF16)
        head_q = pltpu.VMEM((nope + pe_w, qn), BF16)
        scores = pltpu.VMEM((nblk, qn, qn), F32)
        stat = pltpu.VMEM((8, qn), F32)
        head_o = pltpu.VMEM((v_dim, qn), F32)
        o_a, o_b = pl.pallas_call(
            functools.partial(attn_kernel, attn_scale * math.log2(math.e), pairs),
            out_shape=(jax.ShapeDtypeStruct((qn, pairs * v_dim), BF16),) * 2,
            grid_spec=pltpu.PrefetchScalarGridSpec(
                num_scalar_prefetch=1,
                grid=(pairs + 1,),
                in_specs=[
                    whole((qn, q_rank)),
                    whole((seq, kv_w)),
                    whole((2, rot, rows)),
                    pl.BlockSpec((1, qk_dim, q_rank), lambda i, s: (s[1] + jnp.minimum(i, last), 0, 0)),
                    pl.BlockSpec((1, qk_dim, q_rank), lambda i, s: (s[1] + pairs + jnp.minimum(i, last), 0, 0)),
                    pl.BlockSpec((kv_rank, nope), lambda i, s: (0, jnp.minimum(i, last))),
                    pl.BlockSpec((kv_rank, nope), lambda i, s: (0, pairs + jnp.minimum(i, last))),
                    pl.BlockSpec((kv_rank, v_dim), lambda i, s: (0, jnp.minimum(i, last))),
                    pl.BlockSpec((kv_rank, v_dim), lambda i, s: (0, pairs + jnp.minimum(i, last))),
                ],
                out_specs=(pl.BlockSpec((qn, v_dim), lambda i, s: (0, jnp.maximum(i - 1, 0))),) * 2,
                scratch_shapes=[head_k, head_k, head_v, head_v, head_v, head_q, head_q, scores, scores,
                                stat, stat, stat, stat, head_o, head_o,
                                pltpu.VMEM((half, qn), F32), pltpu.VMEM((half, qn), F32)],
            ),
            compiler_params=pltpu.CompilerParams(dimension_semantics=("arbitrary",), vmem_limit_bytes=60 << 20),
        )(idx, cq_all, kv_all, tab_all, wuq_t, wuq_t, wk2, wk2, wv2, wv2)

        nc, bufs = 512, 4
        span = mine * v_dim
        attn_out = pl.pallas_call(
            out_kernel,
            out_shape=jax.ShapeDtypeStruct((rows, model), BF16),
            in_specs=[any_spec] * 3,
            out_specs=any_spec,
            scratch_shapes=[
                pltpu.VMEM((rows, span), BF16),
                pltpu.VMEM((rows, span), BF16),
                pltpu.VMEM((bufs, 2, span, nc), BF16),
                pltpu.VMEM((2, rows, nc), BF16),
                dma((2,)),
                dma((bufs, 2)),
                dma((2,)),
                dma((2,)),
                dma((2,)),
            ],
            compiler_params=pltpu.CompilerParams(collective_id=1, has_side_effects=True, vmem_limit_bytes=60 << 20),
        )(o_a, o_b, w_o.reshape(num_heads * v_dim, model))
        return attn_out, cache_kv, cache_pe

    return jax.shard_map(local_step, mesh=mesh,
                         in_specs=(rows_spec, tok_spec) + (replicated,) * 8,
                         out_specs=(rows_spec, rows_spec, rows_spec), check_vma=False)
```

```python
import functools
import math

import jax
import jax.numpy as jnp
from jax import lax
from jax.experimental import pallas as pl
from jax.experimental.pallas import tpu as pltpu
from jax.sharding import PartitionSpec as P

ROPE_THETA = 10000.0
YARN_FACTOR = 40.0
ORIG_CTX = 4096.0
BETA_FAST = 32.0
BETA_SLOW = 1.0
NORM_EPS = 1e-6

MESH = pl.DeviceIdType.MESH
F32 = jnp.float32
BF16 = jnp.bfloat16
NT = (((1,), (1,)), ((), ()))
TT = (((0,), (1,)), ((), ()))


def rope_freqs(rot_dim):
    half_dim = rot_dim // 2
    log_base = 2.0 * math.log(ROPE_THETA)
    low_idx = max(math.floor(rot_dim * math.log(ORIG_CTX / (BETA_FAST * 2.0 * math.pi)) / log_base), 0)
    high_idx = min(math.ceil(rot_dim * math.log(ORIG_CTX / (BETA_SLOW * 2.0 * math.pi)) / log_base), half_dim - 1)
    spread = max(high_idx - low_idx, 0.001)
    freq_list = []
    for freq_idx in range(half_dim):
        base_freq = ROPE_THETA ** (-2.0 * freq_idx / rot_dim)
        ramp_val = min(max((freq_idx - low_idx) / spread, 0.0), 1.0)
        freq_list.append(base_freq / YARN_FACTOR * ramp_val + base_freq * (1.0 - ramp_val))
    return jnp.asarray(freq_list, dtype=jnp.float32)


def front_kernel(ranks, heads, x_hbm, wkv_hbm, wq_hbm, wuk_hbm, wuv_hbm, gq_ref, gkv_ref, cos_ref, sin_ref,
                 kv_all, cq_all, tab_all, wk_out, wv_out,
                 x_v, wkv_v, wq_v, wu_v, wo_v, wide_v, cq_f, kv_v, cq_v, tab_v,
                 w_sem, own_sem, kv_send, kv_recv, pair_send, pair_recv):
    me = lax.axis_index("sp")
    core = lax.rem(me, 2)
    sib = me + 1 - 2 * core
    rows = x_v.shape[0]
    half = cos_ref.shape[0]
    kv_rank = gkv_ref.shape[0]
    right = lax.rem(me + 2, ranks)
    left = lax.rem(me + ranks - 2, ranks)
    across = lax.rem(me + 4, ranks)

    kchunks, nq = wkv_v.shape[0], wq_v.shape[0]
    kc = wkv_v.shape[2]
    nc = wq_v.shape[2]
    first = core * heads
    loads = [pltpu.make_async_copy(x_hbm, x_v, w_sem.at[0])]
    loads += [pltpu.make_async_copy(wkv_hbm.at[:, pl.ds(k * kc, kc)], wkv_v.at[k], w_sem.at[1 + k]) for k in range(kchunks)]
    loads += [pltpu.make_async_copy(wq_hbm.at[:, pl.ds(k * nc, nc)], wq_v.at[k], w_sem.at[1 + kchunks + k]) for k in range(nq)]
    loads += [pltpu.make_async_copy(h.at[:, pl.ds(first, heads), :], wu_v.at[k], w_sem.at[1 + kchunks + nq + k])
              for k, h in enumerate((wuk_hbm, wuv_hbm))]
    for c in loads:
        c.start()

    barrier = pltpu.get_barrier_semaphore()
    for peer in (sib, right, left):
        pl.semaphore_signal(barrier, inc=1, device_id={"sp": peer}, device_id_type=MESH)
    pl.semaphore_wait(barrier, 3)

    def block(idx, start=0, size=None):
        return kv_all.at[pl.ds(idx * rows + start, size or rows)]

    def remote(src, dst, send, recv, dev):
        return pltpu.make_async_remote_copy(src_ref=src, dst_ref=dst, send_sem=send, recv_sem=recv,
                                            device_id={"sp": dev}, device_id_type=MESH)

    loads[0].wait()
    acc = None
    for k in range(kchunks):
        loads[1 + k].wait()
        part = lax.dot_general(x_v[:, k * kc:(k + 1) * kc], wkv_v[k], NT, preferred_element_type=F32)
        acc = part if acc is None else acc + part
    a = acc[:, :kv_rank]
    inv = lax.rsqrt(jnp.mean(a * a, axis=-1, keepdims=True) + NORM_EPS)
    ckv = (a * inv * gkv_ref[...][None, :]).astype(BF16)
    tab_v[:half, :] = cos_ref[...]
    tab_v[half:, :] = sin_ref[...]
    tab = tab_v[...].T
    cos_t, sin_t = tab[:, :half], tab[:, half:]
    z1 = acc[:, kv_rank:kv_rank + half]
    z2 = acc[:, kv_rank + half:]
    pe = jnp.concatenate([z1 * cos_t - z2 * sin_t, z2 * cos_t + z1 * sin_t], axis=-1).astype(BF16)
    kv_v[:, :kv_rank] = ckv
    kv_v[:, kv_rank:] = jnp.concatenate([pe, jnp.zeros((rows, kv_v.shape[1] - kv_rank - 2 * half), BF16)], axis=-1)

    to_sib = remote(kv_v, block(me), kv_send.at[0], kv_recv.at[0], sib)
    to_right = remote(kv_v, block(me), kv_send.at[1], kv_recv.at[1], right)
    to_left = remote(kv_v, block(me), kv_send.at[2], kv_recv.at[2], left)
    tab_copy = remote(tab_v, tab_all.at[core], pair_send.at[0], pair_recv.at[0], sib)
    for c in (to_right, to_left, to_sib, tab_copy):
        c.start()
    own = [pltpu.make_async_copy(kv_v, block(me), own_sem.at[0]),
           pltpu.make_async_copy(tab_v, tab_all.at[core], own_sem.at[1])]
    for c in own:
        c.start()

    ssq = jnp.zeros((rows, 1), F32)
    for k in range(nq):
        loads[1 + kchunks + k].wait()
        q = jnp.dot(x_v[...], wq_v[k], preferred_element_type=F32)
        cq_f[:, k * nc:(k + 1) * nc] = q
        ssq = ssq + jnp.sum(q * q, axis=-1, keepdims=True)
    inv_q = lax.rsqrt(ssq / cq_f.shape[1] + NORM_EPS)
    cq_v[...] = (cq_f[...] * inv_q * gq_ref[...][None, :]).astype(BF16)
    cq_copy = remote(cq_v, cq_all.at[pl.ds(core * rows, rows)], pair_send.at[1], pair_recv.at[1], sib)
    cq_copy.start()
    own.append(pltpu.make_async_copy(cq_v, cq_all.at[pl.ds(core * rows, rows)], own_sem.at[2]))
    own[-1].start()

    mid = rows // 2
    to_right.wait_recv()
    half_right = remote(block(left, 0, mid), block(left, 0, mid), kv_send.at[3], kv_recv.at[3], right)
    half_right.start()
    sib_left = remote(block(left), block(left), kv_send.at[5], kv_recv.at[5], sib)
    sib_left.start()
    to_left.wait_recv()
    half_left = remote(block(right, mid, mid), block(right, mid, mid), kv_send.at[4], kv_recv.at[4], left)
    half_left.start()
    sib_right = remote(block(right), block(right), kv_send.at[6], kv_recv.at[6], sib)
    sib_right.start()

    depth = wide_v.shape[1] // 8
    groups = wide_v.shape[0]
    width = wide_v.shape[2]
    for t, out in enumerate((wk_out, wv_out)):
        loads[1 + kchunks + nq + t].wait()

        def relayout(i, _, t=t):
            base = pl.multiple_of(i * depth, depth)
            for g in range(groups):
                wide_v[g] = wu_v[t, pl.ds(base, depth), g * 8:(g + 1) * 8, :].astype(F32).reshape(depth * 8, width)
            for g in range(groups):
                for h in range(8):
                    col = (g * 8 + h) * width
                    wo_v[t, pl.ds(base, depth), col:col + width] = wide_v[g, pl.ds(h, depth, stride=8), :].astype(BF16)
            return _

        lax.fori_loop(0, wu_v.shape[1] // depth, relayout, 0)
        own.append(pltpu.make_async_copy(wo_v.at[t], out, own_sem.at[3 + t]))
        own[-1].start()

    half_right.wait_recv()
    half_left.wait_recv()
    sib_across = remote(block(across), block(across), kv_send.at[7], kv_recv.at[7], sib)
    sib_across.start()
    to_sib.wait()
    to_right.wait_send()
    to_left.wait_send()
    half_right.wait_send()
    half_left.wait_send()
    for c in (sib_left, sib_right, sib_across, tab_copy, cq_copy):
        c.wait()
    for c in own:
        c.wait()


def attn_kernel(scale2, steps, cq_ref, kv_ref, tab_ref,
                wqa_ref, wqb_ref, wka_ref, wkb_ref, wva_ref, wvb_ref, oa_ref, ob_ref, ckv_ref, cpe_ref,
                k_v, v_a, v_b, q_v, s_a, s_b, m_a, m_b, l_a, l_b, o_a, o_b, cosq_ref, sinq_ref):
    step = pl.program_id(0)
    me = lax.axis_index("sp")
    full = me // 2
    _, blocks, blk, kdim = k_v.shape
    kv_rank = wka_ref.shape[0]
    nope = wka_ref.shape[1] // 2
    half = cosq_ref.shape[0]
    rot = 2 * half
    sub = blk // 2
    everything = slice(None)

    @pl.when(step == 0)
    def _():
        for kb in range(blocks):
            pe = kv_ref[kb * blk:(kb + 1) * blk, kv_rank:]
            k_v[0, kb, :, nope:] = pe
            k_v[1, kb, :, nope:] = pe
        q_v[:, nope + rot:, :] = jnp.zeros((2, kdim - nope - rot, blk), BF16)
        for c in range(2):
            cosq_ref[:, c * sub:(c + 1) * sub] = tab_ref[c, :half, :]
            sinq_ref[:, c * sub:(c + 1) * sub] = tab_ref[c, half:, :]
        v_b[...] = jnp.zeros_like(v_b)
        s_b[...] = jnp.zeros_like(s_b)
        m_b[...] = jnp.zeros_like(m_b)
        o_a[...] = jnp.zeros_like(o_a)
        l_a[...] = jnp.ones_like(l_a)
        rows = ckv_ref.shape[0]
        own = kv_ref[pl.ds(pl.multiple_of(me * rows, rows), rows), :]
        ckv_ref[...] = own[:, :kv_rank]
        cpe_ref[...] = own[:, kv_rank:kv_rank + rot]

    def q_proj(w_ref):
        w = jnp.concatenate([w_ref[0], w_ref[1]], axis=0)
        both = lax.dot_general(w, cq_ref[...], NT, preferred_element_type=F32)
        for h in range(2):
            u = both[h * (nope + rot):(h + 1) * (nope + rot)]
            q_v[h, :nope, :] = u[:nope].astype(BF16)
            z1 = u[nope:nope + half]
            z2 = u[nope + half:]
            q_v[h, nope:nope + half, :] = (z1 * cosq_ref[...] - z2 * sinq_ref[...]).astype(BF16)
            q_v[h, nope + half:nope + rot, :] = (z2 * cosq_ref[...] + z1 * sinq_ref[...]).astype(BF16)

    def kv_proj(kb, wk, wv, v_ref):
        c = kv_ref[pl.ds(pl.multiple_of(kb * blk, blk), blk), :kv_rank]
        k = jnp.dot(c, wk, preferred_element_type=F32).astype(BF16)
        v = lax.dot_general(wv, c, NT, preferred_element_type=F32).astype(BF16)
        for h in range(2):
            k_v[h, kb, :, :nope] = k[:, h * nope:(h + 1) * nope]
            v_ref[h, kb] = v[h * nope:(h + 1) * nope]

    def fold_max(m_ref, h, s, cols):
        t = jnp.max(s.reshape(s.shape[0] // 8, 8, s.shape[1]), axis=0)
        m_ref[h, :, cols] = jnp.maximum(m_ref[h, :, cols], t)

    def qk(h, kb, s_ref, m_ref):
        s = jnp.dot(k_v[h, kb], q_v[h], preferred_element_type=F32)
        s_ref[h, kb] = s
        fold_max(m_ref, h, s, everything)

    def qk_diag(h, kb, s_ref, m_ref):
        s0 = jnp.dot(k_v[h, kb, :sub, :], q_v[h], preferred_element_type=F32)
        s1 = jnp.dot(k_v[h, kb, sub:, :], q_v[h, :, sub:], preferred_element_type=F32)
        keep = lax.broadcasted_iota(jnp.int32, (sub, sub), 0) <= lax.broadcasted_iota(jnp.int32, (sub, sub), 1)
        s00 = jnp.where(keep, s0[:, :sub], -jnp.inf)
        s1 = jnp.where(keep, s1, -jnp.inf)
        s01 = s0[:, sub:]
        s_ref[h, kb, :sub, :sub] = s00
        s_ref[h, kb, :sub, sub:] = s01
        s_ref[h, kb, sub:, sub:] = s1
        fold_max(m_ref, h, s00, slice(0, sub))
        fold_max(m_ref, h, s01, slice(sub, blk))
        fold_max(m_ref, h, s1, slice(sub, blk))

    def fold_sum(l_ref, h, p, cols):
        l_ref[h, :, cols] += jnp.sum(p.reshape(p.shape[0] // 8, 8, p.shape[1]), axis=0)

    def top(m_ref):
        return [jnp.max(m_ref[h], axis=0, keepdims=True) for h in range(2)]

    def pv(h, kb, v_ref, s_ref, m, l_ref, o_ref):
        p = jnp.exp2((s_ref[h, kb] - m[h]) * scale2)
        fold_sum(l_ref, h, p, everything)
        o_ref[h] += jnp.dot(v_ref[h, kb], p.astype(BF16), preferred_element_type=F32)

    def pv_diag(h, kb, v_ref, s_ref, m, l_ref, o_ref):
        p0 = jnp.exp2((s_ref[h, kb, :sub, :] - m[h]) * scale2)
        p1 = jnp.exp2((s_ref[h, kb, sub:, sub:] - m[h][:, sub:]) * scale2)
        fold_sum(l_ref, h, p0, everything)
        fold_sum(l_ref, h, p1, slice(sub, blk))
        p0 = p0.astype(BF16)
        o_ref[h] += jnp.dot(v_ref[h, kb, :, :sub], p0, preferred_element_type=F32)
        o_ref[h, :, sub:] += jnp.dot(v_ref[h, kb, :, sub:], p1.astype(BF16), preferred_element_type=F32)

    def finish(l_ref, o_ref, out_ref):
        for h in range(2):
            l = jnp.sum(l_ref[h], axis=0, keepdims=True)
            out_ref[:, h * nope:(h + 1) * nope] = (o_ref[h] / l).T.astype(BF16)

    def clear(l_ref, o_ref):
        l_ref[...] = jnp.zeros_like(l_ref)
        o_ref[...] = jnp.zeros_like(o_ref)

    def stage(wq_ref, wk_ref, wv_ref, new, old, done, done_out):
        s_n, m_n, v_n = new
        s_o, m_o, v_o, l_o, out_o = old
        m = top(m_o)
        q_proj(wq_ref)
        finish(done[0], done[1], done_out)
        clear(l_o, out_o)
        m_n[...] = jnp.full_like(m_n, -jnp.inf)
        wk = wk_ref[...]
        wv = wv_ref[...].T

        def body(kb, carry):
            kv_proj(kb, wk, wv, v_n)
            for h in range(2):
                pv(h, kb, v_o, s_o, m, l_o, out_o)
                qk(h, kb, s_n, m_n)
            return carry

        lax.fori_loop(0, full, body, 0)
        kv_proj(full, wk, wv, v_n)
        for h in range(2):
            pv_diag(h, full, v_o, s_o, m, l_o, out_o)
            qk_diag(h, full, s_n, m_n)

    @pl.when(step < steps)
    def _():
        stage(wqa_ref, wka_ref, wva_ref, (s_a, m_a, v_a), (s_b, m_b, v_b, l_b, o_b), (l_a, o_a), oa_ref)
        stage(wqb_ref, wkb_ref, wvb_ref, (s_b, m_b, v_b), (s_a, m_a, v_a, l_a, o_a), (l_b, o_b), ob_ref)

    @pl.when(step == steps)
    def _():
        m = top(m_b)
        clear(l_b, o_b)
        finish(l_a, o_a, oa_ref)

        def body(kb, carry):
            for h in range(2):
                pv(h, kb, v_b, s_b, m, l_b, o_b)
            return carry

        lax.fori_loop(0, full, body, 0)
        for h in range(2):
            pv_diag(h, full, v_b, s_b, m, l_b, o_b)
        finish(l_b, o_b, ob_ref)


def out_kernel(oa_hbm, ob_hbm, wo_hbm, out_hbm, own_v, sib_v, w_v, acc_v, out_v,
               o_sem, w_sem, out_sem, swap_send, swap_recv, res_send, res_recv):
    me = lax.axis_index("sp")
    core = lax.rem(me, 2)
    sib = me + 1 - 2 * core
    wide = oa_hbm.shape[1]
    span = own_v.shape[1]
    rows = out_hbm.shape[0]
    bufs, _, nc = w_v.shape
    steps = acc_v.shape[0]

    def fetch(i):
        part = i // steps
        owner = core + part - 2 * core * part
        col = core * (steps * nc) + lax.rem(i, steps) * nc
        slot = lax.rem(i, bufs)
        return pltpu.make_async_copy(
            wo_hbm.at[pl.ds(pl.multiple_of(owner * span, span), span), pl.ds(pl.multiple_of(col, nc), nc)],
            w_v.at[slot], w_sem.at[slot])

    own = [pltpu.make_async_copy(h, own_v.at[:, pl.ds(k * wide, wide)], o_sem.at[k])
           for k, h in enumerate((oa_hbm, ob_hbm))]
    fetch(0).start()
    for c in own:
        c.start()
    for i in range(1, bufs):
        fetch(i).start()

    barrier = pltpu.get_barrier_semaphore()
    pl.semaphore_signal(barrier, inc=1, device_id={"sp": sib}, device_id_type=MESH)
    pl.semaphore_wait(barrier, 1)
    swap = [pltpu.make_async_remote_copy(
        src_ref=h, dst_ref=sib_v.at[:, pl.ds(k * wide, wide)],
        send_sem=swap_send.at[k], recv_sem=swap_recv.at[k], device_id={"sp": sib}, device_id_type=MESH)
        for k, h in enumerate((oa_hbm, ob_hbm))]
    for c in swap:
        c.start()
    for c in own:
        c.wait()

    def own_half(i, carry):
        fetch(i).wait()
        acc_v[i] = jnp.dot(own_v[...], w_v[lax.rem(i, bufs)], preferred_element_type=F32)

        @pl.when(i + bufs < 2 * steps)
        def _():
            fetch(i + bufs).start()

        return carry

    lax.fori_loop(0, steps, own_half, 0)
    for c in swap:
        c.wait()

    def store(n):
        slot = lax.rem(n, 2)
        cols = pl.ds(pl.multiple_of(core * (steps * nc) + n * nc, nc), nc)
        keep = pltpu.make_async_copy(out_v.at[slot, pl.ds(pl.multiple_of(core * rows, rows), rows)],
                                     out_hbm.at[:, cols], out_sem.at[slot])
        give = pltpu.make_async_remote_copy(
            src_ref=out_v.at[slot, pl.ds(pl.multiple_of((1 - core) * rows, rows), rows)], dst_ref=out_hbm.at[:, cols],
            send_sem=res_send.at[n], recv_sem=res_recv.at[n], device_id={"sp": sib}, device_id_type=MESH)
        return keep, give

    def sib_half(n, carry):
        i = n + steps
        fetch(i).wait()

        @pl.when(n >= 2)
        def _():
            keep, give = store(n - 2)
            keep.wait()
            give.wait_send()

        out_v[lax.rem(n, 2)] = (acc_v[n] + jnp.dot(sib_v[...], w_v[lax.rem(i, bufs)], preferred_element_type=F32)).astype(BF16)
        for c in store(n):
            c.start()

        @pl.when(i + bufs < 2 * steps)
        def _():
            fetch(i + bufs).start()

        return carry

    lax.fori_loop(0, steps, sib_half, 0)
    for n in range(steps - 2, steps):
        keep, give = store(n)
        keep.wait()
        give.wait_send()
    for n in range(steps):
        store(n)[1].wait_recv()


def solution(mesh):
    ranks = mesh.shape["sp"]
    tok_spec = P(("dp", "sp"))
    rows_spec = P(("dp", "sp"), None)
    replicated = P()

    def local_step(tok_in, tok_pos, w_dq, g_q, w_uq, w_dkv, g_kv, w_uk, w_uv, w_o):
        rows, model = tok_in.shape
        num_heads = w_uq.shape[1]
        qk_dim = w_uq.shape[2]
        q_rank = w_dq.shape[1]
        kv_rank = g_kv.shape[0]
        rot = w_dkv.shape[1] - kv_rank
        nope = qk_dim - rot
        v_dim = w_uv.shape[2]
        seq = rows * ranks
        half = rot // 2
        mine = num_heads // 2
        pe_w = 128
        attn_scale = (0.1 * math.log(YARN_FACTOR) + 1.0) ** 2 / math.sqrt(qk_dim)
        angles = rope_freqs(rot)[:, None] * tok_pos.astype(F32)[None, :]
        cos_t, sin_t = jnp.cos(angles), jnp.sin(angles)

        kchunks, nq, depth = 2, 3, 64
        kv_w = kv_rank + pe_w
        any_spec = pl.BlockSpec(memory_space=pl.ANY)
        vmem_spec = pl.BlockSpec(memory_space=pltpu.VMEM)
        dma = pltpu.SemaphoreType.DMA
        kv_all, cq_all, tab_all, wk2, wv2 = pl.pallas_call(
            functools.partial(front_kernel, ranks, mine),
            out_shape=(
                jax.ShapeDtypeStruct((seq, kv_w), BF16),
                jax.ShapeDtypeStruct((2 * rows, q_rank), BF16),
                jax.ShapeDtypeStruct((2, rot, rows), F32),
                jax.ShapeDtypeStruct((kv_rank, mine * nope), BF16),
                jax.ShapeDtypeStruct((kv_rank, mine * v_dim), BF16),
            ),
            in_specs=[any_spec] * 5 + [vmem_spec] * 4,
            out_specs=(any_spec,) * 5,
            scratch_shapes=[
                pltpu.VMEM((rows, model), BF16),
                pltpu.VMEM((kchunks, kv_rank + rot, model // kchunks), BF16),
                pltpu.VMEM((nq, model, q_rank // nq), BF16),
                pltpu.VMEM((2, kv_rank, mine, nope), BF16),
                pltpu.VMEM((2, kv_rank, mine * nope), BF16),
                pltpu.VMEM((mine // 8, depth * 8, nope), F32),
                pltpu.VMEM((rows, q_rank), F32),
                pltpu.VMEM((rows, kv_w), BF16),
                pltpu.VMEM((rows, q_rank), BF16),
                pltpu.VMEM((rot, rows), F32),
                dma((1 + kchunks + nq + 2,)),
                dma((5,)),
                dma((8,)),
                dma((8,)),
                dma((2,)),
                dma((2,)),
            ],
            compiler_params=pltpu.CompilerParams(collective_id=0, has_side_effects=True, vmem_limit_bytes=60 << 20),
            cost_estimate=pl.CostEstimate(flops=2 * rows * model * (q_rank + kv_rank + rot), bytes_accessed=2 * model * (q_rank + kv_rank + rot), transcendentals=0),
        )(tok_in, w_dkv.T, w_dq, w_uk, w_uv, g_q, g_kv, cos_t, sin_t)

        wuq_t = jnp.transpose(w_uq, (1, 2, 0))
        qn = 2 * rows
        nblk = seq // qn
        steps = mine // 4
        last = steps - 1

        def whole(shape):
            return pl.BlockSpec(shape, lambda i: (0,) * len(shape))

        def up_spec(part):
            return pl.BlockSpec((2, qk_dim, q_rank), lambda i: (lax.rem(lax.axis_index("sp"), 2) * (mine // 2) + part * steps + jnp.minimum(i, last), 0, 0))

        def lat_spec(part):
            return pl.BlockSpec((kv_rank, 2 * nope), lambda i: (0, part * steps + jnp.minimum(i, last)))

        head_v = pltpu.VMEM((2, nblk, v_dim, qn), BF16)
        scores = pltpu.VMEM((2, nblk, qn, qn), F32)
        stat = pltpu.VMEM((2, 8, qn), F32)
        head_o = pltpu.VMEM((2, v_dim, qn), F32)
        o_a, o_b, cache_kv, cache_pe = pl.pallas_call(
            functools.partial(attn_kernel, attn_scale * math.log2(math.e), steps),
            out_shape=(jax.ShapeDtypeStruct((qn, 2 * steps * v_dim), BF16),) * 2 + (
                jax.ShapeDtypeStruct((rows, kv_rank), BF16),
                jax.ShapeDtypeStruct((rows, rot), BF16),
            ),
            grid=(steps + 1,),
            in_specs=[
                whole((qn, q_rank)),
                whole((seq, kv_w)),
                whole((2, rot, rows)),
                up_spec(0), up_spec(1), lat_spec(0), lat_spec(1), lat_spec(0), lat_spec(1),
            ],
            out_specs=(pl.BlockSpec((qn, 2 * v_dim), lambda i: (0, jnp.maximum(i - 1, 0))),) * 2 + (
                whole((rows, kv_rank)), whole((rows, rot))),
            scratch_shapes=[pltpu.VMEM((2, nblk, qn, nope + pe_w), BF16), head_v, head_v, pltpu.VMEM((2, nope + pe_w, qn), BF16),
                            scores, scores, stat, stat, stat, stat, head_o, head_o,
                            pltpu.VMEM((half, qn), F32), pltpu.VMEM((half, qn), F32)],
            compiler_params=pltpu.CompilerParams(dimension_semantics=("arbitrary",), vmem_limit_bytes=60 << 20),
        )(cq_all, kv_all, tab_all, wuq_t, wuq_t, wk2, wk2, wv2, wv2)

        nc, bufs = 512, 6
        span = mine * v_dim
        pieces = model // 2 // nc
        attn_out = pl.pallas_call(
            out_kernel,
            out_shape=jax.ShapeDtypeStruct((rows, model), BF16),
            in_specs=[any_spec] * 3,
            out_specs=any_spec,
            scratch_shapes=[
                pltpu.VMEM((qn, span), BF16),
                pltpu.VMEM((qn, span), BF16),
                pltpu.VMEM((bufs, span, nc), BF16),
                pltpu.VMEM((pieces, qn, nc), F32),
                pltpu.VMEM((2, qn, nc), BF16),
                dma((2,)),
                dma((bufs,)),
                dma((2,)),
                dma((2,)),
                dma((2,)),
                dma((pieces,)),
                dma((pieces,)),
            ],
            compiler_params=pltpu.CompilerParams(collective_id=1, has_side_effects=True, vmem_limit_bytes=60 << 20),
        )(o_a, o_b, w_o.reshape(num_heads * v_dim, model))
        return attn_out, cache_kv, cache_pe

    return jax.shard_map(local_step, mesh=mesh,
                         in_specs=(rows_spec, tok_spec) + (replicated,) * 8,
                         out_specs=(rows_spec, rows_spec, rows_spec), check_vma=False)
```

```python
import functools
import math

import jax
import jax.numpy as jnp
from jax import lax
from jax.experimental import pallas as pl
from jax.experimental.pallas import tpu as pltpu
from jax.sharding import PartitionSpec as P

ROPE_THETA = 10000.0
YARN_FACTOR = 40.0
ORIG_CTX = 4096.0
BETA_FAST = 32.0
BETA_SLOW = 1.0
NORM_EPS = 1e-6

MESH = pl.DeviceIdType.MESH
F32 = jnp.float32
BF16 = jnp.bfloat16
NT = (((1,), (1,)), ((), ()))
TT = (((0,), (1,)), ((), ()))


def rope_freqs(rot_dim):
    half_dim = rot_dim // 2
    log_base = 2.0 * math.log(ROPE_THETA)
    low_idx = max(math.floor(rot_dim * math.log(ORIG_CTX / (BETA_FAST * 2.0 * math.pi)) / log_base), 0)
    high_idx = min(math.ceil(rot_dim * math.log(ORIG_CTX / (BETA_SLOW * 2.0 * math.pi)) / log_base), half_dim - 1)
    spread = max(high_idx - low_idx, 0.001)
    freq_list = []
    for freq_idx in range(half_dim):
        base_freq = ROPE_THETA ** (-2.0 * freq_idx / rot_dim)
        ramp_val = min(max((freq_idx - low_idx) / spread, 0.0), 1.0)
        freq_list.append(base_freq / YARN_FACTOR * ramp_val + base_freq * (1.0 - ramp_val))
    return jnp.asarray(freq_list, dtype=jnp.float32)


def front_kernel(ranks, heads, x_hbm, wkv_hbm, wq_hbm, wuk_hbm, wuv_hbm, gq_ref, gkv_ref, cos_ref, sin_ref,
                 kv_all, cq_all, tab_all, wk_out, wv_out,
                 x_v, wkv_v, wq_v, wu_v, wo_v, wide_v, cq_f, kv_v, cq_v, tab_v,
                 w_sem, own_sem, kv_send, kv_recv, pair_send, pair_recv):
    me = lax.axis_index("sp")
    core = lax.rem(me, 2)
    sib = me + 1 - 2 * core
    rows = x_v.shape[0]
    half = cos_ref.shape[0]
    kv_rank = gkv_ref.shape[0]
    right = lax.rem(me + 2, ranks)
    left = lax.rem(me + ranks - 2, ranks)
    across = lax.rem(me + 4, ranks)

    kchunks, nq = wkv_v.shape[0], wq_v.shape[0]
    kc = wkv_v.shape[2]
    nc = wq_v.shape[2]
    first = core * heads
    loads = []
    for k in range(kchunks):
        cols = pl.ds(k * kc, kc)
        loads.append([pltpu.make_async_copy(x_hbm.at[:, cols], x_v.at[:, cols], w_sem.at[2 * k]),
                      pltpu.make_async_copy(wkv_hbm.at[:, cols], wkv_v.at[k], w_sem.at[2 * k + 1])])
    base = 2 * kchunks
    loads += [[pltpu.make_async_copy(wq_hbm.at[:, pl.ds(k * nc, nc)], wq_v.at[k], w_sem.at[base + k])] for k in range(nq)]
    loads += [[pltpu.make_async_copy(h.at[:, pl.ds(first, heads), :], wu_v.at[k], w_sem.at[base + nq + k])]
              for k, h in enumerate((wuk_hbm, wuv_hbm))]
    ahead = 3

    def launch(i):
        if i < len(loads):
            for c in loads[i]:
                c.start()

    def arrive(i):
        for c in loads[i]:
            c.wait()
        launch(i + ahead)

    for i in range(ahead):
        launch(i)

    barrier = pltpu.get_barrier_semaphore()
    for peer in (sib, right, left):
        pl.semaphore_signal(barrier, inc=1, device_id={"sp": peer}, device_id_type=MESH)
    pl.semaphore_wait(barrier, 3)

    def block(idx, start=0, size=None):
        return kv_all.at[pl.ds(idx * rows + start, size or rows)]

    def remote(src, dst, send, recv, dev):
        return pltpu.make_async_remote_copy(src_ref=src, dst_ref=dst, send_sem=send, recv_sem=recv,
                                            device_id={"sp": dev}, device_id_type=MESH)

    acc = None
    for k in range(kchunks):
        arrive(k)
        part = lax.dot_general(x_v[:, k * kc:(k + 1) * kc], wkv_v[k], NT, preferred_element_type=F32)
        acc = part if acc is None else acc + part
    a = acc[:, :kv_rank]
    inv = lax.rsqrt(jnp.mean(a * a, axis=-1, keepdims=True) + NORM_EPS)
    ckv = (a * inv * gkv_ref[...][None, :]).astype(BF16)
    tab_v[:half, :] = cos_ref[...]
    tab_v[half:, :] = sin_ref[...]
    tab = tab_v[...].T
    cos_t, sin_t = tab[:, :half], tab[:, half:]
    z1 = acc[:, kv_rank:kv_rank + half]
    z2 = acc[:, kv_rank + half:]
    pe = jnp.concatenate([z1 * cos_t - z2 * sin_t, z2 * cos_t + z1 * sin_t], axis=-1).astype(BF16)
    kv_v[:, :kv_rank] = ckv
    kv_v[:, kv_rank:] = jnp.concatenate([pe, jnp.zeros((rows, kv_v.shape[1] - kv_rank - 2 * half), BF16)], axis=-1)

    to_sib = remote(kv_v, block(me), kv_send.at[0], kv_recv.at[0], sib)
    to_right = remote(kv_v, block(me), kv_send.at[1], kv_recv.at[1], right)
    to_left = remote(kv_v, block(me), kv_send.at[2], kv_recv.at[2], left)
    tab_copy = remote(tab_v, tab_all.at[core], pair_send.at[0], pair_recv.at[0], sib)
    for c in (to_right, to_left, to_sib, tab_copy):
        c.start()
    own = [pltpu.make_async_copy(kv_v, block(me), own_sem.at[0]),
           pltpu.make_async_copy(tab_v, tab_all.at[core], own_sem.at[1])]
    for c in own:
        c.start()

    ssq = jnp.zeros((rows, 1), F32)
    for k in range(nq):
        arrive(kchunks + k)
        q = jnp.dot(x_v[...], wq_v[k], preferred_element_type=F32)
        cq_f[:, k * nc:(k + 1) * nc] = q
        ssq = ssq + jnp.sum(q * q, axis=-1, keepdims=True)
    inv_q = lax.rsqrt(ssq / cq_f.shape[1] + NORM_EPS)
    cq_v[...] = (cq_f[...] * inv_q * gq_ref[...][None, :]).astype(BF16)
    cq_copy = remote(cq_v, cq_all.at[pl.ds(core * rows, rows)], pair_send.at[1], pair_recv.at[1], sib)
    cq_copy.start()
    own.append(pltpu.make_async_copy(cq_v, cq_all.at[pl.ds(core * rows, rows)], own_sem.at[2]))
    own[-1].start()

    mid = rows // 2
    to_right.wait_recv()
    half_right = remote(block(left, 0, mid), block(left, 0, mid), kv_send.at[3], kv_recv.at[3], right)
    half_right.start()
    sib_left = remote(block(left), block(left), kv_send.at[5], kv_recv.at[5], sib)
    sib_left.start()
    to_left.wait_recv()
    half_left = remote(block(right, mid, mid), block(right, mid, mid), kv_send.at[4], kv_recv.at[4], left)
    half_left.start()
    sib_right = remote(block(right), block(right), kv_send.at[6], kv_recv.at[6], sib)
    sib_right.start()

    depth = wide_v.shape[1] // 8
    groups = wide_v.shape[0]
    width = wide_v.shape[2]
    for t, out in enumerate((wk_out, wv_out)):
        arrive(kchunks + nq + t)

        def relayout(i, _, t=t):
            base = pl.multiple_of(i * depth, depth)
            for g in range(groups):
                wide_v[g] = wu_v[t, pl.ds(base, depth), g * 8:(g + 1) * 8, :].astype(F32).reshape(depth * 8, width)
            for g in range(groups):
                for h in range(8):
                    col = (g * 8 + h) * width
                    wo_v[t, pl.ds(base, depth), col:col + width] = wide_v[g, pl.ds(h, depth, stride=8), :].astype(BF16)
            return _

        lax.fori_loop(0, wu_v.shape[1] // depth, relayout, 0)
        own.append(pltpu.make_async_copy(wo_v.at[t], out, own_sem.at[3 + t]))
        own[-1].start()

    half_right.wait_recv()
    half_left.wait_recv()
    sib_across = remote(block(across), block(across), kv_send.at[7], kv_recv.at[7], sib)
    sib_across.start()
    to_sib.wait()
    to_right.wait_send()
    to_left.wait_send()
    half_right.wait_send()
    half_left.wait_send()
    for c in (sib_left, sib_right, sib_across, tab_copy, cq_copy):
        c.wait()
    for c in own:
        c.wait()


def attn_kernel(scale2, steps, cq_ref, kv_ref, tab_ref,
                wqa_ref, wqb_ref, wka_ref, wkb_ref, wva_ref, wvb_ref, oa_ref, ob_ref, ckv_ref, cpe_ref,
                k_v, v_a, v_b, q_v, s_a, s_b, m_a, m_b, l_a, l_b, o_a, o_b, cosq_ref, sinq_ref):
    step = pl.program_id(0)
    me = lax.axis_index("sp")
    full = me // 2
    _, blocks, blk, kdim = k_v.shape
    kv_rank = wka_ref.shape[0]
    nope = wka_ref.shape[1] // 2
    half = cosq_ref.shape[0]
    rot = 2 * half
    sub = blk // 2
    everything = slice(None)

    @pl.when(step == 0)
    def _():
        for kb in range(blocks):
            pe = kv_ref[kb * blk:(kb + 1) * blk, kv_rank:]
            k_v[0, kb, :, nope:] = pe
            k_v[1, kb, :, nope:] = pe
        q_v[:, nope + rot:, :] = jnp.zeros((2, kdim - nope - rot, blk), BF16)
        for c in range(2):
            cosq_ref[:, c * sub:(c + 1) * sub] = tab_ref[c, :half, :]
            sinq_ref[:, c * sub:(c + 1) * sub] = tab_ref[c, half:, :]
        rows = ckv_ref.shape[0]
        own = kv_ref[pl.ds(pl.multiple_of(me * rows, rows), rows), :]
        ckv_ref[...] = own[:, :kv_rank]
        cpe_ref[...] = own[:, kv_rank:kv_rank + rot]

    def q_proj(w_ref):
        w = jnp.concatenate([w_ref[0], w_ref[1]], axis=0)
        both = lax.dot_general(w, cq_ref[...], NT, preferred_element_type=F32)
        for h in range(2):
            u = both[h * (nope + rot):(h + 1) * (nope + rot)]
            q_v[h, :nope, :] = u[:nope].astype(BF16)
            z1 = u[nope:nope + half]
            z2 = u[nope + half:]
            q_v[h, nope:nope + half, :] = (z1 * cosq_ref[...] - z2 * sinq_ref[...]).astype(BF16)
            q_v[h, nope + half:nope + rot, :] = (z2 * cosq_ref[...] + z1 * sinq_ref[...]).astype(BF16)

    def kv_proj(kb, wk, wv, v_ref):
        c = kv_ref[pl.ds(pl.multiple_of(kb * blk, blk), blk), :kv_rank]
        k = jnp.dot(c, wk, preferred_element_type=F32).astype(BF16)
        v = lax.dot_general(wv, c, NT, preferred_element_type=F32).astype(BF16)
        for h in range(2):
            k_v[h, kb, :, :nope] = k[:, h * nope:(h + 1) * nope]
            v_ref[h, kb] = v[h * nope:(h + 1) * nope]

    def fold_max(m_ref, h, s, cols):
        t = jnp.max(s.reshape(s.shape[0] // 8, 8, s.shape[1]), axis=0)
        m_ref[h, :, cols] = jnp.maximum(m_ref[h, :, cols], t)

    def qk(h, kb, s_ref, m_ref):
        s = jnp.dot(k_v[h, kb], q_v[h], preferred_element_type=F32)
        s_ref[h, kb] = s
        fold_max(m_ref, h, s, everything)

    def qk_diag(h, kb, s_ref, m_ref):
        s0 = jnp.dot(k_v[h, kb, :sub, :], q_v[h], preferred_element_type=F32)
        s1 = jnp.dot(k_v[h, kb, sub:, :], q_v[h, :, sub:], preferred_element_type=F32)
        keep = lax.broadcasted_iota(jnp.int32, (sub, sub), 0) <= lax.broadcasted_iota(jnp.int32, (sub, sub), 1)
        s00 = jnp.where(keep, s0[:, :sub], -jnp.inf)
        s1 = jnp.where(keep, s1, -jnp.inf)
        s01 = s0[:, sub:]
        s_ref[h, kb, :sub, :sub] = s00
        s_ref[h, kb, :sub, sub:] = s01
        s_ref[h, kb, sub:, sub:] = s1
        fold_max(m_ref, h, s00, slice(0, sub))
        fold_max(m_ref, h, s01, slice(sub, blk))
        fold_max(m_ref, h, s1, slice(sub, blk))

    def fold_sum(l_ref, h, p, cols):
        l_ref[h, :, cols] += jnp.sum(p.reshape(p.shape[0] // 8, 8, p.shape[1]), axis=0)

    def top(m_ref):
        return [jnp.max(m_ref[h], axis=0, keepdims=True) for h in range(2)]

    def pv(h, kb, v_ref, s_ref, m, l_ref, o_ref):
        p = jnp.exp2((s_ref[h, kb] - m[h]) * scale2)
        fold_sum(l_ref, h, p, everything)
        o_ref[h] += jnp.dot(v_ref[h, kb], p.astype(BF16), preferred_element_type=F32)

    def pv_diag(h, kb, v_ref, s_ref, m, l_ref, o_ref):
        p0 = jnp.exp2((s_ref[h, kb, :sub, :] - m[h]) * scale2)
        p1 = jnp.exp2((s_ref[h, kb, sub:, sub:] - m[h][:, sub:]) * scale2)
        fold_sum(l_ref, h, p0, everything)
        fold_sum(l_ref, h, p1, slice(sub, blk))
        p0 = p0.astype(BF16)
        o_ref[h] += jnp.dot(v_ref[h, kb, :, :sub], p0, preferred_element_type=F32)
        o_ref[h, :, sub:] += jnp.dot(v_ref[h, kb, :, sub:], p1.astype(BF16), preferred_element_type=F32)

    def finish(l_ref, o_ref, out_ref):
        for h in range(2):
            l = jnp.sum(l_ref[h], axis=0, keepdims=True)
            out_ref[:, h * nope:(h + 1) * nope] = (o_ref[h] / l).T.astype(BF16)

    def clear(l_ref, o_ref):
        l_ref[...] = jnp.zeros_like(l_ref)
        o_ref[...] = jnp.zeros_like(o_ref)

    def stage(wq_ref, wk_ref, wv_ref, new, old, done, done_out):
        s_n, m_n, v_n = new
        s_o, m_o, v_o, l_o, out_o = old
        m = top(m_o)
        q_proj(wq_ref)
        finish(done[0], done[1], done_out)
        clear(l_o, out_o)
        m_n[...] = jnp.full_like(m_n, -jnp.inf)
        wk = wk_ref[...]
        wv = wv_ref[...].T

        def body(kb, carry):
            kv_proj(kb, wk, wv, v_n)
            for h in range(2):
                pv(h, kb, v_o, s_o, m, l_o, out_o)
                qk(h, kb, s_n, m_n)
            return carry

        lax.fori_loop(0, full, body, 0)
        kv_proj(full, wk, wv, v_n)
        for h in range(2):
            pv_diag(h, full, v_o, s_o, m, l_o, out_o)
            qk_diag(h, full, s_n, m_n)

    @pl.when(step < steps)
    def _():
        stage(wqa_ref, wka_ref, wva_ref, (s_a, m_a, v_a), (s_b, m_b, v_b, l_b, o_b), (l_a, o_a), oa_ref)
        stage(wqb_ref, wkb_ref, wvb_ref, (s_b, m_b, v_b), (s_a, m_a, v_a, l_a, o_a), (l_b, o_b), ob_ref)

    @pl.when(step == steps)
    def _():
        m = top(m_b)
        clear(l_b, o_b)
        finish(l_a, o_a, oa_ref)

        def body(kb, carry):
            for h in range(2):
                pv(h, kb, v_b, s_b, m, l_b, o_b)
            return carry

        lax.fori_loop(0, full, body, 0)
        for h in range(2):
            pv_diag(h, full, v_b, s_b, m, l_b, o_b)
        finish(l_b, o_b, ob_ref)


def out_kernel(oa_hbm, ob_hbm, wo_hbm, out_hbm, own_v, sib_v, w_v, acc_v, out_v,
               o_sem, w_sem, out_sem, swap_send, swap_recv, res_send, res_recv):
    me = lax.axis_index("sp")
    core = lax.rem(me, 2)
    sib = me + 1 - 2 * core
    wide = oa_hbm.shape[1]
    span = own_v.shape[1]
    rows = out_hbm.shape[0]
    bufs, _, nc = w_v.shape
    steps = acc_v.shape[0]

    def fetch(i):
        part = i // steps
        owner = core + part - 2 * core * part
        col = core * (steps * nc) + lax.rem(i, steps) * nc
        slot = lax.rem(i, bufs)
        return pltpu.make_async_copy(
            wo_hbm.at[pl.ds(pl.multiple_of(owner * span, span), span), pl.ds(pl.multiple_of(col, nc), nc)],
            w_v.at[slot], w_sem.at[slot])

    own = [pltpu.make_async_copy(h, own_v.at[:, pl.ds(k * wide, wide)], o_sem.at[k])
           for k, h in enumerate((oa_hbm, ob_hbm))]
    fetch(0).start()
    for c in own:
        c.start()
    fetch(1).start()

    barrier = pltpu.get_barrier_semaphore()
    pl.semaphore_signal(barrier, inc=1, device_id={"sp": sib}, device_id_type=MESH)
    pl.semaphore_wait(barrier, 1)
    swap = [pltpu.make_async_remote_copy(
        src_ref=h, dst_ref=sib_v.at[:, pl.ds(k * wide, wide)],
        send_sem=swap_send.at[k], recv_sem=swap_recv.at[k], device_id={"sp": sib}, device_id_type=MESH)
        for k, h in enumerate((oa_hbm, ob_hbm))]
    for c in own:
        c.wait()
    for c in swap:
        c.start()

    def own_half(i, carry):
        fetch(i).wait()
        fetch(i + 2).start()
        acc_v[i] = jnp.dot(own_v[...], w_v[lax.rem(i, bufs)], preferred_element_type=F32)
        return carry

    lax.fori_loop(0, steps, own_half, 0)
    for c in swap:
        c.wait()

    def store(n):
        slot = lax.rem(n, 2)
        cols = pl.ds(pl.multiple_of(core * (steps * nc) + n * nc, nc), nc)
        keep = pltpu.make_async_copy(out_v.at[slot, pl.ds(pl.multiple_of(core * rows, rows), rows)],
                                     out_hbm.at[:, cols], out_sem.at[slot])
        give = pltpu.make_async_remote_copy(
            src_ref=out_v.at[slot, pl.ds(pl.multiple_of((1 - core) * rows, rows), rows)], dst_ref=out_hbm.at[:, cols],
            send_sem=res_send.at[n], recv_sem=res_recv.at[n], device_id={"sp": sib}, device_id_type=MESH)
        return keep, give

    def sib_half(n, carry):
        i = n + steps
        fetch(i).wait()

        @pl.when(i + 2 < 2 * steps)
        def _():
            fetch(i + 2).start()

        @pl.when(n >= 2)
        def _():
            keep, give = store(n - 2)
            keep.wait()
            give.wait_send()

        out_v[lax.rem(n, 2)] = (acc_v[n] + jnp.dot(sib_v[...], w_v[lax.rem(i, bufs)], preferred_element_type=F32)).astype(BF16)
        for c in store(n):
            c.start()
        return carry

    lax.fori_loop(0, steps, sib_half, 0)
    for n in range(steps - 2, steps):
        keep, give = store(n)
        keep.wait()
        give.wait_send()
    for n in range(steps):
        store(n)[1].wait_recv()


def solution(mesh):
    ranks = mesh.shape["sp"]
    tok_spec = P(("dp", "sp"))
    rows_spec = P(("dp", "sp"), None)
    replicated = P()

    def local_step(tok_in, tok_pos, w_dq, g_q, w_uq, w_dkv, g_kv, w_uk, w_uv, w_o):
        rows, model = tok_in.shape
        num_heads = w_uq.shape[1]
        qk_dim = w_uq.shape[2]
        q_rank = w_dq.shape[1]
        kv_rank = g_kv.shape[0]
        rot = w_dkv.shape[1] - kv_rank
        nope = qk_dim - rot
        v_dim = w_uv.shape[2]
        seq = rows * ranks
        half = rot // 2
        mine = num_heads // 2
        pe_w = 128
        attn_scale = (0.1 * math.log(YARN_FACTOR) + 1.0) ** 2 / math.sqrt(qk_dim)
        angles = rope_freqs(rot)[:, None] * tok_pos.astype(F32)[None, :]
        cos_t, sin_t = jnp.cos(angles), jnp.sin(angles)

        kchunks, nq, depth = 4, 3, 64
        kv_w = kv_rank + pe_w
        any_spec = pl.BlockSpec(memory_space=pl.ANY)
        vmem_spec = pl.BlockSpec(memory_space=pltpu.VMEM)
        dma = pltpu.SemaphoreType.DMA
        kv_all, cq_all, tab_all, wk2, wv2 = pl.pallas_call(
            functools.partial(front_kernel, ranks, mine),
            out_shape=(
                jax.ShapeDtypeStruct((seq, kv_w), BF16),
                jax.ShapeDtypeStruct((2 * rows, q_rank), BF16),
                jax.ShapeDtypeStruct((2, rot, rows), F32),
                jax.ShapeDtypeStruct((kv_rank, mine * nope), BF16),
                jax.ShapeDtypeStruct((kv_rank, mine * v_dim), BF16),
            ),
            in_specs=[any_spec] * 5 + [vmem_spec] * 4,
            out_specs=(any_spec,) * 5,
            scratch_shapes=[
                pltpu.VMEM((rows, model), BF16),
                pltpu.VMEM((kchunks, kv_rank + rot, model // kchunks), BF16),
                pltpu.VMEM((nq, model, q_rank // nq), BF16),
                pltpu.VMEM((2, kv_rank, mine, nope), BF16),
                pltpu.VMEM((2, kv_rank, mine * nope), BF16),
                pltpu.VMEM((mine // 8, depth * 8, nope), F32),
                pltpu.VMEM((rows, q_rank), F32),
                pltpu.VMEM((rows, kv_w), BF16),
                pltpu.VMEM((rows, q_rank), BF16),
                pltpu.VMEM((rot, rows), F32),
                dma((2 * kchunks + nq + 2,)),
                dma((5,)),
                dma((8,)),
                dma((8,)),
                dma((2,)),
                dma((2,)),
            ],
            compiler_params=pltpu.CompilerParams(collective_id=0, has_side_effects=True, vmem_limit_bytes=60 << 20),
            cost_estimate=pl.CostEstimate(flops=2 * rows * model * (q_rank + kv_rank + rot), bytes_accessed=2 * model * (q_rank + kv_rank + rot), transcendentals=0),
        )(tok_in, w_dkv.T, w_dq, w_uk, w_uv, g_q, g_kv, cos_t, sin_t)

        wuq_t = jnp.transpose(w_uq, (1, 2, 0))
        qn = 2 * rows
        nblk = seq // qn
        steps = mine // 4
        last = steps - 1

        def whole(shape):
            return pl.BlockSpec(shape, lambda i: (0,) * len(shape))

        def up_spec(part):
            return pl.BlockSpec((2, qk_dim, q_rank), lambda i: (lax.rem(lax.axis_index("sp"), 2) * (mine // 2) + part * steps + jnp.minimum(i, last), 0, 0))

        def lat_spec(part):
            return pl.BlockSpec((kv_rank, 2 * nope), lambda i: (0, part * steps + jnp.minimum(i, last)))

        head_v = pltpu.VMEM((2, nblk, v_dim, qn), BF16)
        scores = pltpu.VMEM((2, nblk, qn, qn), F32)
        stat = pltpu.VMEM((2, 8, qn), F32)
        head_o = pltpu.VMEM((2, v_dim, qn), F32)
        o_a, o_b, cache_kv, cache_pe = pl.pallas_call(
            functools.partial(attn_kernel, attn_scale * math.log2(math.e), steps),
            out_shape=(jax.ShapeDtypeStruct((qn, 2 * steps * v_dim), BF16),) * 2 + (
                jax.ShapeDtypeStruct((rows, kv_rank), BF16),
                jax.ShapeDtypeStruct((rows, rot), BF16),
            ),
            grid=(steps + 1,),
            in_specs=[
                whole((qn, q_rank)),
                whole((seq, kv_w)),
                whole((2, rot, rows)),
                up_spec(0), up_spec(1), lat_spec(0), lat_spec(1), lat_spec(0), lat_spec(1),
            ],
            out_specs=(pl.BlockSpec((qn, 2 * v_dim), lambda i: (0, jnp.maximum(i - 1, 0))),) * 2 + (
                whole((rows, kv_rank)), whole((rows, rot))),
            scratch_shapes=[pltpu.VMEM((2, nblk, qn, nope + pe_w), BF16), head_v, head_v, pltpu.VMEM((2, nope + pe_w, qn), BF16),
                            scores, scores, stat, stat, stat, stat, head_o, head_o,
                            pltpu.VMEM((half, qn), F32), pltpu.VMEM((half, qn), F32)],
            compiler_params=pltpu.CompilerParams(dimension_semantics=("arbitrary",), vmem_limit_bytes=60 << 20),
        )(cq_all, kv_all, tab_all, wuq_t, wuq_t, wk2, wk2, wv2, wv2)

        nc, bufs = 512, 3
        span = mine * v_dim
        pieces = model // 2 // nc
        attn_out = pl.pallas_call(
            out_kernel,
            out_shape=jax.ShapeDtypeStruct((rows, model), BF16),
            in_specs=[any_spec] * 3,
            out_specs=any_spec,
            scratch_shapes=[
                pltpu.VMEM((qn, span), BF16),
                pltpu.VMEM((qn, span), BF16),
                pltpu.VMEM((bufs, span, nc), BF16),
                pltpu.VMEM((pieces, qn, nc), F32),
                pltpu.VMEM((2, qn, nc), BF16),
                dma((2,)),
                dma((bufs,)),
                dma((2,)),
                dma((2,)),
                dma((2,)),
                dma((pieces,)),
                dma((pieces,)),
            ],
            compiler_params=pltpu.CompilerParams(collective_id=1, has_side_effects=True, vmem_limit_bytes=60 << 20),
        )(o_a, o_b, w_o.reshape(num_heads * v_dim, model))
        return attn_out, cache_kv, cache_pe

    return jax.shard_map(local_step, mesh=mesh,
                         in_specs=(rows_spec, tok_spec) + (replicated,) * 8,
                         out_specs=(rows_spec, rows_spec, rows_spec), check_vma=False)
```

```python
import functools
import math

import jax
import jax.numpy as jnp
from jax import lax
from jax.experimental import pallas as pl
from jax.experimental.pallas import tpu as pltpu
from jax.sharding import PartitionSpec as P

ROPE_THETA = 10000.0
YARN_FACTOR = 40.0
ORIG_CTX = 4096.0
BETA_FAST = 32.0
BETA_SLOW = 1.0
NORM_EPS = 1e-6

MESH = pl.DeviceIdType.MESH
F32 = jnp.float32
BF16 = jnp.bfloat16
NT = (((1,), (1,)), ((), ()))
TT = (((0,), (1,)), ((), ()))


def rope_freqs(rot_dim):
    half_dim = rot_dim // 2
    log_base = 2.0 * math.log(ROPE_THETA)
    low_idx = max(math.floor(rot_dim * math.log(ORIG_CTX / (BETA_FAST * 2.0 * math.pi)) / log_base), 0)
    high_idx = min(math.ceil(rot_dim * math.log(ORIG_CTX / (BETA_SLOW * 2.0 * math.pi)) / log_base), half_dim - 1)
    spread = max(high_idx - low_idx, 0.001)
    freq_list = []
    for freq_idx in range(half_dim):
        base_freq = ROPE_THETA ** (-2.0 * freq_idx / rot_dim)
        ramp_val = min(max((freq_idx - low_idx) / spread, 0.0), 1.0)
        freq_list.append(base_freq / YARN_FACTOR * ramp_val + base_freq * (1.0 - ramp_val))
    return jnp.asarray(freq_list, dtype=jnp.float32)


def front_kernel(ranks, heads, x_hbm, wkv_hbm, wq_hbm, wuk_hbm, wuv_hbm, gq_ref, gkv_ref, cos_ref, sin_ref,
                 kv_all, cq_all, tab_all, wk_out, wv_out,
                 x_v, wkv_v, wq_v, wu_v, wo_v, wide_v, cq_f, kv_v, cq_v, tab_v,
                 w_sem, own_sem, kv_send, kv_recv, pair_send, pair_recv):
    me = lax.axis_index("sp")
    core = lax.rem(me, 2)
    sib = me + 1 - 2 * core
    rows = x_v.shape[0]
    half = cos_ref.shape[0]
    kv_rank = gkv_ref.shape[0]
    right = lax.rem(me + 2, ranks)
    left = lax.rem(me + ranks - 2, ranks)
    across = lax.rem(me + 4, ranks)

    kchunks, nq = wkv_v.shape[0], wq_v.shape[0]
    kc = wkv_v.shape[2]
    nc = wq_v.shape[2]
    first = core * heads
    loads = []
    for k in range(kchunks):
        cols = pl.ds(k * kc, kc)
        loads.append([pltpu.make_async_copy(x_hbm.at[:, cols], x_v.at[:, cols], w_sem.at[2 * k]),
                      pltpu.make_async_copy(wkv_hbm.at[:, cols], wkv_v.at[k], w_sem.at[2 * k + 1])])
    base = 2 * kchunks
    loads += [[pltpu.make_async_copy(wq_hbm.at[:, pl.ds(k * nc, nc)], wq_v.at[k], w_sem.at[base + k])] for k in range(nq)]
    loads += [[pltpu.make_async_copy(h.at[:, pl.ds(first, heads), :], wu_v.at[k], w_sem.at[base + nq + k])]
              for k, h in enumerate((wuk_hbm, wuv_hbm))]
    ahead = 3

    def launch(i):
        if i < len(loads):
            for c in loads[i]:
                c.start()

    def arrive(i):
        for c in loads[i]:
            c.wait()
        launch(i + ahead)

    for i in range(ahead):
        launch(i)

    barrier = pltpu.get_barrier_semaphore()
    for peer in (sib, right, left):
        pl.semaphore_signal(barrier, inc=1, device_id={"sp": peer}, device_id_type=MESH)

    def block(idx, start=0, size=None):
        return kv_all.at[pl.ds(idx * rows + start, size or rows)]

    def remote(src, dst, send, recv, dev):
        return pltpu.make_async_remote_copy(src_ref=src, dst_ref=dst, send_sem=send, recv_sem=recv,
                                            device_id={"sp": dev}, device_id_type=MESH)

    acc = None
    for k in range(kchunks):
        arrive(k)
        part = lax.dot_general(x_v[:, k * kc:(k + 1) * kc], wkv_v[k], NT, preferred_element_type=F32)
        acc = part if acc is None else acc + part
    a = acc[:, :kv_rank]
    inv = lax.rsqrt(jnp.mean(a * a, axis=-1, keepdims=True) + NORM_EPS)
    ckv = (a * inv * gkv_ref[...][None, :]).astype(BF16)
    tab_v[:half, :] = cos_ref[...]
    tab_v[half:, :] = sin_ref[...]
    tab = tab_v[...].T
    cos_t, sin_t = tab[:, :half], tab[:, half:]
    z1 = acc[:, kv_rank:kv_rank + half]
    z2 = acc[:, kv_rank + half:]
    pe = jnp.concatenate([z1 * cos_t - z2 * sin_t, z2 * cos_t + z1 * sin_t], axis=-1).astype(BF16)
    kv_v[:, :kv_rank] = ckv
    kv_v[:, kv_rank:] = jnp.concatenate([pe, jnp.zeros((rows, kv_v.shape[1] - kv_rank - 2 * half), BF16)], axis=-1)

    pl.semaphore_wait(barrier, 3)
    to_sib = remote(kv_v, block(me), kv_send.at[0], kv_recv.at[0], sib)
    to_right = remote(kv_v, block(me), kv_send.at[1], kv_recv.at[1], right)
    to_left = remote(kv_v, block(me), kv_send.at[2], kv_recv.at[2], left)
    tab_copy = remote(tab_v, tab_all.at[core], pair_send.at[0], pair_recv.at[0], sib)
    for c in (to_right, to_left, to_sib, tab_copy):
        c.start()
    own = [pltpu.make_async_copy(kv_v, block(me), own_sem.at[0]),
           pltpu.make_async_copy(tab_v, tab_all.at[core], own_sem.at[1])]
    for c in own:
        c.start()

    ssq = jnp.zeros((rows, 1), F32)
    for k in range(nq):
        arrive(kchunks + k)
        q = jnp.dot(x_v[...], wq_v[k], preferred_element_type=F32)
        cq_f[:, k * nc:(k + 1) * nc] = q
        ssq = ssq + jnp.sum(q * q, axis=-1, keepdims=True)
    inv_q = lax.rsqrt(ssq / cq_f.shape[1] + NORM_EPS)
    cq_v[...] = (cq_f[...] * inv_q * gq_ref[...][None, :]).astype(BF16)
    cq_copy = remote(cq_v, cq_all.at[pl.ds(core * rows, rows)], pair_send.at[1], pair_recv.at[1], sib)
    cq_copy.start()
    own.append(pltpu.make_async_copy(cq_v, cq_all.at[pl.ds(core * rows, rows)], own_sem.at[2]))
    own[-1].start()

    mid = rows // 2
    to_right.wait_recv()
    half_right = remote(block(left, 0, mid), block(left, 0, mid), kv_send.at[3], kv_recv.at[3], right)
    half_right.start()
    sib_left = remote(block(left), block(left), kv_send.at[5], kv_recv.at[5], sib)
    sib_left.start()
    to_left.wait_recv()
    half_left = remote(block(right, mid, mid), block(right, mid, mid), kv_send.at[4], kv_recv.at[4], left)
    half_left.start()
    sib_right = remote(block(right), block(right), kv_send.at[6], kv_recv.at[6], sib)
    sib_right.start()

    depth = wide_v.shape[1] // 8
    groups = wide_v.shape[0]
    width = wide_v.shape[2]
    for t, out in enumerate((wk_out, wv_out)):
        arrive(kchunks + nq + t)

        def relayout(i, _, t=t):
            base = pl.multiple_of(i * depth, depth)
            for g in range(groups):
                wide_v[g] = wu_v[t, pl.ds(base, depth), g * 8:(g + 1) * 8, :].astype(F32).reshape(depth * 8, width)
            for g in range(groups):
                for h in range(8):
                    col = (g * 8 + h) * width
                    wo_v[t, pl.ds(base, depth), col:col + width] = wide_v[g, pl.ds(h, depth, stride=8), :].astype(BF16)
            return _

        lax.fori_loop(0, wu_v.shape[1] // depth, relayout, 0)
        own.append(pltpu.make_async_copy(wo_v.at[t], out, own_sem.at[3 + t]))
        own[-1].start()

    half_right.wait_recv()
    half_left.wait_recv()
    sib_across = remote(block(across), block(across), kv_send.at[7], kv_recv.at[7], sib)
    sib_across.start()
    to_sib.wait()
    to_right.wait_send()
    to_left.wait_send()
    half_right.wait_send()
    half_left.wait_send()
    for c in (sib_left, sib_right, sib_across, tab_copy, cq_copy):
        c.wait()
    for c in own:
        c.wait()


def attn_kernel(scale2, steps, cq_ref, kv_ref, tab_ref,
                wqa_ref, wqb_ref, wka_ref, wkb_ref, wva_ref, wvb_ref, oa_ref, ob_ref, ckv_ref, cpe_ref,
                k_v, v_a, v_b, q_v, s_a, s_b, m_a, m_b, l_a, l_b, o_a, o_b, cosq_ref, sinq_ref):
    step = pl.program_id(0)
    me = lax.axis_index("sp")
    full = me // 2
    _, blocks, blk, kdim = k_v.shape
    kv_rank = wka_ref.shape[0]
    nope = wka_ref.shape[1] // 2
    half = cosq_ref.shape[0]
    rot = 2 * half
    sub = blk // 2
    everything = slice(None)

    @pl.when(step == 0)
    def _():
        for kb in range(blocks):
            pe = kv_ref[kb * blk:(kb + 1) * blk, kv_rank:]
            k_v[0, kb, :, nope:] = pe
            k_v[1, kb, :, nope:] = pe
        q_v[:, nope + rot:, :] = jnp.zeros((2, kdim - nope - rot, blk), BF16)
        for c in range(2):
            cosq_ref[:, c * sub:(c + 1) * sub] = tab_ref[c, :half, :]
            sinq_ref[:, c * sub:(c + 1) * sub] = tab_ref[c, half:, :]
        rows = ckv_ref.shape[0]
        own = kv_ref[pl.ds(pl.multiple_of(me * rows, rows), rows), :]
        ckv_ref[...] = own[:, :kv_rank]
        cpe_ref[...] = own[:, kv_rank:kv_rank + rot]

    def q_proj(w_ref):
        w = jnp.concatenate([w_ref[0], w_ref[1]], axis=0)
        both = lax.dot_general(w, cq_ref[...], NT, preferred_element_type=F32)
        for h in range(2):
            u = both[h * (nope + rot):(h + 1) * (nope + rot)]
            q_v[h, :nope, :] = u[:nope].astype(BF16)
            z1 = u[nope:nope + half]
            z2 = u[nope + half:]
            q_v[h, nope:nope + half, :] = (z1 * cosq_ref[...] - z2 * sinq_ref[...]).astype(BF16)
            q_v[h, nope + half:nope + rot, :] = (z2 * cosq_ref[...] + z1 * sinq_ref[...]).astype(BF16)

    def kv_proj(kb, wk, wv, v_ref):
        c = kv_ref[pl.ds(pl.multiple_of(kb * blk, blk), blk), :kv_rank]
        k = jnp.dot(c, wk, preferred_element_type=F32).astype(BF16)
        v = lax.dot_general(wv, c, NT, preferred_element_type=F32).astype(BF16)
        for h in range(2):
            k_v[h, kb, :, :nope] = k[:, h * nope:(h + 1) * nope]
            v_ref[h, kb] = v[h * nope:(h + 1) * nope]

    def fold_max(m_ref, h, s, cols):
        t = jnp.max(s.reshape(s.shape[0] // 8, 8, s.shape[1]), axis=0)
        m_ref[h, :, cols] = jnp.maximum(m_ref[h, :, cols], t)

    def qk(h, kb, s_ref, m_ref):
        s = jnp.dot(k_v[h, kb], q_v[h], preferred_element_type=F32)
        s_ref[h, kb] = s
        fold_max(m_ref, h, s, everything)

    def qk_diag(h, kb, s_ref, m_ref):
        s0 = jnp.dot(k_v[h, kb, :sub, :], q_v[h], preferred_element_type=F32)
        s1 = jnp.dot(k_v[h, kb, sub:, :], q_v[h, :, sub:], preferred_element_type=F32)
        keep = lax.broadcasted_iota(jnp.int32, (sub, sub), 0) <= lax.broadcasted_iota(jnp.int32, (sub, sub), 1)
        s00 = jnp.where(keep, s0[:, :sub], -jnp.inf)
        s1 = jnp.where(keep, s1, -jnp.inf)
        s01 = s0[:, sub:]
        s_ref[h, kb, :sub, :sub] = s00
        s_ref[h, kb, :sub, sub:] = s01
        s_ref[h, kb, sub:, sub:] = s1
        fold_max(m_ref, h, s00, slice(0, sub))
        fold_max(m_ref, h, s01, slice(sub, blk))
        fold_max(m_ref, h, s1, slice(sub, blk))

    def fold_sum(l_ref, h, p, cols):
        l_ref[h, :, cols] += jnp.sum(p.reshape(p.shape[0] // 8, 8, p.shape[1]), axis=0)

    def top(m_ref):
        return [jnp.max(m_ref[h], axis=0, keepdims=True) for h in range(2)]

    def pv(h, kb, v_ref, s_ref, m, l_ref, o_ref):
        p = jnp.exp2((s_ref[h, kb] - m[h]) * scale2)
        fold_sum(l_ref, h, p, everything)
        o_ref[h] += jnp.dot(v_ref[h, kb], p.astype(BF16), preferred_element_type=F32)

    def pv_diag(h, kb, v_ref, s_ref, m, l_ref, o_ref):
        p0 = jnp.exp2((s_ref[h, kb, :sub, :] - m[h]) * scale2)
        p1 = jnp.exp2((s_ref[h, kb, sub:, sub:] - m[h][:, sub:]) * scale2)
        fold_sum(l_ref, h, p0, everything)
        fold_sum(l_ref, h, p1, slice(sub, blk))
        p0 = p0.astype(BF16)
        o_ref[h] += jnp.dot(v_ref[h, kb, :, :sub], p0, preferred_element_type=F32)
        o_ref[h, :, sub:] += jnp.dot(v_ref[h, kb, :, sub:], p1.astype(BF16), preferred_element_type=F32)

    def finish(l_ref, o_ref, out_ref):
        for h in range(2):
            l = jnp.sum(l_ref[h], axis=0, keepdims=True)
            out_ref[:, h * nope:(h + 1) * nope] = (o_ref[h] / l).T.astype(BF16)

    def clear(l_ref, o_ref):
        l_ref[...] = jnp.zeros_like(l_ref)
        o_ref[...] = jnp.zeros_like(o_ref)

    def stage(wq_ref, wk_ref, wv_ref, new, old, done, done_out):
        s_n, m_n, v_n = new
        s_o, m_o, v_o, l_o, out_o = old
        m = top(m_o)
        q_proj(wq_ref)
        finish(done[0], done[1], done_out)
        clear(l_o, out_o)
        m_n[...] = jnp.full_like(m_n, -jnp.inf)
        wk = wk_ref[...]
        wv = wv_ref[...].T

        def body(kb, carry):
            kv_proj(kb, wk, wv, v_n)
            for h in range(2):
                pv(h, kb, v_o, s_o, m, l_o, out_o)
                qk(h, kb, s_n, m_n)
            return carry

        lax.fori_loop(0, full, body, 0)
        kv_proj(full, wk, wv, v_n)
        for h in range(2):
            pv_diag(h, full, v_o, s_o, m, l_o, out_o)
            qk_diag(h, full, s_n, m_n)

    @pl.when(step < steps)
    def _():
        stage(wqa_ref, wka_ref, wva_ref, (s_a, m_a, v_a), (s_b, m_b, v_b, l_b, o_b), (l_a, o_a), oa_ref)
        stage(wqb_ref, wkb_ref, wvb_ref, (s_b, m_b, v_b), (s_a, m_a, v_a, l_a, o_a), (l_b, o_b), ob_ref)

    @pl.when(step == steps)
    def _():
        m = top(m_b)
        clear(l_b, o_b)
        finish(l_a, o_a, oa_ref)

        def body(kb, carry):
            for h in range(2):
                pv(h, kb, v_b, s_b, m, l_b, o_b)
            return carry

        lax.fori_loop(0, full, body, 0)
        for h in range(2):
            pv_diag(h, full, v_b, s_b, m, l_b, o_b)
        finish(l_b, o_b, ob_ref)


def out_kernel(oa_hbm, ob_hbm, wo_hbm, res_v, own_v, sib_v, w_v, acc_v, out_v,
               o_sem, w_sem, swap_send, swap_recv, res_send, res_recv):
    me = lax.axis_index("sp")
    core = lax.rem(me, 2)
    sib = me + 1 - 2 * core
    wide = oa_hbm.shape[1]
    span = own_v.shape[1]
    rows = res_v.shape[0]
    bufs, _, nc = w_v.shape
    steps = acc_v.shape[0]

    def fetch(i):
        part = i // steps
        owner = core + part - 2 * core * part
        col = core * (steps * nc) + lax.rem(i, steps) * nc
        slot = lax.rem(i, bufs)
        return pltpu.make_async_copy(
            wo_hbm.at[pl.ds(pl.multiple_of(owner * span, span), span), pl.ds(pl.multiple_of(col, nc), nc)],
            w_v.at[slot], w_sem.at[slot])

    own = [pltpu.make_async_copy(h, own_v.at[:, pl.ds(k * wide, wide)], o_sem.at[k])
           for k, h in enumerate((oa_hbm, ob_hbm))]
    fetch(0).start()
    for c in own:
        c.start()
    fetch(1).start()

    barrier = pltpu.get_barrier_semaphore()
    pl.semaphore_signal(barrier, inc=1, device_id={"sp": sib}, device_id_type=MESH)
    pl.semaphore_wait(barrier, 1)
    swap = [pltpu.make_async_remote_copy(
        src_ref=h, dst_ref=sib_v.at[:, pl.ds(k * wide, wide)],
        send_sem=swap_send.at[k], recv_sem=swap_recv.at[k], device_id={"sp": sib}, device_id_type=MESH)
        for k, h in enumerate((oa_hbm, ob_hbm))]
    for c in own:
        c.wait()
    for c in swap:
        c.start()

    def own_half(i, carry):
        fetch(i).wait()
        fetch(i + 2).start()
        acc_v[i] = jnp.dot(own_v[...], w_v[lax.rem(i, bufs)], preferred_element_type=F32)
        return carry

    lax.fori_loop(0, steps, own_half, 0)
    for c in swap:
        c.wait()

    def cols(n):
        return pl.ds(pl.multiple_of(core * (steps * nc) + n * nc, nc), nc)

    def give(n):
        return pltpu.make_async_remote_copy(
            src_ref=out_v.at[lax.rem(n, 2), pl.ds(pl.multiple_of((1 - core) * rows, rows), rows)], dst_ref=res_v.at[:, cols(n)],
            send_sem=res_send.at[n], recv_sem=res_recv.at[n], device_id={"sp": sib}, device_id_type=MESH)

    def sib_half(n, carry):
        i = n + steps
        slot = lax.rem(n, 2)
        fetch(i).wait()

        @pl.when(i + 2 < 2 * steps)
        def _():
            fetch(i + 2).start()

        @pl.when(n >= 2)
        def _():
            give(n - 2).wait_send()

        out_v[slot] = (acc_v[n] + jnp.dot(sib_v[...], w_v[lax.rem(i, bufs)], preferred_element_type=F32)).astype(BF16)
        give(n).start()
        res_v[:, cols(n)] = out_v[slot, pl.ds(pl.multiple_of(core * rows, rows), rows), :]
        return carry

    lax.fori_loop(0, steps, sib_half, 0)
    for n in range(steps - 2, steps):
        give(n).wait_send()
    for n in range(steps):
        give(n).wait_recv()


def solution(mesh):
    ranks = mesh.shape["sp"]
    tok_spec = P(("dp", "sp"))
    rows_spec = P(("dp", "sp"), None)
    replicated = P()

    def local_step(tok_in, tok_pos, w_dq, g_q, w_uq, w_dkv, g_kv, w_uk, w_uv, w_o):
        rows, model = tok_in.shape
        num_heads = w_uq.shape[1]
        qk_dim = w_uq.shape[2]
        q_rank = w_dq.shape[1]
        kv_rank = g_kv.shape[0]
        rot = w_dkv.shape[1] - kv_rank
        nope = qk_dim - rot
        v_dim = w_uv.shape[2]
        seq = rows * ranks
        half = rot // 2
        mine = num_heads // 2
        pe_w = 128
        attn_scale = (0.1 * math.log(YARN_FACTOR) + 1.0) ** 2 / math.sqrt(qk_dim)
        angles = rope_freqs(rot)[:, None] * tok_pos.astype(F32)[None, :]
        cos_t, sin_t = jnp.cos(angles), jnp.sin(angles)

        kchunks, nq, depth = 4, 3, 64
        kv_w = kv_rank + pe_w
        any_spec = pl.BlockSpec(memory_space=pl.ANY)
        vmem_spec = pl.BlockSpec(memory_space=pltpu.VMEM)
        dma = pltpu.SemaphoreType.DMA
        kv_all, cq_all, tab_all, wk2, wv2 = pl.pallas_call(
            functools.partial(front_kernel, ranks, mine),
            out_shape=(
                jax.ShapeDtypeStruct((seq, kv_w), BF16),
                jax.ShapeDtypeStruct((2 * rows, q_rank), BF16),
                jax.ShapeDtypeStruct((2, rot, rows), F32),
                jax.ShapeDtypeStruct((kv_rank, mine * nope), BF16),
                jax.ShapeDtypeStruct((kv_rank, mine * v_dim), BF16),
            ),
            in_specs=[any_spec] * 5 + [vmem_spec] * 4,
            out_specs=(any_spec,) * 5,
            scratch_shapes=[
                pltpu.VMEM((rows, model), BF16),
                pltpu.VMEM((kchunks, kv_rank + rot, model // kchunks), BF16),
                pltpu.VMEM((nq, model, q_rank // nq), BF16),
                pltpu.VMEM((2, kv_rank, mine, nope), BF16),
                pltpu.VMEM((2, kv_rank, mine * nope), BF16),
                pltpu.VMEM((mine // 8, depth * 8, nope), F32),
                pltpu.VMEM((rows, q_rank), F32),
                pltpu.VMEM((rows, kv_w), BF16),
                pltpu.VMEM((rows, q_rank), BF16),
                pltpu.VMEM((rot, rows), F32),
                dma((2 * kchunks + nq + 2,)),
                dma((5,)),
                dma((8,)),
                dma((8,)),
                dma((2,)),
                dma((2,)),
            ],
            compiler_params=pltpu.CompilerParams(collective_id=0, has_side_effects=True, vmem_limit_bytes=60 << 20),
            cost_estimate=pl.CostEstimate(flops=2 * rows * model * (q_rank + kv_rank + rot), bytes_accessed=2 * model * (q_rank + kv_rank + rot), transcendentals=0),
        )(tok_in, w_dkv.T, w_dq, w_uk, w_uv, g_q, g_kv, cos_t, sin_t)

        wuq_t = jnp.transpose(w_uq, (1, 2, 0))
        qn = 2 * rows
        nblk = seq // qn
        steps = mine // 4
        last = steps - 1

        def whole(shape):
            return pl.BlockSpec(shape, lambda i: (0,) * len(shape))

        def up_spec(part):
            return pl.BlockSpec((2, qk_dim, q_rank), lambda i: (lax.rem(lax.axis_index("sp"), 2) * (mine // 2) + part * steps + jnp.minimum(i, last), 0, 0))

        def lat_spec(part):
            return pl.BlockSpec((kv_rank, 2 * nope), lambda i: (0, part * steps + jnp.minimum(i, last)))

        head_v = pltpu.VMEM((2, nblk, v_dim, qn), BF16)
        scores = pltpu.VMEM((2, nblk, qn, qn), F32)
        stat = pltpu.VMEM((2, 8, qn), F32)
        head_o = pltpu.VMEM((2, v_dim, qn), F32)
        o_a, o_b, cache_kv, cache_pe = pl.pallas_call(
            functools.partial(attn_kernel, attn_scale * math.log2(math.e), steps),
            out_shape=(jax.ShapeDtypeStruct((qn, 2 * steps * v_dim), BF16),) * 2 + (
                jax.ShapeDtypeStruct((rows, kv_rank), BF16),
                jax.ShapeDtypeStruct((rows, rot), BF16),
            ),
            grid=(steps + 1,),
            in_specs=[
                whole((qn, q_rank)),
                whole((seq, kv_w)),
                whole((2, rot, rows)),
                up_spec(0), up_spec(1), lat_spec(0), lat_spec(1), lat_spec(0), lat_spec(1),
            ],
            out_specs=(pl.BlockSpec((qn, 2 * v_dim), lambda i: (0, jnp.maximum(i - 1, 0))),) * 2 + (
                whole((rows, kv_rank)), whole((rows, rot))),
            scratch_shapes=[pltpu.VMEM((2, nblk, qn, nope + pe_w), BF16), head_v, head_v, pltpu.VMEM((2, nope + pe_w, qn), BF16),
                            scores, scores, stat, stat, stat, stat, head_o, head_o,
                            pltpu.VMEM((half, qn), F32), pltpu.VMEM((half, qn), F32)],
            compiler_params=pltpu.CompilerParams(dimension_semantics=("arbitrary",), vmem_limit_bytes=60 << 20),
        )(cq_all, kv_all, tab_all, wuq_t, wuq_t, wk2, wk2, wv2, wv2)

        nc, bufs = 512, 3
        span = mine * v_dim
        pieces = model // 2 // nc
        attn_out = pl.pallas_call(
            out_kernel,
            out_shape=jax.ShapeDtypeStruct((rows, model), BF16),
            in_specs=[any_spec] * 3,
            out_specs=vmem_spec,
            scratch_shapes=[
                pltpu.VMEM((qn, span), BF16),
                pltpu.VMEM((qn, span), BF16),
                pltpu.VMEM((bufs, span, nc), BF16),
                pltpu.VMEM((pieces, qn, nc), F32),
                pltpu.VMEM((2, qn, nc), BF16),
                dma((2,)),
                dma((bufs,)),
                dma((2,)),
                dma((2,)),
                dma((pieces,)),
                dma((pieces,)),
            ],
            compiler_params=pltpu.CompilerParams(collective_id=1, has_side_effects=True, vmem_limit_bytes=60 << 20),
        )(o_a, o_b, w_o.reshape(num_heads * v_dim, model))
        return attn_out, cache_kv, cache_pe

    return jax.shard_map(local_step, mesh=mesh,
                         in_specs=(rows_spec, tok_spec) + (replicated,) * 8,
                         out_specs=(rows_spec, rows_spec, rows_spec), check_vma=False)
```

```python
import functools
import math

import jax
import jax.numpy as jnp
from jax import lax
from jax.experimental import pallas as pl
from jax.experimental.pallas import tpu as pltpu
from jax.sharding import PartitionSpec as P

ROPE_THETA = 10000.0
YARN_FACTOR = 40.0
ORIG_CTX = 4096.0
BETA_FAST = 32.0
BETA_SLOW = 1.0
NORM_EPS = 1e-6

MESH = pl.DeviceIdType.MESH
F32 = jnp.float32
BF16 = jnp.bfloat16
NT = (((1,), (1,)), ((), ()))
TT = (((0,), (1,)), ((), ()))


def rope_freqs(rot_dim):
    half_dim = rot_dim // 2
    log_base = 2.0 * math.log(ROPE_THETA)
    low_idx = max(math.floor(rot_dim * math.log(ORIG_CTX / (BETA_FAST * 2.0 * math.pi)) / log_base), 0)
    high_idx = min(math.ceil(rot_dim * math.log(ORIG_CTX / (BETA_SLOW * 2.0 * math.pi)) / log_base), half_dim - 1)
    spread = max(high_idx - low_idx, 0.001)
    freq_list = []
    for freq_idx in range(half_dim):
        base_freq = ROPE_THETA ** (-2.0 * freq_idx / rot_dim)
        ramp_val = min(max((freq_idx - low_idx) / spread, 0.0), 1.0)
        freq_list.append(base_freq / YARN_FACTOR * ramp_val + base_freq * (1.0 - ramp_val))
    return jnp.asarray(freq_list, dtype=jnp.float32)


def front_kernel(ranks, heads, x_hbm, wkv_hbm, wq_hbm, wuk_hbm, wuv_hbm, gq_ref, gkv_ref, cos_ref, sin_ref,
                 kv_all, cq_all, tab_all, wk_out, wv_out,
                 x_v, wkv_v, wq_v, wu_v, wo_v, wide_v, cq_f, kv_v, cq_v, tab_v,
                 w_sem, own_sem, kv_send, kv_recv, pair_send, pair_recv):
    me = lax.axis_index("sp")
    core = lax.rem(me, 2)
    sib = me + 1 - 2 * core
    rows = x_v.shape[0]
    half = cos_ref.shape[0]
    kv_rank = gkv_ref.shape[0]
    right = lax.rem(me + 2, ranks)
    left = lax.rem(me + ranks - 2, ranks)
    across = lax.rem(me + 4, ranks)

    kchunks, nq = wkv_v.shape[0], wq_v.shape[0]
    kc = wkv_v.shape[2]
    nc = wq_v.shape[2]
    first = core * heads
    loads = []
    for k in range(kchunks):
        cols = pl.ds(k * kc, kc)
        loads.append([pltpu.make_async_copy(x_hbm.at[:, cols], x_v.at[:, cols], w_sem.at[2 * k]),
                      pltpu.make_async_copy(wkv_hbm.at[:, cols], wkv_v.at[k], w_sem.at[2 * k + 1])])
    base = 2 * kchunks
    loads += [[pltpu.make_async_copy(wq_hbm.at[:, pl.ds(k * nc, nc)], wq_v.at[k], w_sem.at[base + k])] for k in range(nq)]
    loads += [[pltpu.make_async_copy(h.at[:, pl.ds(first, heads), :], wu_v.at[k], w_sem.at[base + nq + k])]
              for k, h in enumerate((wuk_hbm, wuv_hbm))]
    ahead = 3

    def launch(i):
        if i < len(loads):
            for c in loads[i]:
                c.start()

    def arrive(i):
        for c in loads[i]:
            c.wait()
        launch(i + ahead)

    for i in range(ahead):
        launch(i)

    barrier = pltpu.get_barrier_semaphore()
    for peer in (sib, right, left):
        pl.semaphore_signal(barrier, inc=1, device_id={"sp": peer}, device_id_type=MESH)

    def block(idx, start=0, size=None):
        return kv_all.at[pl.ds(idx * rows + start, size or rows)]

    def remote(src, dst, send, recv, dev):
        return pltpu.make_async_remote_copy(src_ref=src, dst_ref=dst, send_sem=send, recv_sem=recv,
                                            device_id={"sp": dev}, device_id_type=MESH)

    acc = None
    for k in range(kchunks):
        arrive(k)
        part = lax.dot_general(x_v[:, k * kc:(k + 1) * kc], wkv_v[k], NT, preferred_element_type=F32)
        acc = part if acc is None else acc + part
    a = acc[:, :kv_rank]
    inv = lax.rsqrt(jnp.mean(a * a, axis=-1, keepdims=True) + NORM_EPS)
    ckv = (a * inv * gkv_ref[...][None, :]).astype(BF16)
    tab_v[:half, :] = cos_ref[...]
    tab_v[half:, :] = sin_ref[...]
    tab = tab_v[...].T
    cos_t, sin_t = tab[:, :half], tab[:, half:]
    z1 = acc[:, kv_rank:kv_rank + half]
    z2 = acc[:, kv_rank + half:]
    pe = jnp.concatenate([z1 * cos_t - z2 * sin_t, z2 * cos_t + z1 * sin_t], axis=-1).astype(BF16)
    kv_v[:, :kv_rank] = ckv
    kv_v[:, kv_rank:] = jnp.concatenate([pe, jnp.zeros((rows, kv_v.shape[1] - kv_rank - 2 * half), BF16)], axis=-1)

    pl.semaphore_wait(barrier, 3)
    to_sib = remote(kv_v, block(me), kv_send.at[0], kv_recv.at[0], sib)
    to_right = remote(kv_v, block(me), kv_send.at[1], kv_recv.at[1], right)
    to_left = remote(kv_v, block(me), kv_send.at[2], kv_recv.at[2], left)
    tab_copy = remote(tab_v, tab_all.at[core], pair_send.at[0], pair_recv.at[0], sib)
    for c in (to_right, to_left, to_sib, tab_copy):
        c.start()
    own = [pltpu.make_async_copy(kv_v, block(me), own_sem.at[0]),
           pltpu.make_async_copy(tab_v, tab_all.at[core], own_sem.at[1])]
    for c in own:
        c.start()

    ssq = jnp.zeros((rows, 1), F32)
    for k in range(nq):
        arrive(kchunks + k)
        q = jnp.dot(x_v[...], wq_v[k], preferred_element_type=F32)
        cq_f[:, k * nc:(k + 1) * nc] = q
        ssq = ssq + jnp.sum(q * q, axis=-1, keepdims=True)
    inv_q = lax.rsqrt(ssq / cq_f.shape[1] + NORM_EPS)
    cq_v[...] = (cq_f[...] * inv_q * gq_ref[...][None, :]).astype(BF16)
    cq_copy = remote(cq_v, cq_all.at[pl.ds(core * rows, rows)], pair_send.at[1], pair_recv.at[1], sib)
    cq_copy.start()
    own.append(pltpu.make_async_copy(cq_v, cq_all.at[pl.ds(core * rows, rows)], own_sem.at[2]))
    own[-1].start()

    mid = rows // 2
    to_right.wait_recv()
    half_right = remote(block(left, 0, mid), block(left, 0, mid), kv_send.at[3], kv_recv.at[3], right)
    half_right.start()
    sib_left = remote(block(left), block(left), kv_send.at[5], kv_recv.at[5], sib)
    sib_left.start()
    to_left.wait_recv()
    half_left = remote(block(right, mid, mid), block(right, mid, mid), kv_send.at[4], kv_recv.at[4], left)
    half_left.start()
    sib_right = remote(block(right), block(right), kv_send.at[6], kv_recv.at[6], sib)
    sib_right.start()

    depth = wide_v.shape[1] // 8
    groups = wide_v.shape[0]
    width = wide_v.shape[2]
    for t, out in enumerate((wk_out, wv_out)):
        arrive(kchunks + nq + t)

        def relayout(i, _, t=t):
            base = pl.multiple_of(i * depth, depth)
            for g in range(groups):
                wide_v[g] = wu_v[t, pl.ds(base, depth), g * 8:(g + 1) * 8, :].astype(F32).reshape(depth * 8, width)
            for g in range(groups):
                for h in range(8):
                    col = (g * 8 + h) * width
                    wo_v[t, pl.ds(base, depth), col:col + width] = wide_v[g, pl.ds(h, depth, stride=8), :].astype(BF16)
            return _

        lax.fori_loop(0, wu_v.shape[1] // depth, relayout, 0)
        own.append(pltpu.make_async_copy(wo_v.at[t], out, own_sem.at[3 + t]))
        own[-1].start()

    half_right.wait_recv()
    half_left.wait_recv()
    sib_across = remote(block(across), block(across), kv_send.at[7], kv_recv.at[7], sib)
    sib_across.start()
    to_sib.wait()
    to_right.wait_send()
    to_left.wait_send()
    half_right.wait_send()
    half_left.wait_send()
    for c in (sib_left, sib_right, sib_across, tab_copy, cq_copy):
        c.wait()
    for c in own:
        c.wait()


def shares(me, ranks, steps):
    chips = ranks // 2
    chip = me // 2
    give = jnp.maximum(chip - chips // 2 + 1, 0)
    take = jnp.maximum(chips // 2 - chip, 0)
    return chip, steps - give, take, give


def weight_step(i, ranks, steps):
    _, n_loc, n_rem, _ = shares(lax.axis_index("sp"), ranks, steps)
    own = jnp.minimum(i, n_loc - 1)
    far = steps - n_rem + jnp.minimum(i - n_loc - 1, n_rem - 1)
    return jnp.where((i <= n_loc) | (n_rem == 0), own, far)


def attn_kernel(scale2, ranks, steps, cq_hbm, kv_ref, tab_ref,
                wqa_ref, wqb_ref, wka_ref, wkb_ref, wva_ref, wvb_ref, oa_hbm, ob_hbm, ckv_ref, cpe_ref,
                cq_v, tab_v, k_v, v_a, v_b, q_v, s_a, s_b, m_a, m_b, l_a, l_b, o_a, o_b, cosq_ref, sinq_ref, oa_v, ob_v,
                cq_sem, lat_send, lat_recv, fwd_send, fwd_recv, o_sem, o_send, oa_recv, ob_recv):
    step = pl.program_id(0)
    final = pl.num_programs(0) - 1
    me = lax.axis_index("sp")
    core = lax.rem(me, 2)
    sib = me + 1 - 2 * core
    chip, n_loc, n_rem, n_give = shares(me, ranks, steps)
    far_chip = ranks // 2 - 1 - chip
    far = 2 * far_chip + core
    most = oa_recv.shape[0]
    is_far = step > n_loc
    qset = jnp.where(is_far, 1, 0)
    full = jnp.where(is_far, far_chip, chip)
    _, blocks, blk, kdim = k_v.shape
    kv_rank = wka_ref.shape[0]
    nope = wka_ref.shape[1] // 2
    half = cosq_ref.shape[1]
    rot = 2 * half
    sub = blk // 2
    everything = slice(None)
    my_rows = pl.ds(pl.multiple_of(core * sub, sub), sub)

    lat = [pltpu.make_async_remote_copy(src_ref=src, dst_ref=dst, send_sem=lat_send.at[k], recv_sem=lat_recv.at[k],
                                        device_id={"sp": far}, device_id_type=MESH)
           for k, (src, dst) in enumerate(((cq_hbm.at[my_rows], cq_v.at[1, my_rows]), (tab_ref.at[core], tab_v.at[core])))]
    fwd = [pltpu.make_async_remote_copy(src_ref=ref, dst_ref=ref, send_sem=fwd_send.at[k], recv_sem=fwd_recv.at[k],
                                        device_id={"sp": sib}, device_id_type=MESH)
           for k, ref in enumerate((cq_v.at[1, my_rows], tab_v.at[core]))]

    def o_cols(at):
        return pl.ds(pl.multiple_of(at * 2 * nope, 2 * nope), 2 * nope)

    def o_local(part, at):
        src, dst = ((oa_v, oa_hbm), (ob_v, ob_hbm))[part]
        return pltpu.make_async_copy(src, dst.at[:, o_cols(at)], o_sem.at[part])

    def o_far(part, r):
        src, dst, recv = ((oa_v, oa_hbm, oa_recv), (ob_v, ob_hbm, ob_recv))[part]
        return pltpu.make_async_remote_copy(src_ref=src, dst_ref=dst.at[:, o_cols(steps - 1 - r)], send_sem=o_send.at[part], recv_sem=recv.at[r],
                                            device_id={"sp": far}, device_id_type=MESH)

    def left_own(s):
        return (s >= 1) & (s <= n_loc)

    def left_far(s):
        return (s >= n_loc + 2) & (s <= n_loc + n_rem + 1)

    def emit(part):
        @pl.when(left_own(step))
        def _():
            o_local(part, step - 1).start()

        @pl.when(left_far(step))
        def _():
            o_far(part, n_loc + n_rem + 1 - step).start()

    def settle(part, s):
        @pl.when(left_own(s))
        def _():
            o_local(part, s - 1).wait()

        @pl.when(left_far(s))
        def _():
            o_far(part, n_loc + n_rem + 1 - s).wait_send()

    @pl.when(step == 0)
    def _():
        own_cq = pltpu.make_async_copy(cq_hbm, cq_v.at[0], cq_sem.at[0])
        own_cq.start()
        barrier = pltpu.get_barrier_semaphore()
        for peer in (sib, far):
            pl.semaphore_signal(barrier, inc=1, device_id={"sp": peer}, device_id_type=MESH)
        pl.semaphore_wait(barrier, 2)

        @pl.when(n_give > 0)
        def _():
            for c in lat:
                c.start()

        for kb in range(blocks):
            pe = kv_ref[kb * blk:(kb + 1) * blk, kv_rank:]
            k_v[0, kb, :, nope:] = pe
            k_v[1, kb, :, nope:] = pe
        q_v[:, nope + rot:, :] = jnp.zeros((2, kdim - nope - rot, blk), BF16)
        for c in range(2):
            cosq_ref[0, :, c * sub:(c + 1) * sub] = tab_ref[c, :half, :]
            sinq_ref[0, :, c * sub:(c + 1) * sub] = tab_ref[c, half:, :]
        rows = ckv_ref.shape[0]
        own = kv_ref[pl.ds(pl.multiple_of(me * rows, rows), rows), :]
        ckv_ref[...] = own[:, :kv_rank]
        cpe_ref[...] = own[:, kv_rank:kv_rank + rot]
        own_cq.wait()

    @pl.when(step > 0)
    def _():
        for part in range(2):
            settle(part, step - 1)

    @pl.when((step == n_loc - 1) & (n_rem > 0))
    def _():
        for c in lat:
            c.wait_recv()
        for c in fwd:
            c.start()

    @pl.when((step == n_loc + 1) & (n_rem > 0))
    def _():
        for c in fwd:
            c.wait()
        for c in range(2):
            cosq_ref[1, :, c * sub:(c + 1) * sub] = tab_v[c, :half, :]
            sinq_ref[1, :, c * sub:(c + 1) * sub] = tab_v[c, half:, :]

    def q_proj(w_ref):
        w = jnp.concatenate([w_ref[0], w_ref[1]], axis=0)
        both = lax.dot_general(w, cq_v[qset], NT, preferred_element_type=F32)
        cos_t, sin_t = cosq_ref[qset], sinq_ref[qset]
        for h in range(2):
            u = both[h * (nope + rot):(h + 1) * (nope + rot)]
            q_v[h, :nope, :] = u[:nope].astype(BF16)
            z1 = u[nope:nope + half]
            z2 = u[nope + half:]
            q_v[h, nope:nope + half, :] = (z1 * cos_t - z2 * sin_t).astype(BF16)
            q_v[h, nope + half:nope + rot, :] = (z2 * cos_t + z1 * sin_t).astype(BF16)

    def kv_proj(kb, wk, wv, v_ref):
        c = kv_ref[pl.ds(pl.multiple_of(kb * blk, blk), blk), :kv_rank]
        k = jnp.dot(c, wk, preferred_element_type=F32).astype(BF16)
        v = lax.dot_general(wv, c, NT, preferred_element_type=F32).astype(BF16)
        for h in range(2):
            k_v[h, kb, :, :nope] = k[:, h * nope:(h + 1) * nope]
            v_ref[h, kb] = v[h * nope:(h + 1) * nope]

    def fold_max(m_ref, h, s, cols):
        t = jnp.max(s.reshape(s.shape[0] // 8, 8, s.shape[1]), axis=0)
        m_ref[h, :, cols] = jnp.maximum(m_ref[h, :, cols], t)

    def qk(h, kb, s_ref, m_ref):
        s = jnp.dot(k_v[h, kb], q_v[h], preferred_element_type=F32)
        s_ref[h, kb] = s
        fold_max(m_ref, h, s, everything)

    def qk_diag(h, kb, s_ref, m_ref):
        s0 = jnp.dot(k_v[h, kb, :sub, :], q_v[h], preferred_element_type=F32)
        s1 = jnp.dot(k_v[h, kb, sub:, :], q_v[h, :, sub:], preferred_element_type=F32)
        keep = lax.broadcasted_iota(jnp.int32, (sub, sub), 0) <= lax.broadcasted_iota(jnp.int32, (sub, sub), 1)
        s00 = jnp.where(keep, s0[:, :sub], -jnp.inf)
        s1 = jnp.where(keep, s1, -jnp.inf)
        s01 = s0[:, sub:]
        s_ref[h, kb, :sub, :sub] = s00
        s_ref[h, kb, :sub, sub:] = s01
        s_ref[h, kb, sub:, sub:] = s1
        fold_max(m_ref, h, s00, slice(0, sub))
        fold_max(m_ref, h, s01, slice(sub, blk))
        fold_max(m_ref, h, s1, slice(sub, blk))

    def fold_sum(l_ref, h, p, cols):
        l_ref[h, :, cols] += jnp.sum(p.reshape(p.shape[0] // 8, 8, p.shape[1]), axis=0)

    def top(m_ref):
        return [jnp.max(m_ref[h], axis=0, keepdims=True) for h in range(2)]

    def pv(h, kb, v_ref, s_ref, m, l_ref, o_ref):
        p = jnp.exp2((s_ref[h, kb] - m[h]) * scale2)
        fold_sum(l_ref, h, p, everything)
        o_ref[h] += jnp.dot(v_ref[h, kb], p.astype(BF16), preferred_element_type=F32)

    def pv_diag(h, kb, v_ref, s_ref, m, l_ref, o_ref):
        p0 = jnp.exp2((s_ref[h, kb, :sub, :] - m[h]) * scale2)
        p1 = jnp.exp2((s_ref[h, kb, sub:, sub:] - m[h][:, sub:]) * scale2)
        fold_sum(l_ref, h, p0, everything)
        fold_sum(l_ref, h, p1, slice(sub, blk))
        p0 = p0.astype(BF16)
        o_ref[h] += jnp.dot(v_ref[h, kb, :, :sub], p0, preferred_element_type=F32)
        o_ref[h, :, sub:] += jnp.dot(v_ref[h, kb, :, sub:], p1.astype(BF16), preferred_element_type=F32)

    def finish(l_ref, o_ref, out_ref):
        for h in range(2):
            l = jnp.sum(l_ref[h], axis=0, keepdims=True)
            out_ref[:, h * nope:(h + 1) * nope] = (o_ref[h] / l).T.astype(BF16)

    def clear(l_ref, o_ref):
        l_ref[...] = jnp.zeros_like(l_ref)
        o_ref[...] = jnp.zeros_like(o_ref)

    def stage(wq_ref, wk_ref, wv_ref, new, old, done, done_out, part):
        s_n, m_n, v_n = new
        s_o, m_o, v_o, l_o, out_o = old
        m = top(m_o)
        q_proj(wq_ref)
        finish(done[0], done[1], done_out)
        emit(part)
        clear(l_o, out_o)
        m_n[...] = jnp.full_like(m_n, -jnp.inf)
        wk = wk_ref[...]
        wv = wv_ref[...].T

        def body(kb, carry):
            kv_proj(kb, wk, wv, v_n)
            for h in range(2):
                pv(h, kb, v_o, s_o, m, l_o, out_o)
                qk(h, kb, s_n, m_n)
            return carry

        lax.fori_loop(0, full, body, 0)
        kv_proj(full, wk, wv, v_n)
        for h in range(2):
            pv_diag(h, full, v_o, s_o, m, l_o, out_o)
            qk_diag(h, full, s_n, m_n)

    @pl.when((step < n_loc) | ((step > n_loc) & (step <= n_loc + n_rem)))
    def _():
        stage(wqa_ref, wka_ref, wva_ref, (s_a, m_a, v_a), (s_b, m_b, v_b, l_b, o_b), (l_a, o_a), oa_v, 0)
        stage(wqb_ref, wkb_ref, wvb_ref, (s_b, m_b, v_b), (s_a, m_a, v_a, l_a, o_a), (l_b, o_b), ob_v, 1)

    @pl.when((step == n_loc) | ((step == n_loc + n_rem + 1) & (n_rem > 0)))
    def _():
        m = top(m_b)
        clear(l_b, o_b)
        finish(l_a, o_a, oa_v)
        emit(0)

        def body(kb, carry):
            for h in range(2):
                pv(h, kb, v_b, s_b, m, l_b, o_b)
            return carry

        lax.fori_loop(0, full, body, 0)
        for h in range(2):
            pv_diag(h, full, v_b, s_b, m, l_b, o_b)
        finish(l_b, o_b, ob_v)
        emit(1)

    @pl.when(step == final)
    def _():
        @pl.when(n_give > 0)
        def _():
            for c in lat:
                c.wait_send()

        for r in range(most):
            @pl.when(n_give > r)
            def _(r=r):
                for part in range(2):
                    o_far(part, r).wait_recv()


def out_kernel(oa_hbm, ob_hbm, wo_hbm, out_hbm, own_v, sib_v, w_v, acc_v, out_v,
               o_sem, w_sem, out_sem, swap_send, swap_recv, res_send, res_recv):
    me = lax.axis_index("sp")
    core = lax.rem(me, 2)
    sib = me + 1 - 2 * core
    wide = oa_hbm.shape[1]
    span = own_v.shape[1]
    rows = out_hbm.shape[0]
    bufs, _, nc = w_v.shape
    steps = acc_v.shape[0]

    def fetch(i):
        part = i // steps
        owner = core + part - 2 * core * part
        col = core * (steps * nc) + lax.rem(i, steps) * nc
        slot = lax.rem(i, bufs)
        return pltpu.make_async_copy(
            wo_hbm.at[pl.ds(pl.multiple_of(owner * span, span), span), pl.ds(pl.multiple_of(col, nc), nc)],
            w_v.at[slot], w_sem.at[slot])

    own = [pltpu.make_async_copy(h, own_v.at[:, pl.ds(k * wide, wide)], o_sem.at[k])
           for k, h in enumerate((oa_hbm, ob_hbm))]
    fetch(0).start()
    for c in own:
        c.start()
    fetch(1).start()

    barrier = pltpu.get_barrier_semaphore()
    pl.semaphore_signal(barrier, inc=1, device_id={"sp": sib}, device_id_type=MESH)
    pl.semaphore_wait(barrier, 1)
    swap = [pltpu.make_async_remote_copy(
        src_ref=h, dst_ref=sib_v.at[:, pl.ds(k * wide, wide)],
        send_sem=swap_send.at[k], recv_sem=swap_recv.at[k], device_id={"sp": sib}, device_id_type=MESH)
        for k, h in enumerate((oa_hbm, ob_hbm))]
    for c in own:
        c.wait()
    for c in swap:
        c.start()

    def own_half(i, carry):
        fetch(i).wait()
        fetch(i + 2).start()
        acc_v[i] = jnp.dot(own_v[...], w_v[lax.rem(i, bufs)], preferred_element_type=F32)
        return carry

    lax.fori_loop(0, steps, own_half, 0)
    for c in swap:
        c.wait()

    def store(n):
        slot = lax.rem(n, 2)
        cols = pl.ds(pl.multiple_of(core * (steps * nc) + n * nc, nc), nc)
        keep = pltpu.make_async_copy(out_v.at[slot, pl.ds(pl.multiple_of(core * rows, rows), rows)],
                                     out_hbm.at[:, cols], out_sem.at[slot])
        give = pltpu.make_async_remote_copy(
            src_ref=out_v.at[slot, pl.ds(pl.multiple_of((1 - core) * rows, rows), rows)], dst_ref=out_hbm.at[:, cols],
            send_sem=res_send.at[n], recv_sem=res_recv.at[n], device_id={"sp": sib}, device_id_type=MESH)
        return keep, give

    def sib_half(n, carry):
        i = n + steps
        fetch(i).wait()

        @pl.when(i + 2 < 2 * steps)
        def _():
            fetch(i + 2).start()

        @pl.when(n >= 2)
        def _():
            keep, give = store(n - 2)
            keep.wait()
            give.wait_send()

        out_v[lax.rem(n, 2)] = (acc_v[n] + jnp.dot(sib_v[...], w_v[lax.rem(i, bufs)], preferred_element_type=F32)).astype(BF16)
        for c in store(n):
            c.start()
        return carry

    lax.fori_loop(0, steps, sib_half, 0)
    for n in range(steps - 2, steps):
        keep, give = store(n)
        keep.wait()
        give.wait_send()
    for n in range(steps):
        store(n)[1].wait_recv()


def solution(mesh):
    ranks = mesh.shape["sp"]
    tok_spec = P(("dp", "sp"))
    rows_spec = P(("dp", "sp"), None)
    replicated = P()

    def local_step(tok_in, tok_pos, w_dq, g_q, w_uq, w_dkv, g_kv, w_uk, w_uv, w_o):
        rows, model = tok_in.shape
        num_heads = w_uq.shape[1]
        qk_dim = w_uq.shape[2]
        q_rank = w_dq.shape[1]
        kv_rank = g_kv.shape[0]
        rot = w_dkv.shape[1] - kv_rank
        nope = qk_dim - rot
        v_dim = w_uv.shape[2]
        seq = rows * ranks
        half = rot // 2
        mine = num_heads // 2
        pe_w = 128
        attn_scale = (0.1 * math.log(YARN_FACTOR) + 1.0) ** 2 / math.sqrt(qk_dim)
        angles = rope_freqs(rot)[:, None] * tok_pos.astype(F32)[None, :]
        cos_t, sin_t = jnp.cos(angles), jnp.sin(angles)

        kchunks, nq, depth = 4, 3, 64
        kv_w = kv_rank + pe_w
        any_spec = pl.BlockSpec(memory_space=pl.ANY)
        vmem_spec = pl.BlockSpec(memory_space=pltpu.VMEM)
        dma = pltpu.SemaphoreType.DMA
        kv_all, cq_all, tab_all, wk2, wv2 = pl.pallas_call(
            functools.partial(front_kernel, ranks, mine),
            out_shape=(
                jax.ShapeDtypeStruct((seq, kv_w), BF16),
                jax.ShapeDtypeStruct((2 * rows, q_rank), BF16),
                jax.ShapeDtypeStruct((2, rot, rows), F32),
                jax.ShapeDtypeStruct((kv_rank, mine * nope), BF16),
                jax.ShapeDtypeStruct((kv_rank, mine * v_dim), BF16),
            ),
            in_specs=[any_spec] * 5 + [vmem_spec] * 4,
            out_specs=(any_spec,) * 5,
            scratch_shapes=[
                pltpu.VMEM((rows, model), BF16),
                pltpu.VMEM((kchunks, kv_rank + rot, model // kchunks), BF16),
                pltpu.VMEM((nq, model, q_rank // nq), BF16),
                pltpu.VMEM((2, kv_rank, mine, nope), BF16),
                pltpu.VMEM((2, kv_rank, mine * nope), BF16),
                pltpu.VMEM((mine // 8, depth * 8, nope), F32),
                pltpu.VMEM((rows, q_rank), F32),
                pltpu.VMEM((rows, kv_w), BF16),
                pltpu.VMEM((rows, q_rank), BF16),
                pltpu.VMEM((rot, rows), F32),
                dma((2 * kchunks + nq + 2,)),
                dma((5,)),
                dma((8,)),
                dma((8,)),
                dma((2,)),
                dma((2,)),
            ],
            compiler_params=pltpu.CompilerParams(collective_id=0, has_side_effects=True, vmem_limit_bytes=60 << 20),
            cost_estimate=pl.CostEstimate(flops=2 * rows * model * (q_rank + kv_rank + rot), bytes_accessed=2 * model * (q_rank + kv_rank + rot), transcendentals=0),
        )(tok_in, w_dkv.T, w_dq, w_uk, w_uv, g_q, g_kv, cos_t, sin_t)

        wuq_t = jnp.transpose(w_uq, (1, 2, 0))
        qn = 2 * rows
        nblk = seq // qn
        steps = mine // 4

        def whole(shape):
            return pl.BlockSpec(shape, lambda i: (0,) * len(shape))

        def up_spec(part):
            return pl.BlockSpec((2, qk_dim, q_rank), lambda i: (lax.rem(lax.axis_index("sp"), 2) * (mine // 2) + part * steps + weight_step(i, ranks, steps), 0, 0))

        def lat_spec(part):
            return pl.BlockSpec((kv_rank, 2 * nope), lambda i: (0, part * steps + weight_step(i, ranks, steps)))

        head_v = pltpu.VMEM((2, nblk, v_dim, qn), BF16)
        scores = pltpu.VMEM((2, nblk, qn, qn), F32)
        stat = pltpu.VMEM((2, 8, qn), F32)
        head_o = pltpu.VMEM((2, v_dim, qn), F32)
        rope_v = pltpu.VMEM((2, half, qn), F32)
        pair_o = pltpu.VMEM((qn, 2 * v_dim), BF16)
        most = ranks // 4
        o_a, o_b, cache_kv, cache_pe = pl.pallas_call(
            functools.partial(attn_kernel, attn_scale * math.log2(math.e), ranks, steps),
            out_shape=(jax.ShapeDtypeStruct((qn, 2 * steps * v_dim), BF16),) * 2 + (
                jax.ShapeDtypeStruct((rows, kv_rank), BF16),
                jax.ShapeDtypeStruct((rows, rot), BF16),
            ),
            grid=(steps + most + 3,),
            in_specs=[
                any_spec,
                whole((seq, kv_w)),
                whole((2, rot, rows)),
                up_spec(0), up_spec(1), lat_spec(0), lat_spec(1), lat_spec(0), lat_spec(1),
            ],
            out_specs=(any_spec, any_spec, whole((rows, kv_rank)), whole((rows, rot))),
            scratch_shapes=[pltpu.VMEM((2, qn, q_rank), BF16), pltpu.VMEM((2, rot, rows), F32),
                            pltpu.VMEM((2, nblk, qn, nope + pe_w), BF16), head_v, head_v, pltpu.VMEM((2, nope + pe_w, qn), BF16),
                            scores, scores, stat, stat, stat, stat, head_o, head_o, rope_v, rope_v, pair_o, pair_o,
                            dma((1,)), dma((2,)), dma((2,)), dma((2,)), dma((2,)), dma((2,)), dma((2,)), dma((most,)), dma((most,))],
            compiler_params=pltpu.CompilerParams(dimension_semantics=("arbitrary",), collective_id=2, has_side_effects=True, vmem_limit_bytes=62 << 20),
        )(cq_all, kv_all, tab_all, wuq_t, wuq_t, wk2, wk2, wv2, wv2)

        nc, bufs = 512, 3
        span = mine * v_dim
        pieces = model // 2 // nc
        attn_out = pl.pallas_call(
            out_kernel,
            out_shape=jax.ShapeDtypeStruct((rows, model), BF16),
            in_specs=[any_spec] * 3,
            out_specs=any_spec,
            scratch_shapes=[
                pltpu.VMEM((qn, span), BF16),
                pltpu.VMEM((qn, span), BF16),
                pltpu.VMEM((bufs, span, nc), BF16),
                pltpu.VMEM((pieces, qn, nc), F32),
                pltpu.VMEM((2, qn, nc), BF16),
                dma((2,)),
                dma((bufs,)),
                dma((2,)),
                dma((2,)),
                dma((2,)),
                dma((pieces,)),
                dma((pieces,)),
            ],
            compiler_params=pltpu.CompilerParams(collective_id=1, has_side_effects=True, vmem_limit_bytes=60 << 20),
        )(o_a, o_b, w_o.reshape(num_heads * v_dim, model))
        return attn_out, cache_kv, cache_pe

    return jax.shard_map(local_step, mesh=mesh,
                         in_specs=(rows_spec, tok_spec) + (replicated,) * 8,
                         out_specs=(rows_spec, rows_spec, rows_spec), check_vma=False)
```

```python
import functools
import math

import jax
import jax.numpy as jnp
from jax import lax
from jax.experimental import pallas as pl
from jax.experimental.pallas import tpu as pltpu
from jax.sharding import PartitionSpec as P

ROPE_THETA = 10000.0
YARN_FACTOR = 40.0
ORIG_CTX = 4096.0
BETA_FAST = 32.0
BETA_SLOW = 1.0
NORM_EPS = 1e-6

MESH = pl.DeviceIdType.MESH
F32 = jnp.float32
BF16 = jnp.bfloat16
NT = (((1,), (1,)), ((), ()))
TT = (((0,), (1,)), ((), ()))


def rope_freqs(rot_dim):
    half_dim = rot_dim // 2
    log_base = 2.0 * math.log(ROPE_THETA)
    low_idx = max(math.floor(rot_dim * math.log(ORIG_CTX / (BETA_FAST * 2.0 * math.pi)) / log_base), 0)
    high_idx = min(math.ceil(rot_dim * math.log(ORIG_CTX / (BETA_SLOW * 2.0 * math.pi)) / log_base), half_dim - 1)
    spread = max(high_idx - low_idx, 0.001)
    freq_list = []
    for freq_idx in range(half_dim):
        base_freq = ROPE_THETA ** (-2.0 * freq_idx / rot_dim)
        ramp_val = min(max((freq_idx - low_idx) / spread, 0.0), 1.0)
        freq_list.append(base_freq / YARN_FACTOR * ramp_val + base_freq * (1.0 - ramp_val))
    return jnp.asarray(freq_list, dtype=jnp.float32)


def front_kernel(ranks, heads, x_hbm, wkv_hbm, wq_hbm, wuk_hbm, wuv_hbm, gq_ref, gkv_ref, cos_ref, sin_ref,
                 kv_all, cq_all, tab_all, wk_out, wv_out,
                 x_v, wkv_v, wq_v, wu_v, wo_v, wide_v, cq_f, kv_v, cq_v, tab_v,
                 w_sem, own_sem, kv_send, kv_recv, pair_send, pair_recv):
    me = lax.axis_index("sp")
    core = lax.rem(me, 2)
    sib = me + 1 - 2 * core
    rows = x_v.shape[0]
    half = cos_ref.shape[0]
    kv_rank = gkv_ref.shape[0]
    right = lax.rem(me + 2, ranks)
    left = lax.rem(me + ranks - 2, ranks)
    across = lax.rem(me + 4, ranks)

    kchunks, nq = wkv_v.shape[0], wq_v.shape[0]
    kc = wkv_v.shape[2]
    nc = wq_v.shape[2]
    first = core * heads
    loads = []
    for k in range(kchunks):
        cols = pl.ds(k * kc, kc)
        loads.append([pltpu.make_async_copy(x_hbm.at[:, cols], x_v.at[:, cols], w_sem.at[2 * k]),
                      pltpu.make_async_copy(wkv_hbm.at[:, cols], wkv_v.at[k], w_sem.at[2 * k + 1])])
    base = 2 * kchunks
    loads += [[pltpu.make_async_copy(wq_hbm.at[:, pl.ds(k * nc, nc)], wq_v.at[k], w_sem.at[base + k])] for k in range(nq)]
    loads += [[pltpu.make_async_copy(h.at[:, pl.ds(first, heads), :], wu_v.at[k], w_sem.at[base + nq + k])]
              for k, h in enumerate((wuk_hbm, wuv_hbm))]
    ahead = 3

    def launch(i):
        if i < len(loads):
            for c in loads[i]:
                c.start()

    def arrive(i):
        for c in loads[i]:
            c.wait()
        launch(i + ahead)

    for i in range(ahead):
        launch(i)

    barrier = pltpu.get_barrier_semaphore()
    for peer in (sib, right, left):
        pl.semaphore_signal(barrier, inc=1, device_id={"sp": peer}, device_id_type=MESH)

    def block(idx, start=0, size=None):
        return kv_all.at[pl.ds(idx * rows + start, size or rows)]

    def remote(src, dst, send, recv, dev):
        return pltpu.make_async_remote_copy(src_ref=src, dst_ref=dst, send_sem=send, recv_sem=recv,
                                            device_id={"sp": dev}, device_id_type=MESH)

    acc = None
    for k in range(kchunks):
        arrive(k)
        part = lax.dot_general(x_v[:, k * kc:(k + 1) * kc], wkv_v[k], NT, preferred_element_type=F32)
        acc = part if acc is None else acc + part
    a = acc[:, :kv_rank]
    inv = lax.rsqrt(jnp.mean(a * a, axis=-1, keepdims=True) + NORM_EPS)
    ckv = (a * inv * gkv_ref[...][None, :]).astype(BF16)
    tab_v[:half, :] = cos_ref[...]
    tab_v[half:, :] = sin_ref[...]
    tab = tab_v[...].T
    cos_t, sin_t = tab[:, :half], tab[:, half:]
    z1 = acc[:, kv_rank:kv_rank + half]
    z2 = acc[:, kv_rank + half:]
    pe = jnp.concatenate([z1 * cos_t - z2 * sin_t, z2 * cos_t + z1 * sin_t], axis=-1).astype(BF16)
    kv_v[:, :kv_rank] = ckv
    kv_v[:, kv_rank:] = jnp.concatenate([pe, jnp.zeros((rows, kv_v.shape[1] - kv_rank - 2 * half), BF16)], axis=-1)

    pl.semaphore_wait(barrier, 3)
    to_sib = remote(kv_v, block(me), kv_send.at[0], kv_recv.at[0], sib)
    to_right = remote(kv_v, block(me), kv_send.at[1], kv_recv.at[1], right)
    to_left = remote(kv_v, block(me), kv_send.at[2], kv_recv.at[2], left)
    tab_copy = remote(tab_v, tab_all.at[core], pair_send.at[0], pair_recv.at[0], sib)
    for c in (to_right, to_left, to_sib, tab_copy):
        c.start()
    own = [pltpu.make_async_copy(kv_v, block(me), own_sem.at[0]),
           pltpu.make_async_copy(tab_v, tab_all.at[core], own_sem.at[1])]
    for c in own:
        c.start()

    ssq = jnp.zeros((rows, 1), F32)
    for k in range(nq):
        arrive(kchunks + k)
        q = jnp.dot(x_v[...], wq_v[k], preferred_element_type=F32)
        cq_f[:, k * nc:(k + 1) * nc] = q
        ssq = ssq + jnp.sum(q * q, axis=-1, keepdims=True)
    inv_q = lax.rsqrt(ssq / cq_f.shape[1] + NORM_EPS)
    cq_v[...] = (cq_f[...] * inv_q * gq_ref[...][None, :]).astype(BF16)
    cq_copy = remote(cq_v, cq_all.at[pl.ds(core * rows, rows)], pair_send.at[1], pair_recv.at[1], sib)
    cq_copy.start()
    own.append(pltpu.make_async_copy(cq_v, cq_all.at[pl.ds(core * rows, rows)], own_sem.at[2]))
    own[-1].start()

    mid = rows // 2
    to_right.wait_recv()
    half_right = remote(block(left, 0, mid), block(left, 0, mid), kv_send.at[3], kv_recv.at[3], right)
    half_right.start()
    sib_left = remote(block(left), block(left), kv_send.at[5], kv_recv.at[5], sib)
    sib_left.start()
    to_left.wait_recv()
    half_left = remote(block(right, mid, mid), block(right, mid, mid), kv_send.at[4], kv_recv.at[4], left)
    half_left.start()
    sib_right = remote(block(right), block(right), kv_send.at[6], kv_recv.at[6], sib)
    sib_right.start()

    depth = wide_v.shape[1] // 8
    groups = wide_v.shape[0]
    width = wide_v.shape[2]
    for t, out in enumerate((wk_out, wv_out)):
        arrive(kchunks + nq + t)

        def relayout(i, _, t=t):
            base = pl.multiple_of(i * depth, depth)
            for g in range(groups):
                wide_v[g] = wu_v[t, pl.ds(base, depth), g * 8:(g + 1) * 8, :].astype(F32).reshape(depth * 8, width)
            for g in range(groups):
                for h in range(8):
                    col = (g * 8 + h) * width
                    wo_v[t, pl.ds(base, depth), col:col + width] = wide_v[g, pl.ds(h, depth, stride=8), :].astype(BF16)
            return _

        lax.fori_loop(0, wu_v.shape[1] // depth, relayout, 0)
        own.append(pltpu.make_async_copy(wo_v.at[t], out, own_sem.at[3 + t]))
        own[-1].start()

    half_right.wait_recv()
    half_left.wait_recv()
    sib_across = remote(block(across), block(across), kv_send.at[7], kv_recv.at[7], sib)
    sib_across.start()
    to_sib.wait()
    to_right.wait_send()
    to_left.wait_send()
    half_right.wait_send()
    half_left.wait_send()
    for c in (sib_left, sib_right, sib_across, tab_copy, cq_copy):
        c.wait()
    for c in own:
        c.wait()


def shares(me, ranks, steps):
    chips = ranks // 2
    chip = me // 2
    give = jnp.maximum(chip - chips // 2 + 1, 0)
    take = jnp.maximum(chips // 2 - chip, 0)
    lead = jnp.where(take > 0, steps // 2 + 2 * (take - 1), steps - give)
    return chip, lead, take, give


def weight_step(i, ranks, steps):
    _, lead, take, _ = shares(lax.axis_index("sp"), ranks, steps)
    far = steps - take + jnp.minimum(i - lead - 1, take - 1)
    late = jnp.where(i <= lead + take + 1, far, jnp.minimum(i - take - 2, steps - 1))
    return jnp.where((i <= lead) | (take == 0), jnp.minimum(i, lead - 1), late)


def attn_kernel(scale2, ranks, steps, cq_hbm, kv_ref, tab_ref,
                wqa_ref, wqb_ref, wka_ref, wkb_ref, wva_ref, wvb_ref, oa_hbm, ob_hbm, ckv_ref, cpe_ref,
                cq_v, tab_v, k_v, v_a, v_b, q_v, s_a, s_b, m_a, m_b, l_a, l_b, o_a, o_b, cosq_ref, sinq_ref, oa_v, ob_v,
                cq_sem, lat_send, lat_recv, fwd_send, fwd_recv, o_sem, oa_send, ob_send, oa_recv, ob_recv):
    step = pl.program_id(0)
    final = pl.num_programs(0) - 1
    me = lax.axis_index("sp")
    core = lax.rem(me, 2)
    sib = me + 1 - 2 * core
    chip, lead, take, give = shares(me, ranks, steps)
    taker = take > 0
    far_chip = ranks // 2 - 1 - chip
    far = 2 * far_chip + core
    most = oa_recv.shape[0]
    is_far = (step > lead) & (step <= lead + take + 1) & taker
    qset = jnp.where(is_far, 1, 0)
    full = jnp.where(is_far, far_chip, chip)
    _, blocks, blk, kdim = k_v.shape
    kv_rank = wka_ref.shape[0]
    nope = wka_ref.shape[1] // 2
    half = cosq_ref.shape[1]
    rot = 2 * half
    sub = blk // 2
    everything = slice(None)
    my_rows = pl.ds(pl.multiple_of(core * sub, sub), sub)

    lat = [pltpu.make_async_remote_copy(src_ref=src, dst_ref=dst, send_sem=lat_send.at[k], recv_sem=lat_recv.at[k],
                                        device_id={"sp": far}, device_id_type=MESH)
           for k, (src, dst) in enumerate(((cq_hbm.at[my_rows], cq_v.at[1, my_rows]), (tab_ref.at[core], tab_v.at[core])))]
    fwd = [pltpu.make_async_remote_copy(src_ref=ref, dst_ref=ref, send_sem=fwd_send.at[k], recv_sem=fwd_recv.at[k],
                                        device_id={"sp": sib}, device_id_type=MESH)
           for k, ref in enumerate((cq_v.at[1, my_rows], tab_v.at[core]))]

    def o_cols(at):
        return pl.ds(pl.multiple_of(at * 2 * nope, 2 * nope), 2 * nope)

    def o_local(part, s):
        src, dst = ((oa_v, oa_hbm), (ob_v, ob_hbm))[part]
        at = jnp.where(s <= lead, s - 1, s - take - 3)
        return pltpu.make_async_copy(src.at[most], dst.at[:, o_cols(at)], o_sem.at[part])

    def o_far(part, r):
        src, dst, send, recv = ((oa_v, oa_hbm, oa_send, oa_recv), (ob_v, ob_hbm, ob_send, ob_recv))[part]
        return pltpu.make_async_remote_copy(src_ref=src.at[r], dst_ref=dst.at[:, o_cols(steps - 1 - r)], send_sem=send.at[r], recv_sem=recv.at[r],
                                            device_id={"sp": far}, device_id_type=MESH)

    def left_own(s):
        return ((s >= 1) & (s <= lead)) | (taker & (s >= lead + take + 3) & (s <= steps + take + 2))

    def left_far(s):
        return taker & (s >= lead + 2) & (s <= lead + take + 1)

    far_slot = lead + take + 1 - step
    slot = jnp.where(left_far(step), far_slot, most)

    def emit(part):
        @pl.when(left_own(step))
        def _():
            o_local(part, step).start()

        @pl.when(left_far(step))
        def _():
            o_far(part, far_slot).start()

    def settle(part, s):
        @pl.when(left_own(s))
        def _():
            o_local(part, s).wait()

    @pl.when(step == 0)
    def _():
        own_cq = pltpu.make_async_copy(cq_hbm, cq_v.at[0], cq_sem.at[0])
        own_cq.start()
        barrier = pltpu.get_barrier_semaphore()
        for peer in (sib, far):
            pl.semaphore_signal(barrier, inc=1, device_id={"sp": peer}, device_id_type=MESH)
        pl.semaphore_wait(barrier, 2)

        @pl.when(give > 0)
        def _():
            for c in lat:
                c.start()

        for kb in range(blocks):
            pe = kv_ref[kb * blk:(kb + 1) * blk, kv_rank:]
            k_v[0, kb, :, nope:] = pe
            k_v[1, kb, :, nope:] = pe
        q_v[:, nope + rot:, :] = jnp.zeros((2, kdim - nope - rot, blk), BF16)
        for c in range(2):
            cosq_ref[0, :, c * sub:(c + 1) * sub] = tab_ref[c, :half, :]
            sinq_ref[0, :, c * sub:(c + 1) * sub] = tab_ref[c, half:, :]
        rows = ckv_ref.shape[0]
        own = kv_ref[pl.ds(pl.multiple_of(me * rows, rows), rows), :]
        ckv_ref[...] = own[:, :kv_rank]
        cpe_ref[...] = own[:, kv_rank:kv_rank + rot]
        own_cq.wait()

    @pl.when(step > 0)
    def _():
        for part in range(2):
            settle(part, step - 1)

    @pl.when((step == lead) & taker)
    def _():
        for c in lat:
            c.wait_recv()
        for c in fwd:
            c.start()

    @pl.when((step == lead + 1) & taker)
    def _():
        for c in fwd:
            c.wait()
        for c in range(2):
            cosq_ref[1, :, c * sub:(c + 1) * sub] = tab_v[c, :half, :]
            sinq_ref[1, :, c * sub:(c + 1) * sub] = tab_v[c, half:, :]

    def q_proj(w_ref):
        w = jnp.concatenate([w_ref[0], w_ref[1]], axis=0)
        both = lax.dot_general(w, cq_v[qset], NT, preferred_element_type=F32)
        cos_t, sin_t = cosq_ref[qset], sinq_ref[qset]
        for h in range(2):
            u = both[h * (nope + rot):(h + 1) * (nope + rot)]
            q_v[h, :nope, :] = u[:nope].astype(BF16)
            z1 = u[nope:nope + half]
            z2 = u[nope + half:]
            q_v[h, nope:nope + half, :] = (z1 * cos_t - z2 * sin_t).astype(BF16)
            q_v[h, nope + half:nope + rot, :] = (z2 * cos_t + z1 * sin_t).astype(BF16)

    def kv_proj(kb, wk, wv, v_ref):
        c = kv_ref[pl.ds(pl.multiple_of(kb * blk, blk), blk), :kv_rank]
        k = jnp.dot(c, wk, preferred_element_type=F32).astype(BF16)
        v = lax.dot_general(wv, c, NT, preferred_element_type=F32).astype(BF16)
        for h in range(2):
            k_v[h, kb, :, :nope] = k[:, h * nope:(h + 1) * nope]
            v_ref[h, kb] = v[h * nope:(h + 1) * nope]

    def fold_max(m_ref, h, s, cols):
        t = jnp.max(s.reshape(s.shape[0] // 8, 8, s.shape[1]), axis=0)
        m_ref[h, :, cols] = jnp.maximum(m_ref[h, :, cols], t)

    def qk(h, kb, s_ref, m_ref):
        s = jnp.dot(k_v[h, kb], q_v[h], preferred_element_type=F32)
        s_ref[h, kb] = s
        fold_max(m_ref, h, s, everything)

    def qk_diag(h, kb, s_ref, m_ref):
        s0 = jnp.dot(k_v[h, kb, :sub, :], q_v[h], preferred_element_type=F32)
        s1 = jnp.dot(k_v[h, kb, sub:, :], q_v[h, :, sub:], preferred_element_type=F32)
        keep = lax.broadcasted_iota(jnp.int32, (sub, sub), 0) <= lax.broadcasted_iota(jnp.int32, (sub, sub), 1)
        s00 = jnp.where(keep, s0[:, :sub], -jnp.inf)
        s1 = jnp.where(keep, s1, -jnp.inf)
        s01 = s0[:, sub:]
        s_ref[h, kb, :sub, :sub] = s00
        s_ref[h, kb, :sub, sub:] = s01
        s_ref[h, kb, sub:, sub:] = s1
        fold_max(m_ref, h, s00, slice(0, sub))
        fold_max(m_ref, h, s01, slice(sub, blk))
        fold_max(m_ref, h, s1, slice(sub, blk))

    def fold_sum(l_ref, h, p, cols):
        l_ref[h, :, cols] += jnp.sum(p.reshape(p.shape[0] // 8, 8, p.shape[1]), axis=0)

    def top(m_ref):
        return [jnp.max(m_ref[h], axis=0, keepdims=True) for h in range(2)]

    def pv(h, kb, v_ref, s_ref, m, l_ref, o_ref):
        p = jnp.exp2((s_ref[h, kb] - m[h]) * scale2)
        fold_sum(l_ref, h, p, everything)
        o_ref[h] += jnp.dot(v_ref[h, kb], p.astype(BF16), preferred_element_type=F32)

    def pv_diag(h, kb, v_ref, s_ref, m, l_ref, o_ref):
        p0 = jnp.exp2((s_ref[h, kb, :sub, :] - m[h]) * scale2)
        p1 = jnp.exp2((s_ref[h, kb, sub:, sub:] - m[h][:, sub:]) * scale2)
        fold_sum(l_ref, h, p0, everything)
        fold_sum(l_ref, h, p1, slice(sub, blk))
        p0 = p0.astype(BF16)
        o_ref[h] += jnp.dot(v_ref[h, kb, :, :sub], p0, preferred_element_type=F32)
        o_ref[h, :, sub:] += jnp.dot(v_ref[h, kb, :, sub:], p1.astype(BF16), preferred_element_type=F32)

    def finish(l_ref, o_ref, out_ref):
        for h in range(2):
            l = jnp.sum(l_ref[h], axis=0, keepdims=True)
            out_ref[slot, :, h * nope:(h + 1) * nope] = (o_ref[h] / l).T.astype(BF16)

    def clear(l_ref, o_ref):
        l_ref[...] = jnp.zeros_like(l_ref)
        o_ref[...] = jnp.zeros_like(o_ref)

    def stage(wq_ref, wk_ref, wv_ref, new, old, done, done_out, part):
        s_n, m_n, v_n = new
        s_o, m_o, v_o, l_o, out_o = old
        m = top(m_o)
        q_proj(wq_ref)
        finish(done[0], done[1], done_out)
        emit(part)
        clear(l_o, out_o)
        m_n[...] = jnp.full_like(m_n, -jnp.inf)
        wk = wk_ref[...]
        wv = wv_ref[...].T

        def body(kb, carry):
            kv_proj(kb, wk, wv, v_n)
            for h in range(2):
                pv(h, kb, v_o, s_o, m, l_o, out_o)
                qk(h, kb, s_n, m_n)
            return carry

        lax.fori_loop(0, full, body, 0)
        kv_proj(full, wk, wv, v_n)
        for h in range(2):
            pv_diag(h, full, v_o, s_o, m, l_o, out_o)
            qk_diag(h, full, s_n, m_n)

    @pl.when((step < lead) | (taker & (step > lead) & (step != lead + take + 1) & (step < steps + take + 2)))
    def _():
        stage(wqa_ref, wka_ref, wva_ref, (s_a, m_a, v_a), (s_b, m_b, v_b, l_b, o_b), (l_a, o_a), oa_v, 0)
        stage(wqb_ref, wkb_ref, wvb_ref, (s_b, m_b, v_b), (s_a, m_a, v_a, l_a, o_a), (l_b, o_b), ob_v, 1)

    @pl.when((step == lead) | (taker & ((step == lead + take + 1) | (step == steps + take + 2))))
    def _():
        m = top(m_b)
        clear(l_b, o_b)
        finish(l_a, o_a, oa_v)
        emit(0)

        def body(kb, carry):
            for h in range(2):
                pv(h, kb, v_b, s_b, m, l_b, o_b)
            return carry

        lax.fori_loop(0, full, body, 0)
        for h in range(2):
            pv_diag(h, full, v_b, s_b, m, l_b, o_b)
        finish(l_b, o_b, ob_v)
        emit(1)

    @pl.when(step == final)
    def _():
        for part in range(2):
            settle(part, step)

        @pl.when(give > 0)
        def _():
            for c in lat:
                c.wait_send()

        for r in range(most):
            @pl.when(give > r)
            def _(r=r):
                for part in range(2):
                    o_far(part, r).wait_recv()

            @pl.when(take > r)
            def _(r=r):
                for part in range(2):
                    o_far(part, r).wait_send()


def out_kernel(oa_hbm, ob_hbm, wo_hbm, out_hbm, own_v, sib_v, w_v, acc_v, out_v,
               o_sem, w_sem, out_sem, swap_send, swap_recv, res_send, res_recv):
    me = lax.axis_index("sp")
    core = lax.rem(me, 2)
    sib = me + 1 - 2 * core
    wide = oa_hbm.shape[1]
    span = own_v.shape[1]
    rows = out_hbm.shape[0]
    bufs, _, nc = w_v.shape
    steps = acc_v.shape[0]

    def fetch(i):
        part = i // steps
        owner = core + part - 2 * core * part
        col = core * (steps * nc) + lax.rem(i, steps) * nc
        slot = lax.rem(i, bufs)
        return pltpu.make_async_copy(
            wo_hbm.at[pl.ds(pl.multiple_of(owner * span, span), span), pl.ds(pl.multiple_of(col, nc), nc)],
            w_v.at[slot], w_sem.at[slot])

    own = [pltpu.make_async_copy(h, own_v.at[:, pl.ds(k * wide, wide)], o_sem.at[k])
           for k, h in enumerate((oa_hbm, ob_hbm))]
    fetch(0).start()
    for c in own:
        c.start()
    fetch(1).start()

    barrier = pltpu.get_barrier_semaphore()
    pl.semaphore_signal(barrier, inc=1, device_id={"sp": sib}, device_id_type=MESH)
    pl.semaphore_wait(barrier, 1)
    swap = [pltpu.make_async_remote_copy(
        src_ref=h, dst_ref=sib_v.at[:, pl.ds(k * wide, wide)],
        send_sem=swap_send.at[k], recv_sem=swap_recv.at[k], device_id={"sp": sib}, device_id_type=MESH)
        for k, h in enumerate((oa_hbm, ob_hbm))]
    for c in own:
        c.wait()
    for c in swap:
        c.start()

    def own_half(i, carry):
        fetch(i).wait()
        fetch(i + 2).start()
        acc_v[i] = jnp.dot(own_v[...], w_v[lax.rem(i, bufs)], preferred_element_type=F32)
        return carry

    lax.fori_loop(0, steps, own_half, 0)
    for c in swap:
        c.wait()

    def store(n):
        slot = lax.rem(n, 2)
        cols = pl.ds(pl.multiple_of(core * (steps * nc) + n * nc, nc), nc)
        keep = pltpu.make_async_copy(out_v.at[slot, pl.ds(pl.multiple_of(core * rows, rows), rows)],
                                     out_hbm.at[:, cols], out_sem.at[slot])
        give = pltpu.make_async_remote_copy(
            src_ref=out_v.at[slot, pl.ds(pl.multiple_of((1 - core) * rows, rows), rows)], dst_ref=out_hbm.at[:, cols],
            send_sem=res_send.at[n], recv_sem=res_recv.at[n], device_id={"sp": sib}, device_id_type=MESH)
        return keep, give

    def sib_half(n, carry):
        i = n + steps
        fetch(i).wait()

        @pl.when(i + 2 < 2 * steps)
        def _():
            fetch(i + 2).start()

        @pl.when(n >= 2)
        def _():
            keep, give = store(n - 2)
            keep.wait()
            give.wait_send()

        out_v[lax.rem(n, 2)] = (acc_v[n] + jnp.dot(sib_v[...], w_v[lax.rem(i, bufs)], preferred_element_type=F32)).astype(BF16)
        for c in store(n):
            c.start()
        return carry

    lax.fori_loop(0, steps, sib_half, 0)
    for n in range(steps - 2, steps):
        keep, give = store(n)
        keep.wait()
        give.wait_send()
    for n in range(steps):
        store(n)[1].wait_recv()


def solution(mesh):
    ranks = mesh.shape["sp"]
    tok_spec = P(("dp", "sp"))
    rows_spec = P(("dp", "sp"), None)
    replicated = P()

    def local_step(tok_in, tok_pos, w_dq, g_q, w_uq, w_dkv, g_kv, w_uk, w_uv, w_o):
        rows, model = tok_in.shape
        num_heads = w_uq.shape[1]
        qk_dim = w_uq.shape[2]
        q_rank = w_dq.shape[1]
        kv_rank = g_kv.shape[0]
        rot = w_dkv.shape[1] - kv_rank
        nope = qk_dim - rot
        v_dim = w_uv.shape[2]
        seq = rows * ranks
        half = rot // 2
        mine = num_heads // 2
        pe_w = 128
        attn_scale = (0.1 * math.log(YARN_FACTOR) + 1.0) ** 2 / math.sqrt(qk_dim)
        angles = rope_freqs(rot)[:, None] * tok_pos.astype(F32)[None, :]
        cos_t, sin_t = jnp.cos(angles), jnp.sin(angles)

        kchunks, nq, depth = 4, 3, 64
        kv_w = kv_rank + pe_w
        any_spec = pl.BlockSpec(memory_space=pl.ANY)
        vmem_spec = pl.BlockSpec(memory_space=pltpu.VMEM)
        dma = pltpu.SemaphoreType.DMA
        kv_all, cq_all, tab_all, wk2, wv2 = pl.pallas_call(
            functools.partial(front_kernel, ranks, mine),
            out_shape=(
                jax.ShapeDtypeStruct((seq, kv_w), BF16),
                jax.ShapeDtypeStruct((2 * rows, q_rank), BF16),
                jax.ShapeDtypeStruct((2, rot, rows), F32),
                jax.ShapeDtypeStruct((kv_rank, mine * nope), BF16),
                jax.ShapeDtypeStruct((kv_rank, mine * v_dim), BF16),
            ),
            in_specs=[any_spec] * 5 + [vmem_spec] * 4,
            out_specs=(any_spec,) * 5,
            scratch_shapes=[
                pltpu.VMEM((rows, model), BF16),
                pltpu.VMEM((kchunks, kv_rank + rot, model // kchunks), BF16),
                pltpu.VMEM((nq, model, q_rank // nq), BF16),
                pltpu.VMEM((2, kv_rank, mine, nope), BF16),
                pltpu.VMEM((2, kv_rank, mine * nope), BF16),
                pltpu.VMEM((mine // 8, depth * 8, nope), F32),
                pltpu.VMEM((rows, q_rank), F32),
                pltpu.VMEM((rows, kv_w), BF16),
                pltpu.VMEM((rows, q_rank), BF16),
                pltpu.VMEM((rot, rows), F32),
                dma((2 * kchunks + nq + 2,)),
                dma((5,)),
                dma((8,)),
                dma((8,)),
                dma((2,)),
                dma((2,)),
            ],
            compiler_params=pltpu.CompilerParams(collective_id=0, has_side_effects=True, vmem_limit_bytes=60 << 20),
            cost_estimate=pl.CostEstimate(flops=2 * rows * model * (q_rank + kv_rank + rot), bytes_accessed=2 * model * (q_rank + kv_rank + rot), transcendentals=0),
        )(tok_in, w_dkv.T, w_dq, w_uk, w_uv, g_q, g_kv, cos_t, sin_t)

        wuq_t = jnp.transpose(w_uq, (1, 2, 0))
        qn = 2 * rows
        nblk = seq // qn
        steps = mine // 4

        def whole(shape):
            return pl.BlockSpec(shape, lambda i: (0,) * len(shape))

        def up_spec(part):
            return pl.BlockSpec((2, qk_dim, q_rank), lambda i: (lax.rem(lax.axis_index("sp"), 2) * (mine // 2) + part * steps + weight_step(i, ranks, steps), 0, 0))

        def lat_spec(part):
            return pl.BlockSpec((kv_rank, 2 * nope), lambda i: (0, part * steps + weight_step(i, ranks, steps)))

        head_v = pltpu.VMEM((2, nblk, v_dim, qn), BF16)
        scores = pltpu.VMEM((2, nblk, qn, qn), F32)
        stat = pltpu.VMEM((2, 8, qn), F32)
        head_o = pltpu.VMEM((2, v_dim, qn), F32)
        rope_v = pltpu.VMEM((2, half, qn), F32)
        most = ranks // 4
        pair_o = pltpu.VMEM((most + 1, qn, 2 * v_dim), BF16)
        o_a, o_b, cache_kv, cache_pe = pl.pallas_call(
            functools.partial(attn_kernel, attn_scale * math.log2(math.e), ranks, steps),
            out_shape=(jax.ShapeDtypeStruct((qn, 2 * steps * v_dim), BF16),) * 2 + (
                jax.ShapeDtypeStruct((rows, kv_rank), BF16),
                jax.ShapeDtypeStruct((rows, rot), BF16),
            ),
            grid=(steps + most + 3,),
            in_specs=[
                any_spec,
                whole((seq, kv_w)),
                whole((2, rot, rows)),
                up_spec(0), up_spec(1), lat_spec(0), lat_spec(1), lat_spec(0), lat_spec(1),
            ],
            out_specs=(any_spec, any_spec, whole((rows, kv_rank)), whole((rows, rot))),
            scratch_shapes=[pltpu.VMEM((2, qn, q_rank), BF16), pltpu.VMEM((2, rot, rows), F32),
                            pltpu.VMEM((2, nblk, qn, nope + pe_w), BF16), head_v, head_v, pltpu.VMEM((2, nope + pe_w, qn), BF16),
                            scores, scores, stat, stat, stat, stat, head_o, head_o, rope_v, rope_v, pair_o, pair_o,
                            dma((1,)), dma((2,)), dma((2,)), dma((2,)), dma((2,)), dma((2,)), dma((most,)), dma((most,)), dma((most,)), dma((most,))],
            compiler_params=pltpu.CompilerParams(dimension_semantics=("arbitrary",), collective_id=2, has_side_effects=True, vmem_limit_bytes=62 << 20),
        )(cq_all, kv_all, tab_all, wuq_t, wuq_t, wk2, wk2, wv2, wv2)

        nc, bufs = 512, 3
        span = mine * v_dim
        pieces = model // 2 // nc
        attn_out = pl.pallas_call(
            out_kernel,
            out_shape=jax.ShapeDtypeStruct((rows, model), BF16),
            in_specs=[any_spec] * 3,
            out_specs=any_spec,
            scratch_shapes=[
                pltpu.VMEM((qn, span), BF16),
                pltpu.VMEM((qn, span), BF16),
                pltpu.VMEM((bufs, span, nc), BF16),
                pltpu.VMEM((pieces, qn, nc), F32),
                pltpu.VMEM((2, qn, nc), BF16),
                dma((2,)),
                dma((bufs,)),
                dma((2,)),
                dma((2,)),
                dma((2,)),
                dma((pieces,)),
                dma((pieces,)),
            ],
            compiler_params=pltpu.CompilerParams(collective_id=1, has_side_effects=True, vmem_limit_bytes=60 << 20),
        )(o_a, o_b, w_o.reshape(num_heads * v_dim, model))
        return attn_out, cache_kv, cache_pe

    return jax.shard_map(local_step, mesh=mesh,
                         in_specs=(rows_spec, tok_spec) + (replicated,) * 8,
                         out_specs=(rows_spec, rows_spec, rows_spec), check_vma=False)
```

```python
import functools
import math

import jax
import jax.numpy as jnp
from jax import lax
from jax.experimental import pallas as pl
from jax.experimental.pallas import tpu as pltpu
from jax.sharding import PartitionSpec as P

ROPE_THETA = 10000.0
YARN_FACTOR = 40.0
ORIG_CTX = 4096.0
BETA_FAST = 32.0
BETA_SLOW = 1.0
NORM_EPS = 1e-6

MESH = pl.DeviceIdType.MESH
F32 = jnp.float32
BF16 = jnp.bfloat16
NT = (((1,), (1,)), ((), ()))
TT = (((0,), (1,)), ((), ()))


def rope_freqs(rot_dim):
    half_dim = rot_dim // 2
    log_base = 2.0 * math.log(ROPE_THETA)
    low_idx = max(math.floor(rot_dim * math.log(ORIG_CTX / (BETA_FAST * 2.0 * math.pi)) / log_base), 0)
    high_idx = min(math.ceil(rot_dim * math.log(ORIG_CTX / (BETA_SLOW * 2.0 * math.pi)) / log_base), half_dim - 1)
    spread = max(high_idx - low_idx, 0.001)
    freq_list = []
    for freq_idx in range(half_dim):
        base_freq = ROPE_THETA ** (-2.0 * freq_idx / rot_dim)
        ramp_val = min(max((freq_idx - low_idx) / spread, 0.0), 1.0)
        freq_list.append(base_freq / YARN_FACTOR * ramp_val + base_freq * (1.0 - ramp_val))
    return jnp.asarray(freq_list, dtype=jnp.float32)


def front_kernel(ranks, heads, x_hbm, wkv_hbm, wq_hbm, wuk_hbm, wuv_hbm, gq_ref, gkv_ref, cos_ref, sin_ref,
                 kv_all, cq_all, tab_all, wk_out, wv_out,
                 x_v, wkv_v, wq_v, wu_v, wo_v, wide_v, cq_f, kv_v, cq_v, tab_v,
                 w_sem, own_sem, kv_send, kv_recv, pair_send, pair_recv):
    me = lax.axis_index("sp")
    core = lax.rem(me, 2)
    sib = me + 1 - 2 * core
    rows = x_v.shape[0]
    half = cos_ref.shape[0]
    kv_rank = gkv_ref.shape[0]
    right = lax.rem(me + 2, ranks)
    left = lax.rem(me + ranks - 2, ranks)
    across = lax.rem(me + 4, ranks)

    kchunks, nq = wkv_v.shape[0], wq_v.shape[0]
    kc = wkv_v.shape[2]
    nc = wq_v.shape[2]
    first = core * heads
    loads = []
    for k in range(kchunks):
        cols = pl.ds(k * kc, kc)
        loads.append([pltpu.make_async_copy(x_hbm.at[:, cols], x_v.at[:, cols], w_sem.at[2 * k]),
                      pltpu.make_async_copy(wkv_hbm.at[:, cols], wkv_v.at[k], w_sem.at[2 * k + 1])])
    base = 2 * kchunks
    loads += [[pltpu.make_async_copy(wq_hbm.at[:, pl.ds(k * nc, nc)], wq_v.at[k], w_sem.at[base + k])] for k in range(nq)]
    loads += [[pltpu.make_async_copy(h.at[:, pl.ds(first, heads), :], wu_v.at[k], w_sem.at[base + nq + k])]
              for k, h in enumerate((wuk_hbm, wuv_hbm))]
    ahead = 3

    def launch(i):
        if i < len(loads):
            for c in loads[i]:
                c.start()

    def arrive(i):
        for c in loads[i]:
            c.wait()
        launch(i + ahead)

    for i in range(ahead):
        launch(i)

    barrier = pltpu.get_barrier_semaphore()
    for peer in (sib, right, left):
        pl.semaphore_signal(barrier, inc=1, device_id={"sp": peer}, device_id_type=MESH)

    def block(idx, start=0, size=None):
        return kv_all.at[pl.ds(idx * rows + start, size or rows)]

    def remote(src, dst, send, recv, dev):
        return pltpu.make_async_remote_copy(src_ref=src, dst_ref=dst, send_sem=send, recv_sem=recv,
                                            device_id={"sp": dev}, device_id_type=MESH)

    acc = None
    for k in range(kchunks):
        arrive(k)
        part = lax.dot_general(x_v[:, k * kc:(k + 1) * kc], wkv_v[k], NT, preferred_element_type=F32)
        acc = part if acc is None else acc + part
    a = acc[:, :kv_rank]
    inv = lax.rsqrt(jnp.mean(a * a, axis=-1, keepdims=True) + NORM_EPS)
    ckv = (a * inv * gkv_ref[...][None, :]).astype(BF16)
    tab_v[:half, :] = cos_ref[...]
    tab_v[half:, :] = sin_ref[...]
    tab = tab_v[...].T
    cos_t, sin_t = tab[:, :half], tab[:, half:]
    z1 = acc[:, kv_rank:kv_rank + half]
    z2 = acc[:, kv_rank + half:]
    pe = jnp.concatenate([z1 * cos_t - z2 * sin_t, z2 * cos_t + z1 * sin_t], axis=-1).astype(BF16)
    kv_v[:, :kv_rank] = ckv
    kv_v[:, kv_rank:] = jnp.concatenate([pe, jnp.zeros((rows, kv_v.shape[1] - kv_rank - 2 * half), BF16)], axis=-1)

    pl.semaphore_wait(barrier, 3)
    to_sib = remote(kv_v, block(me), kv_send.at[0], kv_recv.at[0], sib)
    to_right = remote(kv_v, block(me), kv_send.at[1], kv_recv.at[1], right)
    to_left = remote(kv_v, block(me), kv_send.at[2], kv_recv.at[2], left)
    tab_copy = remote(tab_v, tab_all.at[core], pair_send.at[0], pair_recv.at[0], sib)
    for c in (to_right, to_left, to_sib, tab_copy):
        c.start()
    own = [pltpu.make_async_copy(kv_v, block(me), own_sem.at[0]),
           pltpu.make_async_copy(tab_v, tab_all.at[core], own_sem.at[1])]
    for c in own:
        c.start()

    ssq = jnp.zeros((rows, 1), F32)
    for k in range(nq):
        arrive(kchunks + k)
        q = jnp.dot(x_v[...], wq_v[k], preferred_element_type=F32)
        cq_f[:, k * nc:(k + 1) * nc] = q
        ssq = ssq + jnp.sum(q * q, axis=-1, keepdims=True)
    inv_q = lax.rsqrt(ssq / cq_f.shape[1] + NORM_EPS)
    cq_v[...] = (cq_f[...] * inv_q * gq_ref[...][None, :]).astype(BF16)
    cq_copy = remote(cq_v, cq_all.at[pl.ds(core * rows, rows)], pair_send.at[1], pair_recv.at[1], sib)
    cq_copy.start()
    own.append(pltpu.make_async_copy(cq_v, cq_all.at[pl.ds(core * rows, rows)], own_sem.at[2]))
    own[-1].start()

    depth = wide_v.shape[1] // 8
    groups = wide_v.shape[0]
    width = wide_v.shape[2]

    def up_relayout(t, out):
        arrive(kchunks + nq + t)

        def relayout(i, carry):
            base = pl.multiple_of(i * depth, depth)
            for g in range(groups):
                wide_v[g] = wu_v[t, pl.ds(base, depth), g * 8:(g + 1) * 8, :].astype(F32).reshape(depth * 8, width)
            for g in range(groups):
                for h in range(8):
                    col = (g * 8 + h) * width
                    wo_v[t, pl.ds(base, depth), col:col + width] = wide_v[g, pl.ds(h, depth, stride=8), :].astype(BF16)
            return carry

        lax.fori_loop(0, wu_v.shape[1] // depth, relayout, 0)
        own.append(pltpu.make_async_copy(wo_v.at[t], out, own_sem.at[3 + t]))
        own[-1].start()

    up_relayout(0, wk_out)
    mid = rows // 2
    to_right.wait_recv()
    half_right = remote(block(left, 0, mid), block(left, 0, mid), kv_send.at[3], kv_recv.at[3], right)
    half_right.start()
    sib_left = remote(block(left), block(left), kv_send.at[5], kv_recv.at[5], sib)
    sib_left.start()
    to_left.wait_recv()
    half_left = remote(block(right, mid, mid), block(right, mid, mid), kv_send.at[4], kv_recv.at[4], left)
    half_left.start()
    sib_right = remote(block(right), block(right), kv_send.at[6], kv_recv.at[6], sib)
    sib_right.start()
    up_relayout(1, wv_out)
    half_right.wait_recv()
    half_left.wait_recv()
    sib_across = remote(block(across), block(across), kv_send.at[7], kv_recv.at[7], sib)
    sib_across.start()
    to_sib.wait()
    to_right.wait_send()
    to_left.wait_send()
    half_right.wait_send()
    half_left.wait_send()
    for c in (sib_left, sib_right, sib_across, tab_copy, cq_copy):
        c.wait()
    for c in own:
        c.wait()


def shares(me, ranks, steps):
    chips = ranks // 2
    chip = me // 2
    give = jnp.maximum(chip - chips // 2 + 1, 0)
    take = jnp.maximum(chips // 2 - chip, 0)
    lead = jnp.where(take > 0, steps // 2 + take - 1, steps - give)
    return chip, lead, take, give


def weight_step(i, ranks, steps):
    _, lead, take, _ = shares(lax.axis_index("sp"), ranks, steps)
    far = steps - take + jnp.minimum(i - lead - 1, take - 1)
    late = jnp.where(i <= lead + take + 1, far, jnp.minimum(i - take - 2, steps - 1))
    return jnp.where((i <= lead) | (take == 0), jnp.minimum(i, lead - 1), late)


def attn_kernel(scale2, ranks, steps, cq_hbm, kv_ref, tab_ref,
                wqa_ref, wqb_ref, wka_ref, wkb_ref, wva_ref, wvb_ref, oa_hbm, ob_hbm, ckv_ref, cpe_ref,
                cq_v, tab_v, k_v, v_a, v_b, q_v, s_a, s_b, m_a, m_b, l_a, l_b, o_a, o_b, cosq_ref, sinq_ref, oa_v, ob_v,
                cq_sem, lat_send, lat_recv, fwd_send, fwd_recv, o_sem, oa_send, ob_send, oa_recv, ob_recv):
    step = pl.program_id(0)
    final = pl.num_programs(0) - 1
    me = lax.axis_index("sp")
    core = lax.rem(me, 2)
    sib = me + 1 - 2 * core
    chip, lead, take, give = shares(me, ranks, steps)
    taker = take > 0
    far_chip = ranks // 2 - 1 - chip
    far = 2 * far_chip + core
    most = oa_recv.shape[0]
    is_far = (step > lead) & (step <= lead + take + 1) & taker
    qset = jnp.where(is_far, 1, 0)
    full = jnp.where(is_far, far_chip, chip)
    _, blocks, blk, kdim = k_v.shape
    kv_rank = wka_ref.shape[0]
    nope = wka_ref.shape[1] // 2
    half = cosq_ref.shape[1]
    rot = 2 * half
    sub = blk // 2
    everything = slice(None)
    my_rows = pl.ds(pl.multiple_of(core * sub, sub), sub)

    lat = [pltpu.make_async_remote_copy(src_ref=src, dst_ref=dst, send_sem=lat_send.at[k], recv_sem=lat_recv.at[k],
                                        device_id={"sp": far}, device_id_type=MESH)
           for k, (src, dst) in enumerate(((cq_hbm.at[my_rows], cq_v.at[1, my_rows]), (tab_ref.at[core], tab_v.at[core])))]
    fwd = [pltpu.make_async_remote_copy(src_ref=ref, dst_ref=ref, send_sem=fwd_send.at[k], recv_sem=fwd_recv.at[k],
                                        device_id={"sp": sib}, device_id_type=MESH)
           for k, ref in enumerate((cq_v.at[1, my_rows], tab_v.at[core]))]

    def o_cols(at):
        return pl.ds(pl.multiple_of(at * 2 * nope, 2 * nope), 2 * nope)

    def o_local(part, s):
        src, dst = ((oa_v, oa_hbm), (ob_v, ob_hbm))[part]
        at = jnp.where(s <= lead, s - 1, s - take - 3)
        return pltpu.make_async_copy(src.at[most], dst.at[:, o_cols(at)], o_sem.at[part])

    def o_far(part, r):
        src, dst, send, recv = ((oa_v, oa_hbm, oa_send, oa_recv), (ob_v, ob_hbm, ob_send, ob_recv))[part]
        return pltpu.make_async_remote_copy(src_ref=src.at[r], dst_ref=dst.at[:, o_cols(steps - 1 - r)], send_sem=send.at[r], recv_sem=recv.at[r],
                                            device_id={"sp": far}, device_id_type=MESH)

    def left_own(s):
        return ((s >= 1) & (s <= lead)) | (taker & (s >= lead + take + 3) & (s <= steps + take + 2))

    def left_far(s):
        return taker & (s >= lead + 2) & (s <= lead + take + 1)

    far_slot = lead + take + 1 - step
    slot = jnp.where(left_far(step), far_slot, most)

    def emit(part):
        @pl.when(left_own(step))
        def _():
            o_local(part, step).start()

        @pl.when(left_far(step))
        def _():
            o_far(part, far_slot).start()

    def settle(part, s):
        @pl.when(left_own(s))
        def _():
            o_local(part, s).wait()

    @pl.when(step == 0)
    def _():
        own_cq = pltpu.make_async_copy(cq_hbm, cq_v.at[0], cq_sem.at[0])
        own_cq.start()
        barrier = pltpu.get_barrier_semaphore()
        for peer in (sib, far):
            pl.semaphore_signal(barrier, inc=1, device_id={"sp": peer}, device_id_type=MESH)
        pl.semaphore_wait(barrier, 2)

        @pl.when(give > 0)
        def _():
            for c in lat:
                c.start()

        for kb in range(blocks):
            pe = kv_ref[kb * blk:(kb + 1) * blk, kv_rank:]
            k_v[0, kb, :, nope:] = pe
            k_v[1, kb, :, nope:] = pe
        q_v[:, nope + rot:, :] = jnp.zeros((2, kdim - nope - rot, blk), BF16)
        for c in range(2):
            cosq_ref[0, :, c * sub:(c + 1) * sub] = tab_ref[c, :half, :]
            sinq_ref[0, :, c * sub:(c + 1) * sub] = tab_ref[c, half:, :]
        rows = ckv_ref.shape[0]
        own = kv_ref[pl.ds(pl.multiple_of(me * rows, rows), rows), :]
        ckv_ref[...] = own[:, :kv_rank]
        cpe_ref[...] = own[:, kv_rank:kv_rank + rot]
        own_cq.wait()

    @pl.when(step > 0)
    def _():
        for part in range(2):
            settle(part, step - 1)

    @pl.when((step == lead) & taker)
    def _():
        for c in lat:
            c.wait_recv()
        for c in fwd:
            c.start()

    @pl.when((step == lead + 1) & taker)
    def _():
        for c in fwd:
            c.wait()
        for c in range(2):
            cosq_ref[1, :, c * sub:(c + 1) * sub] = tab_v[c, :half, :]
            sinq_ref[1, :, c * sub:(c + 1) * sub] = tab_v[c, half:, :]

    def q_proj(w_ref):
        w = jnp.concatenate([w_ref[0], w_ref[1]], axis=0)
        both = lax.dot_general(w, cq_v[qset], NT, preferred_element_type=F32)
        cos_t, sin_t = cosq_ref[qset], sinq_ref[qset]
        for h in range(2):
            u = both[h * (nope + rot):(h + 1) * (nope + rot)]
            q_v[h, :nope, :] = u[:nope].astype(BF16)
            z1 = u[nope:nope + half]
            z2 = u[nope + half:]
            q_v[h, nope:nope + half, :] = (z1 * cos_t - z2 * sin_t).astype(BF16)
            q_v[h, nope + half:nope + rot, :] = (z2 * cos_t + z1 * sin_t).astype(BF16)

    def kv_proj(kb, wk, wv, v_ref):
        c = kv_ref[pl.ds(pl.multiple_of(kb * blk, blk), blk), :kv_rank]
        k = jnp.dot(c, wk, preferred_element_type=F32).astype(BF16)
        v = lax.dot_general(wv, c, NT, preferred_element_type=F32).astype(BF16)
        for h in range(2):
            k_v[h, kb, :, :nope] = k[:, h * nope:(h + 1) * nope]
            v_ref[h, kb] = v[h * nope:(h + 1) * nope]

    def fold_max(m_ref, h, s, cols):
        t = jnp.max(s.reshape(s.shape[0] // 8, 8, s.shape[1]), axis=0)
        m_ref[h, :, cols] = jnp.maximum(m_ref[h, :, cols], t)

    def qk(h, kb, s_ref, m_ref):
        s = jnp.dot(k_v[h, kb], q_v[h], preferred_element_type=F32)
        s_ref[h, kb] = s
        fold_max(m_ref, h, s, everything)

    def qk_diag(h, kb, s_ref, m_ref):
        s0 = jnp.dot(k_v[h, kb, :sub, :], q_v[h], preferred_element_type=F32)
        s1 = jnp.dot(k_v[h, kb, sub:, :], q_v[h, :, sub:], preferred_element_type=F32)
        keep = lax.broadcasted_iota(jnp.int32, (sub, sub), 0) <= lax.broadcasted_iota(jnp.int32, (sub, sub), 1)
        s00 = jnp.where(keep, s0[:, :sub], -jnp.inf)
        s1 = jnp.where(keep, s1, -jnp.inf)
        s01 = s0[:, sub:]
        s_ref[h, kb, :sub, :sub] = s00
        s_ref[h, kb, :sub, sub:] = s01
        s_ref[h, kb, sub:, sub:] = s1
        fold_max(m_ref, h, s00, slice(0, sub))
        fold_max(m_ref, h, s01, slice(sub, blk))
        fold_max(m_ref, h, s1, slice(sub, blk))

    def fold_sum(l_ref, h, p, cols):
        l_ref[h, :, cols] += jnp.sum(p.reshape(p.shape[0] // 8, 8, p.shape[1]), axis=0)

    def top(m_ref):
        return [jnp.max(m_ref[h], axis=0, keepdims=True) for h in range(2)]

    def pv(h, kb, v_ref, s_ref, m, l_ref, o_ref):
        p = jnp.exp2((s_ref[h, kb] - m[h]) * scale2)
        fold_sum(l_ref, h, p, everything)
        o_ref[h] += jnp.dot(v_ref[h, kb], p.astype(BF16), preferred_element_type=F32)

    def pv_diag(h, kb, v_ref, s_ref, m, l_ref, o_ref):
        p0 = jnp.exp2((s_ref[h, kb, :sub, :] - m[h]) * scale2)
        p1 = jnp.exp2((s_ref[h, kb, sub:, sub:] - m[h][:, sub:]) * scale2)
        fold_sum(l_ref, h, p0, everything)
        fold_sum(l_ref, h, p1, slice(sub, blk))
        p0 = p0.astype(BF16)
        o_ref[h] += jnp.dot(v_ref[h, kb, :, :sub], p0, preferred_element_type=F32)
        o_ref[h, :, sub:] += jnp.dot(v_ref[h, kb, :, sub:], p1.astype(BF16), preferred_element_type=F32)

    def finish(l_ref, o_ref, out_ref):
        for h in range(2):
            l = jnp.sum(l_ref[h], axis=0, keepdims=True)
            out_ref[slot, :, h * nope:(h + 1) * nope] = (o_ref[h] / l).T.astype(BF16)

    def clear(l_ref, o_ref):
        l_ref[...] = jnp.zeros_like(l_ref)
        o_ref[...] = jnp.zeros_like(o_ref)

    def stage(wq_ref, wk_ref, wv_ref, new, old, done, done_out, part):
        s_n, m_n, v_n = new
        s_o, m_o, v_o, l_o, out_o = old
        m = top(m_o)
        q_proj(wq_ref)
        finish(done[0], done[1], done_out)
        emit(part)
        clear(l_o, out_o)
        m_n[...] = jnp.full_like(m_n, -jnp.inf)
        wk = wk_ref[...]
        wv = wv_ref[...].T

        def body(kb, carry):
            kv_proj(kb, wk, wv, v_n)
            for h in range(2):
                pv(h, kb, v_o, s_o, m, l_o, out_o)
                qk(h, kb, s_n, m_n)
            return carry

        lax.fori_loop(0, full, body, 0)
        kv_proj(full, wk, wv, v_n)
        for h in range(2):
            pv_diag(h, full, v_o, s_o, m, l_o, out_o)
            qk_diag(h, full, s_n, m_n)

    @pl.when((step < lead) | (taker & (step > lead) & (step != lead + take + 1) & (step < steps + take + 2)))
    def _():
        stage(wqa_ref, wka_ref, wva_ref, (s_a, m_a, v_a), (s_b, m_b, v_b, l_b, o_b), (l_a, o_a), oa_v, 0)
        stage(wqb_ref, wkb_ref, wvb_ref, (s_b, m_b, v_b), (s_a, m_a, v_a, l_a, o_a), (l_b, o_b), ob_v, 1)

    @pl.when((step == lead) | (taker & ((step == lead + take + 1) | (step == steps + take + 2))))
    def _():
        m = top(m_b)
        clear(l_b, o_b)
        finish(l_a, o_a, oa_v)
        emit(0)

        def body(kb, carry):
            for h in range(2):
                pv(h, kb, v_b, s_b, m, l_b, o_b)
            return carry

        lax.fori_loop(0, full, body, 0)
        for h in range(2):
            pv_diag(h, full, v_b, s_b, m, l_b, o_b)
        finish(l_b, o_b, ob_v)
        emit(1)

    @pl.when(step == final)
    def _():
        for part in range(2):
            settle(part, step)

        @pl.when(give > 0)
        def _():
            for c in lat:
                c.wait_send()

        for r in range(most):
            @pl.when(give > r)
            def _(r=r):
                for part in range(2):
                    o_far(part, r).wait_recv()

            @pl.when(take > r)
            def _(r=r):
                for part in range(2):
                    o_far(part, r).wait_send()


def out_kernel(oa_hbm, ob_hbm, wo_hbm, out_hbm, own_v, sib_v, w_v, acc_v, out_v,
               o_sem, w_sem, out_sem, swap_send, swap_recv, res_send, res_recv):
    me = lax.axis_index("sp")
    core = lax.rem(me, 2)
    sib = me + 1 - 2 * core
    wide = oa_hbm.shape[1]
    span = own_v.shape[1]
    rows = out_hbm.shape[0]
    bufs, _, nc = w_v.shape
    steps = acc_v.shape[0]

    def fetch(i):
        part = i // steps
        owner = core + part - 2 * core * part
        col = core * (steps * nc) + lax.rem(i, steps) * nc
        slot = lax.rem(i, bufs)
        return pltpu.make_async_copy(
            wo_hbm.at[pl.ds(pl.multiple_of(owner * span, span), span), pl.ds(pl.multiple_of(col, nc), nc)],
            w_v.at[slot], w_sem.at[slot])

    own = [pltpu.make_async_copy(h, own_v.at[:, pl.ds(k * wide, wide)], o_sem.at[k])
           for k, h in enumerate((oa_hbm, ob_hbm))]
    fetch(0).start()
    for c in own:
        c.start()
    fetch(1).start()

    barrier = pltpu.get_barrier_semaphore()
    pl.semaphore_signal(barrier, inc=1, device_id={"sp": sib}, device_id_type=MESH)
    pl.semaphore_wait(barrier, 1)
    swap = [pltpu.make_async_remote_copy(
        src_ref=h, dst_ref=sib_v.at[:, pl.ds(k * wide, wide)],
        send_sem=swap_send.at[k], recv_sem=swap_recv.at[k], device_id={"sp": sib}, device_id_type=MESH)
        for k, h in enumerate((oa_hbm, ob_hbm))]
    for c in own:
        c.wait()
    for c in swap:
        c.start()

    def own_half(i, carry):
        fetch(i).wait()
        fetch(i + 2).start()
        acc_v[i] = jnp.dot(own_v[...], w_v[lax.rem(i, bufs)], preferred_element_type=F32)
        return carry

    lax.fori_loop(0, steps, own_half, 0)
    for c in swap:
        c.wait()

    def store(n):
        slot = lax.rem(n, 2)
        cols = pl.ds(pl.multiple_of(core * (steps * nc) + n * nc, nc), nc)
        keep = pltpu.make_async_copy(out_v.at[slot, pl.ds(pl.multiple_of(core * rows, rows), rows)],
                                     out_hbm.at[:, cols], out_sem.at[slot])
        give = pltpu.make_async_remote_copy(
            src_ref=out_v.at[slot, pl.ds(pl.multiple_of((1 - core) * rows, rows), rows)], dst_ref=out_hbm.at[:, cols],
            send_sem=res_send.at[n], recv_sem=res_recv.at[n], device_id={"sp": sib}, device_id_type=MESH)
        return keep, give

    def sib_half(n, carry):
        i = n + steps
        fetch(i).wait()

        @pl.when(i + 2 < 2 * steps)
        def _():
            fetch(i + 2).start()

        @pl.when(n >= 2)
        def _():
            keep, give = store(n - 2)
            keep.wait()
            give.wait_send()

        out_v[lax.rem(n, 2)] = (acc_v[n] + jnp.dot(sib_v[...], w_v[lax.rem(i, bufs)], preferred_element_type=F32)).astype(BF16)
        for c in store(n):
            c.start()
        return carry

    lax.fori_loop(0, steps, sib_half, 0)
    for n in range(steps - 2, steps):
        keep, give = store(n)
        keep.wait()
        give.wait_send()
    for n in range(steps):
        store(n)[1].wait_recv()


def solution(mesh):
    ranks = mesh.shape["sp"]
    tok_spec = P(("dp", "sp"))
    rows_spec = P(("dp", "sp"), None)
    replicated = P()

    def local_step(tok_in, tok_pos, w_dq, g_q, w_uq, w_dkv, g_kv, w_uk, w_uv, w_o):
        rows, model = tok_in.shape
        num_heads = w_uq.shape[1]
        qk_dim = w_uq.shape[2]
        q_rank = w_dq.shape[1]
        kv_rank = g_kv.shape[0]
        rot = w_dkv.shape[1] - kv_rank
        nope = qk_dim - rot
        v_dim = w_uv.shape[2]
        seq = rows * ranks
        half = rot // 2
        mine = num_heads // 2
        pe_w = 128
        attn_scale = (0.1 * math.log(YARN_FACTOR) + 1.0) ** 2 / math.sqrt(qk_dim)
        angles = rope_freqs(rot)[:, None] * tok_pos.astype(F32)[None, :]
        cos_t, sin_t = jnp.cos(angles), jnp.sin(angles)

        kchunks, nq, depth = 4, 3, 64
        kv_w = kv_rank + pe_w
        any_spec = pl.BlockSpec(memory_space=pl.ANY)
        vmem_spec = pl.BlockSpec(memory_space=pltpu.VMEM)
        dma = pltpu.SemaphoreType.DMA
        kv_all, cq_all, tab_all, wk2, wv2 = pl.pallas_call(
            functools.partial(front_kernel, ranks, mine),
            out_shape=(
                jax.ShapeDtypeStruct((seq, kv_w), BF16),
                jax.ShapeDtypeStruct((2 * rows, q_rank), BF16),
                jax.ShapeDtypeStruct((2, rot, rows), F32),
                jax.ShapeDtypeStruct((kv_rank, mine * nope), BF16),
                jax.ShapeDtypeStruct((kv_rank, mine * v_dim), BF16),
            ),
            in_specs=[any_spec] * 5 + [vmem_spec] * 4,
            out_specs=(any_spec,) * 5,
            scratch_shapes=[
                pltpu.VMEM((rows, model), BF16),
                pltpu.VMEM((kchunks, kv_rank + rot, model // kchunks), BF16),
                pltpu.VMEM((nq, model, q_rank // nq), BF16),
                pltpu.VMEM((2, kv_rank, mine, nope), BF16),
                pltpu.VMEM((2, kv_rank, mine * nope), BF16),
                pltpu.VMEM((mine // 8, depth * 8, nope), F32),
                pltpu.VMEM((rows, q_rank), F32),
                pltpu.VMEM((rows, kv_w), BF16),
                pltpu.VMEM((rows, q_rank), BF16),
                pltpu.VMEM((rot, rows), F32),
                dma((2 * kchunks + nq + 2,)),
                dma((5,)),
                dma((8,)),
                dma((8,)),
                dma((2,)),
                dma((2,)),
            ],
            compiler_params=pltpu.CompilerParams(collective_id=0, has_side_effects=True, vmem_limit_bytes=60 << 20),
            cost_estimate=pl.CostEstimate(flops=2 * rows * model * (q_rank + kv_rank + rot), bytes_accessed=2 * model * (q_rank + kv_rank + rot), transcendentals=0),
        )(tok_in, w_dkv.T, w_dq, w_uk, w_uv, g_q, g_kv, cos_t, sin_t)

        wuq_t = jnp.transpose(w_uq, (1, 2, 0))
        qn = 2 * rows
        nblk = seq // qn
        steps = mine // 4

        def whole(shape):
            return pl.BlockSpec(shape, lambda i: (0,) * len(shape))

        def up_spec(part):
            return pl.BlockSpec((2, qk_dim, q_rank), lambda i: (lax.rem(lax.axis_index("sp"), 2) * (mine // 2) + part * steps + weight_step(i, ranks, steps), 0, 0))

        def lat_spec(part):
            return pl.BlockSpec((kv_rank, 2 * nope), lambda i: (0, part * steps + weight_step(i, ranks, steps)))

        head_v = pltpu.VMEM((2, nblk, v_dim, qn), BF16)
        scores = pltpu.VMEM((2, nblk, qn, qn), F32)
        stat = pltpu.VMEM((2, 8, qn), F32)
        head_o = pltpu.VMEM((2, v_dim, qn), F32)
        rope_v = pltpu.VMEM((2, half, qn), F32)
        most = ranks // 4
        pair_o = pltpu.VMEM((most + 1, qn, 2 * v_dim), BF16)
        o_a, o_b, cache_kv, cache_pe = pl.pallas_call(
            functools.partial(attn_kernel, attn_scale * math.log2(math.e), ranks, steps),
            out_shape=(jax.ShapeDtypeStruct((qn, 2 * steps * v_dim), BF16),) * 2 + (
                jax.ShapeDtypeStruct((rows, kv_rank), BF16),
                jax.ShapeDtypeStruct((rows, rot), BF16),
            ),
            grid=(steps + most + 3,),
            in_specs=[
                any_spec,
                whole((seq, kv_w)),
                whole((2, rot, rows)),
                up_spec(0), up_spec(1), lat_spec(0), lat_spec(1), lat_spec(0), lat_spec(1),
            ],
            out_specs=(any_spec, any_spec, whole((rows, kv_rank)), whole((rows, rot))),
            scratch_shapes=[pltpu.VMEM((2, qn, q_rank), BF16), pltpu.VMEM((2, rot, rows), F32),
                            pltpu.VMEM((2, nblk, qn, nope + pe_w), BF16), head_v, head_v, pltpu.VMEM((2, nope + pe_w, qn), BF16),
                            scores, scores, stat, stat, stat, stat, head_o, head_o, rope_v, rope_v, pair_o, pair_o,
                            dma((1,)), dma((2,)), dma((2,)), dma((2,)), dma((2,)), dma((2,)), dma((most,)), dma((most,)), dma((most,)), dma((most,))],
            compiler_params=pltpu.CompilerParams(dimension_semantics=("arbitrary",), collective_id=2, has_side_effects=True, vmem_limit_bytes=62 << 20),
        )(cq_all, kv_all, tab_all, wuq_t, wuq_t, wk2, wk2, wv2, wv2)

        nc, bufs = 512, 3
        span = mine * v_dim
        pieces = model // 2 // nc
        attn_out = pl.pallas_call(
            out_kernel,
            out_shape=jax.ShapeDtypeStruct((rows, model), BF16),
            in_specs=[any_spec] * 3,
            out_specs=any_spec,
            scratch_shapes=[
                pltpu.VMEM((qn, span), BF16),
                pltpu.VMEM((qn, span), BF16),
                pltpu.VMEM((bufs, span, nc), BF16),
                pltpu.VMEM((pieces, qn, nc), F32),
                pltpu.VMEM((2, qn, nc), BF16),
                dma((2,)),
                dma((bufs,)),
                dma((2,)),
                dma((2,)),
                dma((2,)),
                dma((pieces,)),
                dma((pieces,)),
            ],
            compiler_params=pltpu.CompilerParams(collective_id=1, has_side_effects=True, vmem_limit_bytes=60 << 20),
        )(o_a, o_b, w_o.reshape(num_heads * v_dim, model))
        return attn_out, cache_kv, cache_pe

    return jax.shard_map(local_step, mesh=mesh,
                         in_specs=(rows_spec, tok_spec) + (replicated,) * 8,
                         out_specs=(rows_spec, rows_spec, rows_spec), check_vma=False)
```

```python
import functools
import math

import jax
import jax.numpy as jnp
from jax import lax
from jax.experimental import pallas as pl
from jax.experimental.pallas import tpu as pltpu
from jax.sharding import PartitionSpec as P

ROPE_THETA = 10000.0
YARN_FACTOR = 40.0
ORIG_CTX = 4096.0
BETA_FAST = 32.0
BETA_SLOW = 1.0
NORM_EPS = 1e-6

MESH = pl.DeviceIdType.MESH
F32 = jnp.float32
BF16 = jnp.bfloat16
NT = (((1,), (1,)), ((), ()))
TT = (((0,), (1,)), ((), ()))


def rope_freqs(rot_dim):
    half_dim = rot_dim // 2
    log_base = 2.0 * math.log(ROPE_THETA)
    low_idx = max(math.floor(rot_dim * math.log(ORIG_CTX / (BETA_FAST * 2.0 * math.pi)) / log_base), 0)
    high_idx = min(math.ceil(rot_dim * math.log(ORIG_CTX / (BETA_SLOW * 2.0 * math.pi)) / log_base), half_dim - 1)
    spread = max(high_idx - low_idx, 0.001)
    freq_list = []
    for freq_idx in range(half_dim):
        base_freq = ROPE_THETA ** (-2.0 * freq_idx / rot_dim)
        ramp_val = min(max((freq_idx - low_idx) / spread, 0.0), 1.0)
        freq_list.append(base_freq / YARN_FACTOR * ramp_val + base_freq * (1.0 - ramp_val))
    return jnp.asarray(freq_list, dtype=jnp.float32)


def front_kernel(ranks, heads, x_hbm, wkv_hbm, wq_hbm, wuk_hbm, wuv_hbm, gq_ref, gkv_ref, pos_ref, freq_ref,
                 kv_all, cq_all, tab_all, wk_out, wv_out,
                 x_v, wkv_v, wq_v, wu_v, wo_v, wide_v, cq_f, kv_v, cq_v, tab_v,
                 w_sem, own_sem, kv_send, kv_recv, pair_send, pair_recv):
    me = lax.axis_index("sp")
    core = lax.rem(me, 2)
    sib = me + 1 - 2 * core
    rows = x_v.shape[0]
    half = freq_ref.shape[0]
    kv_rank = gkv_ref.shape[0]
    right = lax.rem(me + 2, ranks)
    left = lax.rem(me + ranks - 2, ranks)
    across = lax.rem(me + 4, ranks)

    kchunks, nq = wkv_v.shape[0], wq_v.shape[0]
    kc = wkv_v.shape[2]
    nc = wq_v.shape[2]
    first = core * heads
    loads = []
    for k in range(kchunks):
        cols = pl.ds(k * kc, kc)
        loads.append([pltpu.make_async_copy(x_hbm.at[:, cols], x_v.at[:, cols], w_sem.at[2 * k]),
                      pltpu.make_async_copy(wkv_hbm.at[:, cols], wkv_v.at[k], w_sem.at[2 * k + 1])])
    base = 2 * kchunks
    loads += [[pltpu.make_async_copy(wq_hbm.at[:, pl.ds(k * nc, nc)], wq_v.at[k], w_sem.at[base + k])] for k in range(nq)]
    loads += [[pltpu.make_async_copy(h.at[:, pl.ds(first, heads), :], wu_v.at[k], w_sem.at[base + nq + k])]
              for k, h in enumerate((wuk_hbm, wuv_hbm))]
    ahead = 3

    def launch(i):
        if i < len(loads):
            for c in loads[i]:
                c.start()

    def arrive(i):
        for c in loads[i]:
            c.wait()
        launch(i + ahead)

    for i in range(ahead):
        launch(i)

    barrier = pltpu.get_barrier_semaphore()
    for peer in (sib, right, left):
        pl.semaphore_signal(barrier, inc=1, device_id={"sp": peer}, device_id_type=MESH)

    def block(idx):
        return kv_all.at[pl.ds(idx * rows, rows)]

    def remote(src, dst, send, recv, dev):
        return pltpu.make_async_remote_copy(src_ref=src, dst_ref=dst, send_sem=send, recv_sem=recv,
                                            device_id={"sp": dev}, device_id_type=MESH)

    acc = None
    for k in range(kchunks):
        arrive(k)
        part = lax.dot_general(x_v[:, k * kc:(k + 1) * kc], wkv_v[k], NT, preferred_element_type=F32)
        acc = part if acc is None else acc + part
    a = acc[:, :kv_rank]
    inv = lax.rsqrt(jnp.mean(a * a, axis=-1, keepdims=True) + NORM_EPS)
    ckv = (a * inv * gkv_ref[...][None, :]).astype(BF16)
    angles = freq_ref[...] * pos_ref[...].astype(F32)[None, :]
    tab_v[:half, :] = jnp.cos(angles)
    tab_v[half:, :] = jnp.sin(angles)
    tab = tab_v[...].T
    cos_t, sin_t = tab[:, :half], tab[:, half:]
    z1 = acc[:, kv_rank:kv_rank + half]
    z2 = acc[:, kv_rank + half:]
    pe = jnp.concatenate([z1 * cos_t - z2 * sin_t, z2 * cos_t + z1 * sin_t], axis=-1).astype(BF16)
    kv_v[:, :kv_rank] = ckv
    kv_v[:, kv_rank:] = jnp.concatenate([pe, jnp.zeros((rows, kv_v.shape[1] - kv_rank - 2 * half), BF16)], axis=-1)

    pl.semaphore_wait(barrier, 3)
    mid = rows // 2

    def piece(h):
        return pl.ds(h * mid, mid)

    def part(idx, h):
        return kv_all.at[pl.ds(idx * rows + h * mid, mid)]

    to_sib = remote(kv_v, block(me), kv_send.at[0], kv_recv.at[0], sib)
    to_right = [remote(kv_v.at[piece(h)], part(me, h), kv_send.at[1 + h], kv_recv.at[1 + h], right) for h in range(2)]
    to_left = [remote(kv_v.at[piece(h)], part(me, h), kv_send.at[3 + h], kv_recv.at[3 + h], left) for h in range(2)]
    tab_copy = remote(tab_v, tab_all.at[core], pair_send.at[0], pair_recv.at[0], sib)
    for c in (to_right[0], to_left[1], to_right[1], to_left[0], to_sib, tab_copy):
        c.start()
    own = [pltpu.make_async_copy(kv_v, block(me), own_sem.at[0]),
           pltpu.make_async_copy(tab_v, tab_all.at[core], own_sem.at[1])]
    for c in own:
        c.start()

    ssq = jnp.zeros((rows, 1), F32)
    for k in range(nq):
        arrive(kchunks + k)
        q = jnp.dot(x_v[...], wq_v[k], preferred_element_type=F32)
        cq_f[:, k * nc:(k + 1) * nc] = q
        ssq = ssq + jnp.sum(q * q, axis=-1, keepdims=True)
    inv_q = lax.rsqrt(ssq / cq_f.shape[1] + NORM_EPS)
    cq_v[...] = (cq_f[...] * inv_q * gq_ref[...][None, :]).astype(BF16)
    cq_copy = remote(cq_v, cq_all.at[pl.ds(core * rows, rows)], pair_send.at[1], pair_recv.at[1], sib)
    cq_copy.start()
    own.append(pltpu.make_async_copy(cq_v, cq_all.at[pl.ds(core * rows, rows)], own_sem.at[2]))
    own[-1].start()

    to_right[0].wait_recv()
    half_right = remote(part(left, 0), part(left, 0), kv_send.at[5], kv_recv.at[5], right)
    half_right.start()
    to_left[1].wait_recv()
    half_left = remote(part(right, 1), part(right, 1), kv_send.at[6], kv_recv.at[6], left)
    half_left.start()

    depth = wide_v.shape[1] // 8
    groups = wide_v.shape[0]
    width = wide_v.shape[2]

    def up_relayout(t, out):
        arrive(kchunks + nq + t)

        def relayout(i, carry):
            base = pl.multiple_of(i * depth, depth)
            for g in range(groups):
                wide_v[g] = wu_v[t, pl.ds(base, depth), g * 8:(g + 1) * 8, :].astype(F32).reshape(depth * 8, width)
            for g in range(groups):
                for h in range(8):
                    col = (g * 8 + h) * width
                    wo_v[t, pl.ds(base, depth), col:col + width] = wide_v[g, pl.ds(h, depth, stride=8), :].astype(BF16)
            return carry

        lax.fori_loop(0, wu_v.shape[1] // depth, relayout, 0)
        own.append(pltpu.make_async_copy(wo_v.at[t], out, own_sem.at[3 + t]))
        own[-1].start()

    up_relayout(0, wk_out)
    to_right[1].wait_recv()
    sib_left = remote(block(left), block(left), kv_send.at[7], kv_recv.at[7], sib)
    sib_left.start()
    to_left[0].wait_recv()
    sib_right = remote(block(right), block(right), kv_send.at[8], kv_recv.at[8], sib)
    sib_right.start()
    up_relayout(1, wv_out)
    half_right.wait_recv()
    sib_across0 = remote(part(across, 0), part(across, 0), kv_send.at[9], kv_recv.at[9], sib)
    sib_across0.start()
    half_left.wait_recv()
    sib_across1 = remote(part(across, 1), part(across, 1), kv_send.at[10], kv_recv.at[10], sib)
    sib_across1.start()
    to_sib.wait()
    for c in to_right + to_left + [half_right, half_left]:
        c.wait_send()
    for c in (sib_left, sib_right, sib_across0, sib_across1, tab_copy, cq_copy):
        c.wait()
    for c in own:
        c.wait()


def shares(me, ranks, steps):
    chips = ranks // 2
    chip = me // 2
    give = jnp.maximum(chip - chips // 2 + 1, 0)
    take = jnp.maximum(chips // 2 - chip, 0)
    lead = jnp.where(take > 0, steps // 2 + take - 1, steps - give)
    return chip, lead, take, give


def weight_step(i, ranks, steps):
    _, lead, take, _ = shares(lax.axis_index("sp"), ranks, steps)
    far = steps - take + jnp.minimum(i - lead - 1, take - 1)
    late = jnp.where(i <= lead + take + 1, far, jnp.minimum(i - take - 2, steps - 1))
    return jnp.where((i <= lead) | (take == 0), jnp.minimum(i, lead - 1), late)


def attn_kernel(scale2, ranks, steps, cq_hbm, kv_ref, tab_ref,
                wqa_ref, wqb_ref, wka_ref, wkb_ref, wva_ref, wvb_ref, oa_hbm, ob_hbm, ckv_ref, cpe_ref,
                cq_v, tab_v, k_v, v_a, v_b, q_v, s_a, s_b, m_a, m_b, l_a, l_b, o_a, o_b, cosq_ref, sinq_ref, oa_v, ob_v,
                cq_sem, lat_send, lat_recv, fwd_send, fwd_recv, o_sem, oa_send, ob_send, oa_recv, ob_recv):
    step = pl.program_id(0)
    final = pl.num_programs(0) - 1
    me = lax.axis_index("sp")
    core = lax.rem(me, 2)
    sib = me + 1 - 2 * core
    chip, lead, take, give = shares(me, ranks, steps)
    taker = take > 0
    far_chip = ranks // 2 - 1 - chip
    far = 2 * far_chip + core
    most = oa_recv.shape[0]
    is_far = (step > lead) & (step <= lead + take + 1) & taker
    qset = jnp.where(is_far, 1, 0)
    full = jnp.where(is_far, far_chip, chip)
    _, blocks, blk, kdim = k_v.shape
    kv_rank = wka_ref.shape[0]
    nope = wka_ref.shape[1] // 2
    half = cosq_ref.shape[1]
    rot = 2 * half
    sub = blk // 2
    everything = slice(None)
    my_rows = pl.ds(pl.multiple_of(core * sub, sub), sub)

    lat = [pltpu.make_async_remote_copy(src_ref=src, dst_ref=dst, send_sem=lat_send.at[k], recv_sem=lat_recv.at[k],
                                        device_id={"sp": far}, device_id_type=MESH)
           for k, (src, dst) in enumerate(((cq_hbm.at[my_rows], cq_v.at[1, my_rows]), (tab_ref.at[core], tab_v.at[core])))]
    fwd = [pltpu.make_async_remote_copy(src_ref=ref, dst_ref=ref, send_sem=fwd_send.at[k], recv_sem=fwd_recv.at[k],
                                        device_id={"sp": sib}, device_id_type=MESH)
           for k, ref in enumerate((cq_v.at[1, my_rows], tab_v.at[core]))]

    def o_cols(at):
        return pl.ds(pl.multiple_of(at * 2 * nope, 2 * nope), 2 * nope)

    def o_local(part, s):
        src, dst = ((oa_v, oa_hbm), (ob_v, ob_hbm))[part]
        at = jnp.where(s <= lead, s - 1, s - take - 3)
        return pltpu.make_async_copy(src.at[most], dst.at[:, o_cols(at)], o_sem.at[part])

    def o_far(part, r):
        src, dst, send, recv = ((oa_v, oa_hbm, oa_send, oa_recv), (ob_v, ob_hbm, ob_send, ob_recv))[part]
        return pltpu.make_async_remote_copy(src_ref=src.at[r], dst_ref=dst.at[:, o_cols(steps - 1 - r)], send_sem=send.at[r], recv_sem=recv.at[r],
                                            device_id={"sp": far}, device_id_type=MESH)

    def left_own(s):
        return ((s >= 1) & (s <= lead)) | (taker & (s >= lead + take + 3) & (s <= steps + take + 2))

    def left_far(s):
        return taker & (s >= lead + 2) & (s <= lead + take + 1)

    far_slot = lead + take + 1 - step
    slot = jnp.where(left_far(step), far_slot, most)

    def emit(part):
        @pl.when(left_own(step))
        def _():
            o_local(part, step).start()

        @pl.when(left_far(step))
        def _():
            o_far(part, far_slot).start()

    def settle(part, s):
        @pl.when(left_own(s))
        def _():
            o_local(part, s).wait()

    @pl.when(step == 0)
    def _():
        own_cq = pltpu.make_async_copy(cq_hbm, cq_v.at[0], cq_sem.at[0])
        own_cq.start()
        barrier = pltpu.get_barrier_semaphore()
        for peer in (sib, far):
            pl.semaphore_signal(barrier, inc=1, device_id={"sp": peer}, device_id_type=MESH)
        pl.semaphore_wait(barrier, 2)

        @pl.when(give > 0)
        def _():
            for c in lat:
                c.start()

        for kb in range(blocks):
            pe = kv_ref[kb * blk:(kb + 1) * blk, kv_rank:]
            k_v[0, kb, :, nope:] = pe
            k_v[1, kb, :, nope:] = pe
        q_v[:, nope + rot:, :] = jnp.zeros((2, kdim - nope - rot, blk), BF16)
        for c in range(2):
            cosq_ref[0, :, c * sub:(c + 1) * sub] = tab_ref[c, :half, :]
            sinq_ref[0, :, c * sub:(c + 1) * sub] = tab_ref[c, half:, :]
        rows = ckv_ref.shape[0]
        own = kv_ref[pl.ds(pl.multiple_of(me * rows, rows), rows), :]
        ckv_ref[...] = own[:, :kv_rank]
        cpe_ref[...] = own[:, kv_rank:kv_rank + rot]
        own_cq.wait()

    @pl.when(step > 0)
    def _():
        for part in range(2):
            settle(part, step - 1)

    @pl.when((step == lead) & taker)
    def _():
        for c in lat:
            c.wait_recv()
        for c in fwd:
            c.start()

    @pl.when((step == lead + 1) & taker)
    def _():
        for c in fwd:
            c.wait()
        for c in range(2):
            cosq_ref[1, :, c * sub:(c + 1) * sub] = tab_v[c, :half, :]
            sinq_ref[1, :, c * sub:(c + 1) * sub] = tab_v[c, half:, :]

    def q_proj(w_ref):
        w = jnp.concatenate([w_ref[0], w_ref[1]], axis=0)
        both = lax.dot_general(w, cq_v[qset], NT, preferred_element_type=F32)
        cos_t, sin_t = cosq_ref[qset], sinq_ref[qset]
        for h in range(2):
            u = both[h * (nope + rot):(h + 1) * (nope + rot)]
            q_v[h, :nope, :] = u[:nope].astype(BF16)
            z1 = u[nope:nope + half]
            z2 = u[nope + half:]
            q_v[h, nope:nope + half, :] = (z1 * cos_t - z2 * sin_t).astype(BF16)
            q_v[h, nope + half:nope + rot, :] = (z2 * cos_t + z1 * sin_t).astype(BF16)

    def kv_proj(kb, wk, wv, v_ref):
        c = kv_ref[pl.ds(pl.multiple_of(kb * blk, blk), blk), :kv_rank]
        k = jnp.dot(c, wk, preferred_element_type=F32).astype(BF16)
        v = lax.dot_general(wv, c, NT, preferred_element_type=F32).astype(BF16)
        for h in range(2):
            k_v[h, kb, :, :nope] = k[:, h * nope:(h + 1) * nope]
            v_ref[h, kb] = v[h * nope:(h + 1) * nope]

    def fold_max(m_ref, h, s, cols):
        t = jnp.max(s.reshape(s.shape[0] // 8, 8, s.shape[1]), axis=0)
        m_ref[h, :, cols] = jnp.maximum(m_ref[h, :, cols], t)

    def qk(h, kb, s_ref, m_ref):
        s = jnp.dot(k_v[h, kb], q_v[h], preferred_element_type=F32)
        s_ref[h, kb] = s
        fold_max(m_ref, h, s, everything)

    def qk_diag(h, kb, s_ref, m_ref):
        s0 = jnp.dot(k_v[h, kb, :sub, :], q_v[h], preferred_element_type=F32)
        s1 = jnp.dot(k_v[h, kb, sub:, :], q_v[h, :, sub:], preferred_element_type=F32)
        keep = lax.broadcasted_iota(jnp.int32, (sub, sub), 0) <= lax.broadcasted_iota(jnp.int32, (sub, sub), 1)
        s00 = jnp.where(keep, s0[:, :sub], -jnp.inf)
        s1 = jnp.where(keep, s1, -jnp.inf)
        s01 = s0[:, sub:]
        s_ref[h, kb, :sub, :sub] = s00
        s_ref[h, kb, :sub, sub:] = s01
        s_ref[h, kb, sub:, sub:] = s1
        fold_max(m_ref, h, s00, slice(0, sub))
        fold_max(m_ref, h, s01, slice(sub, blk))
        fold_max(m_ref, h, s1, slice(sub, blk))

    def fold_sum(l_ref, h, p, cols):
        l_ref[h, :, cols] += jnp.sum(p.reshape(p.shape[0] // 8, 8, p.shape[1]), axis=0)

    def top(m_ref):
        return [jnp.max(m_ref[h], axis=0, keepdims=True) for h in range(2)]

    def pv(h, kb, v_ref, s_ref, m, l_ref, o_ref):
        p = jnp.exp2((s_ref[h, kb] - m[h]) * scale2)
        fold_sum(l_ref, h, p, everything)
        o_ref[h] += jnp.dot(v_ref[h, kb], p.astype(BF16), preferred_element_type=F32)

    def pv_diag(h, kb, v_ref, s_ref, m, l_ref, o_ref):
        p0 = jnp.exp2((s_ref[h, kb, :sub, :] - m[h]) * scale2)
        p1 = jnp.exp2((s_ref[h, kb, sub:, sub:] - m[h][:, sub:]) * scale2)
        fold_sum(l_ref, h, p0, everything)
        fold_sum(l_ref, h, p1, slice(sub, blk))
        p0 = p0.astype(BF16)
        o_ref[h] += jnp.dot(v_ref[h, kb, :, :sub], p0, preferred_element_type=F32)
        o_ref[h, :, sub:] += jnp.dot(v_ref[h, kb, :, sub:], p1.astype(BF16), preferred_element_type=F32)

    def finish(l_ref, o_ref, out_ref):
        for h in range(2):
            l = jnp.sum(l_ref[h], axis=0, keepdims=True)
            out_ref[slot, :, h * nope:(h + 1) * nope] = (o_ref[h] / l).T.astype(BF16)

    def clear(l_ref, o_ref):
        l_ref[...] = jnp.zeros_like(l_ref)
        o_ref[...] = jnp.zeros_like(o_ref)

    def stage(wq_ref, wk_ref, wv_ref, new, old, done, done_out, part):
        s_n, m_n, v_n = new
        s_o, m_o, v_o, l_o, out_o = old
        m = top(m_o)
        q_proj(wq_ref)
        finish(done[0], done[1], done_out)
        emit(part)
        clear(l_o, out_o)
        m_n[...] = jnp.full_like(m_n, -jnp.inf)
        wk = wk_ref[...]
        wv = wv_ref[...].T

        def body(kb, carry):
            kv_proj(kb, wk, wv, v_n)
            for h in range(2):
                pv(h, kb, v_o, s_o, m, l_o, out_o)
                qk(h, kb, s_n, m_n)
            return carry

        lax.fori_loop(0, full, body, 0)
        kv_proj(full, wk, wv, v_n)
        for h in range(2):
            pv_diag(h, full, v_o, s_o, m, l_o, out_o)
            qk_diag(h, full, s_n, m_n)

    @pl.when((step < lead) | (taker & (step > lead) & (step != lead + take + 1) & (step < steps + take + 2)))
    def _():
        stage(wqa_ref, wka_ref, wva_ref, (s_a, m_a, v_a), (s_b, m_b, v_b, l_b, o_b), (l_a, o_a), oa_v, 0)
        stage(wqb_ref, wkb_ref, wvb_ref, (s_b, m_b, v_b), (s_a, m_a, v_a, l_a, o_a), (l_b, o_b), ob_v, 1)

    @pl.when((step == lead) | (taker & ((step == lead + take + 1) | (step == steps + take + 2))))
    def _():
        m = top(m_b)
        clear(l_b, o_b)
        finish(l_a, o_a, oa_v)
        emit(0)

        def body(kb, carry):
            for h in range(2):
                pv(h, kb, v_b, s_b, m, l_b, o_b)
            return carry

        lax.fori_loop(0, full, body, 0)
        for h in range(2):
            pv_diag(h, full, v_b, s_b, m, l_b, o_b)
        finish(l_b, o_b, ob_v)
        emit(1)

    @pl.when(step == final)
    def _():
        for part in range(2):
            settle(part, step)

        @pl.when(give > 0)
        def _():
            for c in lat:
                c.wait_send()

        for r in range(most):
            @pl.when(give > r)
            def _(r=r):
                for part in range(2):
                    o_far(part, r).wait_recv()

            @pl.when(take > r)
            def _(r=r):
                for part in range(2):
                    o_far(part, r).wait_send()


def out_kernel(oa_hbm, ob_hbm, wo_hbm, out_hbm, own_v, sib_v, w_v, acc_v, out_v,
               o_sem, lead_sem, w_sem, out_sem, swap_send, swap_recv, res_send, res_recv):
    me = lax.axis_index("sp")
    core = lax.rem(me, 2)
    sib = me + 1 - 2 * core
    wide = oa_hbm.shape[1]
    span = own_v.shape[1]
    rows = out_hbm.shape[0]
    bufs, _, nc = w_v.shape
    steps = acc_v.shape[0]

    def fetch(i):
        part = i // steps
        owner = core + part - 2 * core * part
        col = core * (steps * nc) + lax.rem(i, steps) * nc
        slot = lax.rem(i, bufs)
        return pltpu.make_async_copy(
            wo_hbm.at[pl.ds(pl.multiple_of(owner * span, span), span), pl.ds(pl.multiple_of(col, nc), nc)],
            w_v.at[slot], w_sem.at[slot])

    own = [pltpu.make_async_copy(h, own_v.at[:, pl.ds(k * wide, wide)], o_sem.at[k])
           for k, h in enumerate((oa_hbm, ob_hbm))]
    lead = [pltpu.make_async_copy(
        wo_hbm.at[pl.ds(pl.multiple_of(core * span + k * wide, wide), wide), pl.ds(pl.multiple_of(core * (steps * nc), nc), nc)],
        w_v.at[0, pl.ds(k * wide, wide)], lead_sem.at[k]) for k in range(2)]
    for k in range(2):
        own[k].start()
        lead[k].start()

    barrier = pltpu.get_barrier_semaphore()
    pl.semaphore_signal(barrier, inc=1, device_id={"sp": sib}, device_id_type=MESH)
    swap = [pltpu.make_async_remote_copy(
        src_ref=h, dst_ref=sib_v.at[:, pl.ds(k * wide, wide)],
        send_sem=swap_send.at[k], recv_sem=swap_recv.at[k], device_id={"sp": sib}, device_id_type=MESH)
        for k, h in enumerate((oa_hbm, ob_hbm))]
    own[0].wait()
    lead[0].wait()
    fetch(1).start()
    acc_v[0] = jnp.dot(own_v[:, :wide], w_v[0, :wide, :], preferred_element_type=F32)
    own[1].wait()
    lead[1].wait()
    fetch(2).start()
    pl.semaphore_wait(barrier, 1)
    for c in swap:
        c.start()
    acc_v[0] += jnp.dot(own_v[:, wide:], w_v[0, wide:, :], preferred_element_type=F32)

    def own_half(i, carry):
        fetch(i).wait()
        fetch(i + 2).start()
        acc_v[i] = jnp.dot(own_v[...], w_v[lax.rem(i, bufs)], preferred_element_type=F32)
        return carry

    lax.fori_loop(1, steps, own_half, 0)
    for c in swap:
        c.wait()

    def store(n):
        slot = lax.rem(n, 2)
        cols = pl.ds(pl.multiple_of(core * (steps * nc) + n * nc, nc), nc)
        keep = pltpu.make_async_copy(out_v.at[slot, pl.ds(pl.multiple_of(core * rows, rows), rows)],
                                     out_hbm.at[:, cols], out_sem.at[slot])
        give = pltpu.make_async_remote_copy(
            src_ref=out_v.at[slot, pl.ds(pl.multiple_of((1 - core) * rows, rows), rows)], dst_ref=out_hbm.at[:, cols],
            send_sem=res_send.at[n], recv_sem=res_recv.at[n], device_id={"sp": sib}, device_id_type=MESH)
        return keep, give

    def sib_half(n, carry):
        i = n + steps
        fetch(i).wait()

        @pl.when(i + 2 < 2 * steps)
        def _():
            fetch(i + 2).start()

        @pl.when(n >= 2)
        def _():
            keep, give = store(n - 2)
            keep.wait()
            give.wait_send()

        out_v[lax.rem(n, 2)] = (acc_v[n] + jnp.dot(sib_v[...], w_v[lax.rem(i, bufs)], preferred_element_type=F32)).astype(BF16)
        for c in store(n):
            c.start()
        return carry

    lax.fori_loop(0, steps, sib_half, 0)
    for n in range(steps - 2, steps):
        keep, give = store(n)
        keep.wait()
        give.wait_send()
    for n in range(steps):
        store(n)[1].wait_recv()


def solution(mesh):
    ranks = mesh.shape["sp"]
    tok_spec = P(("dp", "sp"))
    rows_spec = P(("dp", "sp"), None)
    replicated = P()

    def local_step(tok_in, tok_pos, w_dq, g_q, w_uq, w_dkv, g_kv, w_uk, w_uv, w_o):
        rows, model = tok_in.shape
        num_heads = w_uq.shape[1]
        qk_dim = w_uq.shape[2]
        q_rank = w_dq.shape[1]
        kv_rank = g_kv.shape[0]
        rot = w_dkv.shape[1] - kv_rank
        nope = qk_dim - rot
        v_dim = w_uv.shape[2]
        seq = rows * ranks
        half = rot // 2
        mine = num_heads // 2
        pe_w = 128
        attn_scale = (0.1 * math.log(YARN_FACTOR) + 1.0) ** 2 / math.sqrt(qk_dim)
        kchunks, nq, depth = 4, 3, 64
        kv_w = kv_rank + pe_w
        any_spec = pl.BlockSpec(memory_space=pl.ANY)
        vmem_spec = pl.BlockSpec(memory_space=pltpu.VMEM)
        dma = pltpu.SemaphoreType.DMA
        kv_all, cq_all, tab_all, wk2, wv2 = pl.pallas_call(
            functools.partial(front_kernel, ranks, mine),
            out_shape=(
                jax.ShapeDtypeStruct((seq, kv_w), BF16),
                jax.ShapeDtypeStruct((2 * rows, q_rank), BF16),
                jax.ShapeDtypeStruct((2, rot, rows), F32),
                jax.ShapeDtypeStruct((kv_rank, mine * nope), BF16),
                jax.ShapeDtypeStruct((kv_rank, mine * v_dim), BF16),
            ),
            in_specs=[any_spec] * 5 + [vmem_spec] * 4,
            out_specs=(any_spec,) * 5,
            scratch_shapes=[
                pltpu.VMEM((rows, model), BF16),
                pltpu.VMEM((kchunks, kv_rank + rot, model // kchunks), BF16),
                pltpu.VMEM((nq, model, q_rank // nq), BF16),
                pltpu.VMEM((2, kv_rank, mine, nope), BF16),
                pltpu.VMEM((2, kv_rank, mine * nope), BF16),
                pltpu.VMEM((mine // 8, depth * 8, nope), F32),
                pltpu.VMEM((rows, q_rank), F32),
                pltpu.VMEM((rows, kv_w), BF16),
                pltpu.VMEM((rows, q_rank), BF16),
                pltpu.VMEM((rot, rows), F32),
                dma((2 * kchunks + nq + 2,)),
                dma((5,)),
                dma((11,)),
                dma((11,)),
                dma((2,)),
                dma((2,)),
            ],
            compiler_params=pltpu.CompilerParams(collective_id=0, has_side_effects=True, vmem_limit_bytes=60 << 20),
            cost_estimate=pl.CostEstimate(flops=2 * rows * model * (q_rank + kv_rank + rot), bytes_accessed=2 * model * (q_rank + kv_rank + rot), transcendentals=0),
        )(tok_in, w_dkv.T, w_dq, w_uk, w_uv, g_q, g_kv, tok_pos, rope_freqs(rot)[:, None])

        wuq_t = jnp.transpose(w_uq, (1, 2, 0))
        qn = 2 * rows
        nblk = seq // qn
        steps = mine // 4

        def whole(shape):
            return pl.BlockSpec(shape, lambda i: (0,) * len(shape))

        def up_spec(part):
            return pl.BlockSpec((2, qk_dim, q_rank), lambda i: (lax.rem(lax.axis_index("sp"), 2) * (mine // 2) + part * steps + weight_step(i, ranks, steps), 0, 0))

        def lat_spec(part):
            return pl.BlockSpec((kv_rank, 2 * nope), lambda i: (0, part * steps + weight_step(i, ranks, steps)))

        head_v = pltpu.VMEM((2, nblk, v_dim, qn), BF16)
        scores = pltpu.VMEM((2, nblk, qn, qn), F32)
        stat = pltpu.VMEM((2, 8, qn), F32)
        head_o = pltpu.VMEM((2, v_dim, qn), F32)
        rope_v = pltpu.VMEM((2, half, qn), F32)
        most = ranks // 4
        pair_o = pltpu.VMEM((most + 1, qn, 2 * v_dim), BF16)
        o_a, o_b, cache_kv, cache_pe = pl.pallas_call(
            functools.partial(attn_kernel, attn_scale * math.log2(math.e), ranks, steps),
            out_shape=(jax.ShapeDtypeStruct((qn, 2 * steps * v_dim), BF16),) * 2 + (
                jax.ShapeDtypeStruct((rows, kv_rank), BF16),
                jax.ShapeDtypeStruct((rows, rot), BF16),
            ),
            grid=(steps + most + 3,),
            in_specs=[
                any_spec,
                whole((seq, kv_w)),
                whole((2, rot, rows)),
                up_spec(0), up_spec(1), lat_spec(0), lat_spec(1), lat_spec(0), lat_spec(1),
            ],
            out_specs=(any_spec, any_spec, whole((rows, kv_rank)), whole((rows, rot))),
            scratch_shapes=[pltpu.VMEM((2, qn, q_rank), BF16), pltpu.VMEM((2, rot, rows), F32),
                            pltpu.VMEM((2, nblk, qn, nope + pe_w), BF16), head_v, head_v, pltpu.VMEM((2, nope + pe_w, qn), BF16),
                            scores, scores, stat, stat, stat, stat, head_o, head_o, rope_v, rope_v, pair_o, pair_o,
                            dma((1,)), dma((2,)), dma((2,)), dma((2,)), dma((2,)), dma((2,)), dma((most,)), dma((most,)), dma((most,)), dma((most,))],
            compiler_params=pltpu.CompilerParams(dimension_semantics=("arbitrary",), collective_id=2, has_side_effects=True, vmem_limit_bytes=62 << 20),
        )(cq_all, kv_all, tab_all, wuq_t, wuq_t, wk2, wk2, wv2, wv2)

        nc, bufs = 512, 3
        span = mine * v_dim
        pieces = model // 2 // nc
        attn_out = pl.pallas_call(
            out_kernel,
            out_shape=jax.ShapeDtypeStruct((rows, model), BF16),
            in_specs=[any_spec] * 3,
            out_specs=any_spec,
            scratch_shapes=[
                pltpu.VMEM((qn, span), BF16),
                pltpu.VMEM((qn, span), BF16),
                pltpu.VMEM((bufs, span, nc), BF16),
                pltpu.VMEM((pieces, qn, nc), F32),
                pltpu.VMEM((2, qn, nc), BF16),
                dma((2,)),
                dma((2,)),
                dma((bufs,)),
                dma((2,)),
                dma((2,)),
                dma((2,)),
                dma((pieces,)),
                dma((pieces,)),
            ],
            compiler_params=pltpu.CompilerParams(collective_id=1, has_side_effects=True, vmem_limit_bytes=60 << 20),
        )(o_a, o_b, w_o.reshape(num_heads * v_dim, model))
        return attn_out, cache_kv, cache_pe

    return jax.shard_map(local_step, mesh=mesh,
                         in_specs=(rows_spec, tok_spec) + (replicated,) * 8,
                         out_specs=(rows_spec, rows_spec, rows_spec), check_vma=False)
```

```python
import functools
import math

import jax
import jax.numpy as jnp
from jax import lax
from jax.experimental import pallas as pl
from jax.experimental.pallas import tpu as pltpu
from jax.sharding import PartitionSpec as P

ROPE_THETA = 10000.0
YARN_FACTOR = 40.0
ORIG_CTX = 4096.0
BETA_FAST = 32.0
BETA_SLOW = 1.0
NORM_EPS = 1e-6

MESH = pl.DeviceIdType.MESH
F32 = jnp.float32
BF16 = jnp.bfloat16
NT = (((1,), (1,)), ((), ()))
TT = (((0,), (1,)), ((), ()))


def rope_freqs(rot_dim):
    half_dim = rot_dim // 2
    log_base = 2.0 * math.log(ROPE_THETA)
    low_idx = max(math.floor(rot_dim * math.log(ORIG_CTX / (BETA_FAST * 2.0 * math.pi)) / log_base), 0)
    high_idx = min(math.ceil(rot_dim * math.log(ORIG_CTX / (BETA_SLOW * 2.0 * math.pi)) / log_base), half_dim - 1)
    spread = max(high_idx - low_idx, 0.001)
    freq_list = []
    for freq_idx in range(half_dim):
        base_freq = ROPE_THETA ** (-2.0 * freq_idx / rot_dim)
        ramp_val = min(max((freq_idx - low_idx) / spread, 0.0), 1.0)
        freq_list.append(base_freq / YARN_FACTOR * ramp_val + base_freq * (1.0 - ramp_val))
    return jnp.asarray(freq_list, dtype=jnp.float32)


def front_kernel(ranks, heads, x_hbm, wkv_hbm, wq_hbm, wuk_hbm, wuv_hbm, gq_ref, gkv_ref, pos_ref, freq_ref,
                 kv_all, cq_all, tab_all, wk_out, wv_out,
                 x_v, wkv_v, wq_v, wu_v, wo_v, wide_v, cq_f, kv_v, cq_v, tab_v,
                 w_sem, own_sem, kv_send, kv_recv, pair_send, pair_recv):
    me = lax.axis_index("sp")
    core = lax.rem(me, 2)
    sib = me + 1 - 2 * core
    rows = x_v.shape[0]
    half = freq_ref.shape[0]
    kv_rank = gkv_ref.shape[0]
    right = lax.rem(me + 2, ranks)
    left = lax.rem(me + ranks - 2, ranks)
    across = lax.rem(me + 4, ranks)

    kchunks, nq = wkv_v.shape[0], wq_v.shape[0]
    kc = wkv_v.shape[2]
    nc = wq_v.shape[2]
    first = core * heads
    loads = []
    for k in range(kchunks):
        cols = pl.ds(k * kc, kc)
        loads.append([pltpu.make_async_copy(x_hbm.at[:, cols], x_v.at[:, cols], w_sem.at[2 * k]),
                      pltpu.make_async_copy(wkv_hbm.at[:, cols], wkv_v.at[k], w_sem.at[2 * k + 1])])
    base = 2 * kchunks
    loads += [[pltpu.make_async_copy(wq_hbm.at[:, pl.ds(k * nc, nc)], wq_v.at[k], w_sem.at[base + k])] for k in range(nq)]
    loads += [[pltpu.make_async_copy(h.at[:, pl.ds(first, heads), :], wu_v.at[k], w_sem.at[base + nq + k])]
              for k, h in enumerate((wuk_hbm, wuv_hbm))]
    ahead = 3

    def launch(i):
        if i < len(loads):
            for c in loads[i]:
                c.start()

    def arrive(i):
        for c in loads[i]:
            c.wait()
        launch(i + ahead)

    for i in range(ahead):
        launch(i)

    barrier = pltpu.get_barrier_semaphore()
    for peer in (sib, right, left):
        pl.semaphore_signal(barrier, inc=1, device_id={"sp": peer}, device_id_type=MESH)

    def block(idx):
        return kv_all.at[pl.ds(idx * rows, rows)]

    def remote(src, dst, send, recv, dev):
        return pltpu.make_async_remote_copy(src_ref=src, dst_ref=dst, send_sem=send, recv_sem=recv,
                                            device_id={"sp": dev}, device_id_type=MESH)

    acc = None
    for k in range(kchunks):
        arrive(k)
        part = lax.dot_general(x_v[:, k * kc:(k + 1) * kc], wkv_v[k], NT, preferred_element_type=F32)
        acc = part if acc is None else acc + part
    a = acc[:, :kv_rank]
    inv = lax.rsqrt(jnp.mean(a * a, axis=-1, keepdims=True) + NORM_EPS)
    ckv = (a * inv * gkv_ref[...][None, :]).astype(BF16)
    angles = freq_ref[...] * pos_ref[...].astype(F32)[None, :]
    tab_v[:half, :] = jnp.cos(angles)
    tab_v[half:, :] = jnp.sin(angles)
    tab = tab_v[...].T
    cos_t, sin_t = tab[:, :half], tab[:, half:]
    z1 = acc[:, kv_rank:kv_rank + half]
    z2 = acc[:, kv_rank + half:]
    pe = jnp.concatenate([z1 * cos_t - z2 * sin_t, z2 * cos_t + z1 * sin_t], axis=-1).astype(BF16)
    kv_v[:, :kv_rank] = ckv
    kv_v[:, kv_rank:] = jnp.concatenate([pe, jnp.zeros((rows, kv_v.shape[1] - kv_rank - 2 * half), BF16)], axis=-1)

    pl.semaphore_wait(barrier, 3)
    mid = rows // 2

    def piece(h):
        return pl.ds(h * mid, mid)

    def part(idx, h):
        return kv_all.at[pl.ds(idx * rows + h * mid, mid)]

    to_sib = remote(kv_v, block(me), kv_send.at[0], kv_recv.at[0], sib)
    to_right = [remote(kv_v.at[piece(h)], part(me, h), kv_send.at[1 + h], kv_recv.at[1 + h], right) for h in range(2)]
    to_left = [remote(kv_v.at[piece(h)], part(me, h), kv_send.at[3 + h], kv_recv.at[3 + h], left) for h in range(2)]
    tab_copy = remote(tab_v, tab_all.at[core], pair_send.at[0], pair_recv.at[0], sib)
    for c in (to_right[0], to_left[1], to_right[1], to_left[0], to_sib, tab_copy):
        c.start()
    own = [pltpu.make_async_copy(kv_v, block(me), own_sem.at[0]),
           pltpu.make_async_copy(tab_v, tab_all.at[core], own_sem.at[1])]
    for c in own:
        c.start()

    ssq = jnp.zeros((rows, 1), F32)
    for k in range(nq):
        arrive(kchunks + k)
        q = jnp.dot(x_v[...], wq_v[k], preferred_element_type=F32)
        cq_f[:, k * nc:(k + 1) * nc] = q
        ssq = ssq + jnp.sum(q * q, axis=-1, keepdims=True)
    inv_q = lax.rsqrt(ssq / cq_f.shape[1] + NORM_EPS)
    cq_v[...] = (cq_f[...] * inv_q * gq_ref[...][None, :]).astype(BF16)
    cq_copy = remote(cq_v, cq_all.at[pl.ds(core * rows, rows)], pair_send.at[1], pair_recv.at[1], sib)
    cq_copy.start()
    own.append(pltpu.make_async_copy(cq_v, cq_all.at[pl.ds(core * rows, rows)], own_sem.at[2]))
    own[-1].start()

    to_right[0].wait_recv()
    half_right = remote(part(left, 0), part(left, 0), kv_send.at[5], kv_recv.at[5], right)
    half_right.start()
    to_left[1].wait_recv()
    half_left = remote(part(right, 1), part(right, 1), kv_send.at[6], kv_recv.at[6], left)
    half_left.start()

    depth = wide_v.shape[1] // 8
    groups = wide_v.shape[0]
    width = wide_v.shape[2]

    def up_relayout(t, out):
        arrive(kchunks + nq + t)

        def relayout(i, carry):
            base = pl.multiple_of(i * depth, depth)
            for g in range(groups):
                wide_v[g] = wu_v[t, pl.ds(base, depth), g * 8:(g + 1) * 8, :].astype(F32).reshape(depth * 8, width)
            for g in range(groups):
                for h in range(8):
                    col = (g * 8 + h) * width
                    wo_v[t, pl.ds(base, depth), col:col + width] = wide_v[g, pl.ds(h, depth, stride=8), :].astype(BF16)
            return carry

        lax.fori_loop(0, wu_v.shape[1] // depth, relayout, 0)
        own.append(pltpu.make_async_copy(wo_v.at[t], out, own_sem.at[3 + t]))
        own[-1].start()

    up_relayout(0, wk_out)
    to_right[1].wait_recv()
    sib_left = remote(block(left), block(left), kv_send.at[7], kv_recv.at[7], sib)
    sib_left.start()
    to_left[0].wait_recv()
    sib_right = remote(block(right), block(right), kv_send.at[8], kv_recv.at[8], sib)
    sib_right.start()
    up_relayout(1, wv_out)
    half_right.wait_recv()
    sib_across0 = remote(part(across, 0), part(across, 0), kv_send.at[9], kv_recv.at[9], sib)
    sib_across0.start()
    half_left.wait_recv()
    sib_across1 = remote(part(across, 1), part(across, 1), kv_send.at[10], kv_recv.at[10], sib)
    sib_across1.start()
    to_sib.wait()
    for c in to_right + to_left + [half_right, half_left]:
        c.wait_send()
    for c in (sib_left, sib_right, sib_across0, sib_across1, tab_copy, cq_copy):
        c.wait()
    for c in own:
        c.wait()


def shares(me, ranks, steps):
    chips = ranks // 2
    chip = me // 2
    give = jnp.maximum(chip - chips // 2 + 1, 0)
    take = jnp.maximum(chips // 2 - chip, 0)
    lead = jnp.where(take > 0, steps // 2 + take - 1, steps - give)
    return chip, lead, take, give


def weight_step(i, ranks, steps):
    _, lead, take, _ = shares(lax.axis_index("sp"), ranks, steps)
    far = steps - take + jnp.minimum(i - lead - 1, take - 1)
    late = jnp.where(i <= lead + take + 1, far, jnp.minimum(i - take - 2, steps - 1))
    return jnp.where((i <= lead) | (take == 0), jnp.minimum(i, lead - 1), late)


def attn_kernel(scale2, ranks, steps, cq_ref, kv_ref, tab_ref,
                wqa_ref, wqb_ref, wka_ref, wkb_ref, wva_ref, wvb_ref, oa_hbm, ob_hbm,
                cq_v, tab_v, k_v, v_a, v_b, q_v, s_a, s_b, m_a, m_b, l_a, l_b, o_a, o_b, cosq_ref, sinq_ref, oa_v, ob_v,
                lat_send, lat_recv, fwd_send, fwd_recv, o_sem, oa_send, ob_send, oa_recv, ob_recv):
    step = pl.program_id(0)
    final = pl.num_programs(0) - 1
    me = lax.axis_index("sp")
    core = lax.rem(me, 2)
    sib = me + 1 - 2 * core
    chip, lead, take, give = shares(me, ranks, steps)
    taker = take > 0
    far_chip = ranks // 2 - 1 - chip
    far = 2 * far_chip + core
    most = oa_recv.shape[0]
    is_far = (step > lead) & (step <= lead + take + 1) & taker
    qset = jnp.where(is_far, 1, 0)
    full = jnp.where(is_far, far_chip, chip)
    _, blocks, blk, kdim = k_v.shape
    kv_rank = wka_ref.shape[0]
    nope = wka_ref.shape[1] // 2
    half = cosq_ref.shape[1]
    rot = 2 * half
    sub = blk // 2
    everything = slice(None)
    my_rows = pl.ds(pl.multiple_of(core * sub, sub), sub)

    lat = [pltpu.make_async_remote_copy(src_ref=src, dst_ref=dst, send_sem=lat_send.at[k], recv_sem=lat_recv.at[k],
                                        device_id={"sp": far}, device_id_type=MESH)
           for k, (src, dst) in enumerate(((cq_ref.at[my_rows], cq_v.at[1, my_rows]), (tab_ref.at[core], tab_v.at[core])))]
    fwd = [pltpu.make_async_remote_copy(src_ref=ref, dst_ref=ref, send_sem=fwd_send.at[k], recv_sem=fwd_recv.at[k],
                                        device_id={"sp": sib}, device_id_type=MESH)
           for k, ref in enumerate((cq_v.at[1, my_rows], tab_v.at[core]))]

    def o_cols(at):
        return pl.ds(pl.multiple_of(at * 2 * nope, 2 * nope), 2 * nope)

    def o_local(part, s):
        src, dst = ((oa_v, oa_hbm), (ob_v, ob_hbm))[part]
        at = jnp.where(s <= lead, s - 1, s - take - 3)
        return pltpu.make_async_copy(src.at[most], dst.at[:, o_cols(at)], o_sem.at[part])

    def o_far(part, r):
        src, dst, send, recv = ((oa_v, oa_hbm, oa_send, oa_recv), (ob_v, ob_hbm, ob_send, ob_recv))[part]
        return pltpu.make_async_remote_copy(src_ref=src.at[r], dst_ref=dst.at[:, o_cols(steps - 1 - r)], send_sem=send.at[r], recv_sem=recv.at[r],
                                            device_id={"sp": far}, device_id_type=MESH)

    def left_own(s):
        return ((s >= 1) & (s <= lead)) | (taker & (s >= lead + take + 3) & (s <= steps + take + 2))

    def left_far(s):
        return taker & (s >= lead + 2) & (s <= lead + take + 1)

    far_slot = lead + take + 1 - step
    slot = jnp.where(left_far(step), far_slot, most)

    def emit(part):
        @pl.when(left_own(step))
        def _():
            o_local(part, step).start()

        @pl.when(left_far(step))
        def _():
            o_far(part, far_slot).start()

    def settle(part, s):
        @pl.when(left_own(s))
        def _():
            o_local(part, s).wait()

    @pl.when(step == 0)
    def _():
        barrier = pltpu.get_barrier_semaphore()
        for peer in (sib, far):
            pl.semaphore_signal(barrier, inc=1, device_id={"sp": peer}, device_id_type=MESH)
        pl.semaphore_wait(barrier, 2)

        @pl.when(give > 0)
        def _():
            for c in lat:
                c.start()

        for kb in range(blocks):
            pe = kv_ref[kb * blk:(kb + 1) * blk, kv_rank:]
            k_v[0, kb, :, nope:] = pe
            k_v[1, kb, :, nope:] = pe
        q_v[:, nope + rot:, :] = jnp.zeros((2, kdim - nope - rot, blk), BF16)
        for c in range(2):
            cosq_ref[0, :, c * sub:(c + 1) * sub] = tab_ref[c, :half, :]
            sinq_ref[0, :, c * sub:(c + 1) * sub] = tab_ref[c, half:, :]
        cq_v[0] = cq_ref[...]

    @pl.when(step > 0)
    def _():
        for part in range(2):
            settle(part, step - 1)

    @pl.when((step == lead) & taker)
    def _():
        for c in lat:
            c.wait_recv()
        for c in fwd:
            c.start()

    @pl.when((step == lead + 1) & taker)
    def _():
        for c in fwd:
            c.wait()
        for c in range(2):
            cosq_ref[1, :, c * sub:(c + 1) * sub] = tab_v[c, :half, :]
            sinq_ref[1, :, c * sub:(c + 1) * sub] = tab_v[c, half:, :]

    def q_proj(w_ref):
        w = jnp.concatenate([w_ref[0], w_ref[1]], axis=0)
        both = lax.dot_general(w, cq_v[qset], NT, preferred_element_type=F32)
        cos_t, sin_t = cosq_ref[qset], sinq_ref[qset]
        for h in range(2):
            u = both[h * (nope + rot):(h + 1) * (nope + rot)]
            q_v[h, :nope, :] = u[:nope].astype(BF16)
            z1 = u[nope:nope + half]
            z2 = u[nope + half:]
            q_v[h, nope:nope + half, :] = (z1 * cos_t - z2 * sin_t).astype(BF16)
            q_v[h, nope + half:nope + rot, :] = (z2 * cos_t + z1 * sin_t).astype(BF16)

    def kv_proj(kb, wk, wv, v_ref):
        c = kv_ref[pl.ds(pl.multiple_of(kb * blk, blk), blk), :kv_rank]
        k = jnp.dot(c, wk, preferred_element_type=F32).astype(BF16)
        v = lax.dot_general(wv, c, NT, preferred_element_type=F32).astype(BF16)
        for h in range(2):
            k_v[h, kb, :, :nope] = k[:, h * nope:(h + 1) * nope]
            v_ref[h, kb] = v[h * nope:(h + 1) * nope]

    def fold_max(m_ref, h, s, cols):
        t = jnp.max(s.reshape(s.shape[0] // 8, 8, s.shape[1]), axis=0)
        m_ref[h, :, cols] = jnp.maximum(m_ref[h, :, cols], t)

    def qk(h, kb, s_ref, m_ref):
        s = jnp.dot(k_v[h, kb], q_v[h], preferred_element_type=F32)
        s_ref[h, kb] = s
        fold_max(m_ref, h, s, everything)

    def qk_diag(h, kb, s_ref, m_ref):
        s0 = jnp.dot(k_v[h, kb, :sub, :], q_v[h], preferred_element_type=F32)
        s1 = jnp.dot(k_v[h, kb, sub:, :], q_v[h, :, sub:], preferred_element_type=F32)
        keep = lax.broadcasted_iota(jnp.int32, (sub, sub), 0) <= lax.broadcasted_iota(jnp.int32, (sub, sub), 1)
        s00 = jnp.where(keep, s0[:, :sub], -jnp.inf)
        s1 = jnp.where(keep, s1, -jnp.inf)
        s01 = s0[:, sub:]
        s_ref[h, kb, :sub, :sub] = s00
        s_ref[h, kb, :sub, sub:] = s01
        s_ref[h, kb, sub:, sub:] = s1
        fold_max(m_ref, h, s00, slice(0, sub))
        fold_max(m_ref, h, s01, slice(sub, blk))
        fold_max(m_ref, h, s1, slice(sub, blk))

    def fold_sum(l_ref, h, p, cols):
        l_ref[h, :, cols] += jnp.sum(p.reshape(p.shape[0] // 8, 8, p.shape[1]), axis=0)

    def top(m_ref):
        return [jnp.max(m_ref[h], axis=0, keepdims=True) for h in range(2)]

    def pv(h, kb, v_ref, s_ref, m, l_ref, o_ref):
        p = jnp.exp2((s_ref[h, kb] - m[h]) * scale2)
        fold_sum(l_ref, h, p, everything)
        o_ref[h] += jnp.dot(v_ref[h, kb], p.astype(BF16), preferred_element_type=F32)

    def pv_diag(h, kb, v_ref, s_ref, m, l_ref, o_ref):
        p0 = jnp.exp2((s_ref[h, kb, :sub, :] - m[h]) * scale2)
        p1 = jnp.exp2((s_ref[h, kb, sub:, sub:] - m[h][:, sub:]) * scale2)
        fold_sum(l_ref, h, p0, everything)
        fold_sum(l_ref, h, p1, slice(sub, blk))
        p0 = p0.astype(BF16)
        o_ref[h] += jnp.dot(v_ref[h, kb, :, :sub], p0, preferred_element_type=F32)
        o_ref[h, :, sub:] += jnp.dot(v_ref[h, kb, :, sub:], p1.astype(BF16), preferred_element_type=F32)

    def finish(l_ref, o_ref, out_ref):
        for h in range(2):
            l = jnp.sum(l_ref[h], axis=0, keepdims=True)
            out_ref[slot, :, h * nope:(h + 1) * nope] = (o_ref[h] / l).T.astype(BF16)

    def clear(l_ref, o_ref):
        l_ref[...] = jnp.zeros_like(l_ref)
        o_ref[...] = jnp.zeros_like(o_ref)

    def stage(wq_ref, wk_ref, wv_ref, new, old, done, done_out, part):
        s_n, m_n, v_n = new
        s_o, m_o, v_o, l_o, out_o = old
        m = top(m_o)
        q_proj(wq_ref)
        finish(done[0], done[1], done_out)
        emit(part)
        clear(l_o, out_o)
        m_n[...] = jnp.full_like(m_n, -jnp.inf)
        wk = wk_ref[...]
        wv = wv_ref[...].T

        def body(kb, carry):
            kv_proj(kb, wk, wv, v_n)
            for h in range(2):
                pv(h, kb, v_o, s_o, m, l_o, out_o)
                qk(h, kb, s_n, m_n)
            return carry

        lax.fori_loop(0, full, body, 0)
        kv_proj(full, wk, wv, v_n)
        for h in range(2):
            pv_diag(h, full, v_o, s_o, m, l_o, out_o)
            qk_diag(h, full, s_n, m_n)

    @pl.when((step < lead) | (taker & (step > lead) & (step != lead + take + 1) & (step < steps + take + 2)))
    def _():
        stage(wqa_ref, wka_ref, wva_ref, (s_a, m_a, v_a), (s_b, m_b, v_b, l_b, o_b), (l_a, o_a), oa_v, 0)
        stage(wqb_ref, wkb_ref, wvb_ref, (s_b, m_b, v_b), (s_a, m_a, v_a, l_a, o_a), (l_b, o_b), ob_v, 1)

    @pl.when((step == lead) | (taker & ((step == lead + take + 1) | (step == steps + take + 2))))
    def _():
        m = top(m_b)
        clear(l_b, o_b)
        finish(l_a, o_a, oa_v)
        emit(0)

        def body(kb, carry):
            for h in range(2):
                pv(h, kb, v_b, s_b, m, l_b, o_b)
            return carry

        lax.fori_loop(0, full, body, 0)
        for h in range(2):
            pv_diag(h, full, v_b, s_b, m, l_b, o_b)
        finish(l_b, o_b, ob_v)
        emit(1)

    @pl.when(step == final)
    def _():
        for part in range(2):
            settle(part, step)

        @pl.when(give > 0)
        def _():
            for c in lat:
                c.wait_send()

        for r in range(most):
            @pl.when(give > r)
            def _(r=r):
                for part in range(2):
                    o_far(part, r).wait_recv()

            @pl.when(take > r)
            def _(r=r):
                for part in range(2):
                    o_far(part, r).wait_send()


def out_kernel(oa_hbm, ob_hbm, wo_hbm, out_hbm, own_v, sib_v, w_v, acc_v, out_v,
               o_sem, lead_sem, w_sem, out_sem, swap_send, swap_recv, res_send, res_recv):
    me = lax.axis_index("sp")
    core = lax.rem(me, 2)
    sib = me + 1 - 2 * core
    wide = oa_hbm.shape[1]
    span = own_v.shape[1]
    rows = out_hbm.shape[0]
    bufs, _, nc = w_v.shape
    steps = acc_v.shape[0]

    def fetch(i):
        part = i // steps
        owner = core + part - 2 * core * part
        col = core * (steps * nc) + lax.rem(i, steps) * nc
        slot = lax.rem(i, bufs)
        return pltpu.make_async_copy(
            wo_hbm.at[pl.ds(pl.multiple_of(owner * span, span), span), pl.ds(pl.multiple_of(col, nc), nc)],
            w_v.at[slot], w_sem.at[slot])

    own = [pltpu.make_async_copy(h, own_v.at[:, pl.ds(k * wide, wide)], o_sem.at[k])
           for k, h in enumerate((oa_hbm, ob_hbm))]
    lead = [pltpu.make_async_copy(
        wo_hbm.at[pl.ds(pl.multiple_of(core * span + k * wide, wide), wide), pl.ds(pl.multiple_of(core * (steps * nc), nc), nc)],
        w_v.at[0, pl.ds(k * wide, wide)], lead_sem.at[k]) for k in range(2)]
    for k in range(2):
        own[k].start()
        lead[k].start()

    barrier = pltpu.get_barrier_semaphore()
    pl.semaphore_signal(barrier, inc=1, device_id={"sp": sib}, device_id_type=MESH)
    swap = [pltpu.make_async_remote_copy(
        src_ref=h, dst_ref=sib_v.at[:, pl.ds(k * wide, wide)],
        send_sem=swap_send.at[k], recv_sem=swap_recv.at[k], device_id={"sp": sib}, device_id_type=MESH)
        for k, h in enumerate((oa_hbm, ob_hbm))]
    own[0].wait()
    lead[0].wait()
    fetch(1).start()
    acc_v[0] = jnp.dot(own_v[:, :wide], w_v[0, :wide, :], preferred_element_type=F32)
    own[1].wait()
    lead[1].wait()
    fetch(2).start()
    pl.semaphore_wait(barrier, 1)
    for c in swap:
        c.start()
    acc_v[0] += jnp.dot(own_v[:, wide:], w_v[0, wide:, :], preferred_element_type=F32)

    def own_half(i, carry):
        fetch(i).wait()
        fetch(i + 2).start()
        acc_v[i] = jnp.dot(own_v[...], w_v[lax.rem(i, bufs)], preferred_element_type=F32)
        return carry

    lax.fori_loop(1, steps, own_half, 0)
    for c in swap:
        c.wait()

    def store(n):
        slot = lax.rem(n, 2)
        cols = pl.ds(pl.multiple_of(core * (steps * nc) + n * nc, nc), nc)
        keep = pltpu.make_async_copy(out_v.at[slot, pl.ds(pl.multiple_of(core * rows, rows), rows)],
                                     out_hbm.at[:, cols], out_sem.at[slot])
        give = pltpu.make_async_remote_copy(
            src_ref=out_v.at[slot, pl.ds(pl.multiple_of((1 - core) * rows, rows), rows)], dst_ref=out_hbm.at[:, cols],
            send_sem=res_send.at[n], recv_sem=res_recv.at[n], device_id={"sp": sib}, device_id_type=MESH)
        return keep, give

    def sib_half(n, carry):
        i = n + steps
        fetch(i).wait()

        @pl.when(i + 2 < 2 * steps)
        def _():
            fetch(i + 2).start()

        @pl.when(n >= 2)
        def _():
            keep, give = store(n - 2)
            keep.wait()
            give.wait_send()

        out_v[lax.rem(n, 2)] = (acc_v[n] + jnp.dot(sib_v[...], w_v[lax.rem(i, bufs)], preferred_element_type=F32)).astype(BF16)
        for c in store(n):
            c.start()
        return carry

    lax.fori_loop(0, steps, sib_half, 0)
    for n in range(steps - 2, steps):
        keep, give = store(n)
        keep.wait()
        give.wait_send()
    for n in range(steps):
        store(n)[1].wait_recv()


def result_kernel(res_hbm, kv_hbm, out_hbm, ckv_hbm, pe_hbm, res_v, kv_v, pe_v, in_sem, out_sem):
    me = lax.axis_index("sp")
    chunks, rows, width = res_v.shape
    kv_rank = ckv_hbm.shape[1]
    rot = pe_hbm.shape[0]
    take = [pltpu.make_async_copy(kv_hbm.at[pl.ds(pl.multiple_of(me * rows, rows), rows)], kv_v, in_sem.at[chunks])]
    take += [pltpu.make_async_copy(res_hbm.at[:, pl.ds(c * width, width)], res_v.at[c], in_sem.at[c]) for c in range(chunks)]
    for c in take:
        c.start()
    take[0].wait()
    pe_v[...] = kv_v[:, kv_rank:].astype(F32).T[:rot].astype(BF16)
    give = [pltpu.make_async_copy(kv_v.at[:, pl.ds(0, kv_rank)], ckv_hbm, out_sem.at[chunks]),
            pltpu.make_async_copy(pe_v, pe_hbm, out_sem.at[chunks + 1])]
    for c in give:
        c.start()
    for c in range(chunks):
        take[1 + c].wait()
        give.append(pltpu.make_async_copy(res_v.at[c], out_hbm.at[:, pl.ds(c * width, width)], out_sem.at[c]))
        give[-1].start()
    for c in give:
        c.wait()


def solution(mesh):
    ranks = mesh.shape["sp"]
    tok_spec = P(("dp", "sp"))
    rows_spec = P(("dp", "sp"), None)
    replicated = P()

    def local_step(tok_in, tok_pos, w_dq, g_q, w_uq, w_dkv, g_kv, w_uk, w_uv, w_o):
        rows, model = tok_in.shape
        num_heads = w_uq.shape[1]
        qk_dim = w_uq.shape[2]
        q_rank = w_dq.shape[1]
        kv_rank = g_kv.shape[0]
        rot = w_dkv.shape[1] - kv_rank
        nope = qk_dim - rot
        v_dim = w_uv.shape[2]
        seq = rows * ranks
        half = rot // 2
        mine = num_heads // 2
        pe_w = 128
        attn_scale = (0.1 * math.log(YARN_FACTOR) + 1.0) ** 2 / math.sqrt(qk_dim)
        kchunks, nq, depth = 4, 3, 64
        kv_w = kv_rank + pe_w
        any_spec = pl.BlockSpec(memory_space=pl.ANY)
        vmem_spec = pl.BlockSpec(memory_space=pltpu.VMEM)
        dma = pltpu.SemaphoreType.DMA
        kv_all, cq_all, tab_all, wk2, wv2 = pl.pallas_call(
            functools.partial(front_kernel, ranks, mine),
            out_shape=(
                jax.ShapeDtypeStruct((seq, kv_w), BF16),
                jax.ShapeDtypeStruct((2 * rows, q_rank), BF16),
                jax.ShapeDtypeStruct((2, rot, rows), F32),
                jax.ShapeDtypeStruct((kv_rank, mine * nope), BF16),
                jax.ShapeDtypeStruct((kv_rank, mine * v_dim), BF16),
            ),
            in_specs=[any_spec] * 5 + [vmem_spec] * 4,
            out_specs=(any_spec,) * 5,
            scratch_shapes=[
                pltpu.VMEM((rows, model), BF16),
                pltpu.VMEM((kchunks, kv_rank + rot, model // kchunks), BF16),
                pltpu.VMEM((nq, model, q_rank // nq), BF16),
                pltpu.VMEM((2, kv_rank, mine, nope), BF16),
                pltpu.VMEM((2, kv_rank, mine * nope), BF16),
                pltpu.VMEM((mine // 8, depth * 8, nope), F32),
                pltpu.VMEM((rows, q_rank), F32),
                pltpu.VMEM((rows, kv_w), BF16),
                pltpu.VMEM((rows, q_rank), BF16),
                pltpu.VMEM((rot, rows), F32),
                dma((2 * kchunks + nq + 2,)),
                dma((5,)),
                dma((11,)),
                dma((11,)),
                dma((2,)),
                dma((2,)),
            ],
            compiler_params=pltpu.CompilerParams(collective_id=0, has_side_effects=True, vmem_limit_bytes=60 << 20),
            cost_estimate=pl.CostEstimate(flops=2 * rows * model * (q_rank + kv_rank + rot), bytes_accessed=2 * model * (q_rank + kv_rank + rot), transcendentals=0),
        )(tok_in, w_dkv.T, w_dq, w_uk, w_uv, g_q, g_kv, tok_pos, rope_freqs(rot)[:, None])

        wuq_t = jnp.transpose(w_uq, (1, 2, 0))
        qn = 2 * rows
        nblk = seq // qn
        steps = mine // 4

        def whole(shape):
            return pl.BlockSpec(shape, lambda i: (0,) * len(shape))

        def up_spec(part):
            return pl.BlockSpec((2, qk_dim, q_rank), lambda i: (lax.rem(lax.axis_index("sp"), 2) * (mine // 2) + part * steps + weight_step(i, ranks, steps), 0, 0))

        def lat_spec(part):
            return pl.BlockSpec((kv_rank, 2 * nope), lambda i: (0, part * steps + weight_step(i, ranks, steps)))

        head_v = pltpu.VMEM((2, nblk, v_dim, qn), BF16)
        scores = pltpu.VMEM((2, nblk, qn, qn), F32)
        stat = pltpu.VMEM((2, 8, qn), F32)
        head_o = pltpu.VMEM((2, v_dim, qn), F32)
        rope_v = pltpu.VMEM((2, half, qn), F32)
        most = ranks // 4
        pair_o = pltpu.VMEM((most + 1, qn, 2 * v_dim), BF16)
        o_a, o_b = pl.pallas_call(
            functools.partial(attn_kernel, attn_scale * math.log2(math.e), ranks, steps),
            out_shape=(jax.ShapeDtypeStruct((qn, 2 * steps * v_dim), BF16),) * 2,
            grid=(steps + most + 3,),
            in_specs=[
                whole((qn, q_rank)),
                whole((seq, kv_w)),
                whole((2, rot, rows)),
                up_spec(0), up_spec(1), lat_spec(0), lat_spec(1), lat_spec(0), lat_spec(1),
            ],
            out_specs=(any_spec, any_spec),
            scratch_shapes=[pltpu.VMEM((2, qn, q_rank), BF16), pltpu.VMEM((2, rot, rows), F32),
                            pltpu.VMEM((2, nblk, qn, nope + pe_w), BF16), head_v, head_v, pltpu.VMEM((2, nope + pe_w, qn), BF16),
                            scores, scores, stat, stat, stat, stat, head_o, head_o, rope_v, rope_v, pair_o, pair_o,
                            dma((2,)), dma((2,)), dma((2,)), dma((2,)), dma((2,)), dma((most,)), dma((most,)), dma((most,)), dma((most,))],
            compiler_params=pltpu.CompilerParams(dimension_semantics=("arbitrary",), collective_id=2, has_side_effects=True, vmem_limit_bytes=62 << 20),
        )(cq_all, kv_all, tab_all, wuq_t, wuq_t, wk2, wk2, wv2, wv2)

        nc, bufs = 512, 3
        span = mine * v_dim
        pieces = model // 2 // nc
        res = pl.pallas_call(
            out_kernel,
            out_shape=jax.ShapeDtypeStruct((rows, model), BF16),
            in_specs=[any_spec] * 3,
            out_specs=any_spec,
            scratch_shapes=[
                pltpu.VMEM((qn, span), BF16),
                pltpu.VMEM((qn, span), BF16),
                pltpu.VMEM((bufs, span, nc), BF16),
                pltpu.VMEM((pieces, qn, nc), F32),
                pltpu.VMEM((2, qn, nc), BF16),
                dma((2,)),
                dma((2,)),
                dma((bufs,)),
                dma((2,)),
                dma((2,)),
                dma((2,)),
                dma((pieces,)),
                dma((pieces,)),
            ],
            compiler_params=pltpu.CompilerParams(collective_id=1, has_side_effects=True, vmem_limit_bytes=60 << 20),
        )(o_a, o_b, w_o.reshape(num_heads * v_dim, model))
        chunks = 8
        attn_out, cache_kv, pe_t = pl.pallas_call(
            result_kernel,
            out_shape=(
                jax.ShapeDtypeStruct((rows, model), BF16),
                jax.ShapeDtypeStruct((rows, kv_rank), BF16),
                jax.ShapeDtypeStruct((rot, rows), BF16),
            ),
            in_specs=[any_spec] * 2,
            out_specs=(any_spec,) * 3,
            scratch_shapes=[
                pltpu.VMEM((chunks, rows, model // chunks), BF16),
                pltpu.VMEM((rows, kv_w), BF16),
                pltpu.VMEM((rot, rows), BF16),
                dma((chunks + 1,)),
                dma((chunks + 2,)),
            ],
            compiler_params=pltpu.CompilerParams(vmem_limit_bytes=62 << 20),
        )(res, kv_all)
        return attn_out, cache_kv, pe_t.T

    return jax.shard_map(local_step, mesh=mesh,
                         in_specs=(rows_spec, tok_spec) + (replicated,) * 8,
                         out_specs=(rows_spec, rows_spec, rows_spec), check_vma=False)
```

```python
import functools
import math

import jax
import jax.numpy as jnp
from jax import lax
from jax.experimental import pallas as pl
from jax.experimental.pallas import tpu as pltpu
from jax.sharding import PartitionSpec as P

ROPE_THETA = 10000.0
YARN_FACTOR = 40.0
ORIG_CTX = 4096.0
BETA_FAST = 32.0
BETA_SLOW = 1.0
NORM_EPS = 1e-6

MESH = pl.DeviceIdType.MESH
F32 = jnp.float32
BF16 = jnp.bfloat16
NT = (((1,), (1,)), ((), ()))
TT = (((0,), (1,)), ((), ()))


def rope_freqs(rot_dim):
    half_dim = rot_dim // 2
    log_base = 2.0 * math.log(ROPE_THETA)
    low_idx = max(math.floor(rot_dim * math.log(ORIG_CTX / (BETA_FAST * 2.0 * math.pi)) / log_base), 0)
    high_idx = min(math.ceil(rot_dim * math.log(ORIG_CTX / (BETA_SLOW * 2.0 * math.pi)) / log_base), half_dim - 1)
    spread = max(high_idx - low_idx, 0.001)
    freq_list = []
    for freq_idx in range(half_dim):
        base_freq = ROPE_THETA ** (-2.0 * freq_idx / rot_dim)
        ramp_val = min(max((freq_idx - low_idx) / spread, 0.0), 1.0)
        freq_list.append(base_freq / YARN_FACTOR * ramp_val + base_freq * (1.0 - ramp_val))
    return jnp.asarray(freq_list, dtype=jnp.float32)


def front_kernel(ranks, heads, x_hbm, wkv_hbm, wq_hbm, wuk_hbm, wuv_hbm, gq_ref, gkv_ref, pos_ref, freq_ref,
                 kv_all, cq_all, tab_all, wk_out, wv_out,
                 x_v, wkv_v, wq_v, wu_v, wo_v, wide_v, cq_f, kv_v, cq_v, tab_v,
                 w_sem, own_sem, kv_send, kv_recv, pair_send, pair_recv):
    me = lax.axis_index("sp")
    core = lax.rem(me, 2)
    sib = me + 1 - 2 * core
    rows = x_v.shape[0]
    half = freq_ref.shape[0]
    kv_rank = gkv_ref.shape[0]
    right = lax.rem(me + 2, ranks)
    left = lax.rem(me + ranks - 2, ranks)
    across = lax.rem(me + 4, ranks)

    kchunks, nq = wkv_v.shape[0], wq_v.shape[0]
    kc = wkv_v.shape[2]
    nc = wq_v.shape[2]
    first = core * heads
    loads = []
    for k in range(kchunks):
        cols = pl.ds(k * kc, kc)
        loads.append([pltpu.make_async_copy(x_hbm.at[:, cols], x_v.at[:, cols], w_sem.at[2 * k]),
                      pltpu.make_async_copy(wkv_hbm.at[:, cols], wkv_v.at[k], w_sem.at[2 * k + 1])])
    base = 2 * kchunks
    loads += [[pltpu.make_async_copy(wq_hbm.at[:, pl.ds(k * nc, nc)], wq_v.at[k], w_sem.at[base + k])] for k in range(nq)]
    loads += [[pltpu.make_async_copy(h.at[:, pl.ds(first, heads), :], wu_v.at[k], w_sem.at[base + nq + k])]
              for k, h in enumerate((wuk_hbm, wuv_hbm))]
    ahead = 3

    def launch(i):
        if i < len(loads):
            for c in loads[i]:
                c.start()

    def arrive(i):
        for c in loads[i]:
            c.wait()
        launch(i + ahead)

    for i in range(ahead):
        launch(i)

    barrier = pltpu.get_barrier_semaphore()
    for peer in (sib, right, left):
        pl.semaphore_signal(barrier, inc=1, device_id={"sp": peer}, device_id_type=MESH)

    def block(idx):
        return kv_all.at[pl.ds(idx * rows, rows)]

    def remote(src, dst, send, recv, dev):
        return pltpu.make_async_remote_copy(src_ref=src, dst_ref=dst, send_sem=send, recv_sem=recv,
                                            device_id={"sp": dev}, device_id_type=MESH)

    acc = None
    for k in range(kchunks):
        arrive(k)
        part = lax.dot_general(x_v[:, k * kc:(k + 1) * kc], wkv_v[k], NT, preferred_element_type=F32)
        acc = part if acc is None else acc + part
    a = acc[:, :kv_rank]
    inv = lax.rsqrt(jnp.mean(a * a, axis=-1, keepdims=True) + NORM_EPS)
    ckv = (a * inv * gkv_ref[...][None, :]).astype(BF16)
    angles = freq_ref[...] * pos_ref[...].astype(F32)[None, :]
    tab_v[:half, :] = jnp.cos(angles)
    tab_v[half:, :] = jnp.sin(angles)
    tab = tab_v[...].T
    cos_t, sin_t = tab[:, :half], tab[:, half:]
    z1 = acc[:, kv_rank:kv_rank + half]
    z2 = acc[:, kv_rank + half:]
    pe = jnp.concatenate([z1 * cos_t - z2 * sin_t, z2 * cos_t + z1 * sin_t], axis=-1).astype(BF16)
    kv_v[:, :kv_rank] = ckv
    kv_v[:, kv_rank:] = jnp.concatenate([pe, jnp.zeros((rows, kv_v.shape[1] - kv_rank - 2 * half), BF16)], axis=-1)

    pl.semaphore_wait(barrier, 3)
    mid = rows // 2

    def piece(h):
        return pl.ds(h * mid, mid)

    def part(idx, h):
        return kv_all.at[pl.ds(idx * rows + h * mid, mid)]

    to_sib = remote(kv_v, block(me), kv_send.at[0], kv_recv.at[0], sib)
    to_right = [remote(kv_v.at[piece(h)], part(me, h), kv_send.at[1 + h], kv_recv.at[1 + h], right) for h in range(2)]
    to_left = [remote(kv_v.at[piece(h)], part(me, h), kv_send.at[3 + h], kv_recv.at[3 + h], left) for h in range(2)]
    tab_copy = remote(tab_v, tab_all.at[core], pair_send.at[0], pair_recv.at[0], sib)
    for c in (to_right[0], to_left[1], to_right[1], to_left[0], to_sib, tab_copy):
        c.start()
    own = [pltpu.make_async_copy(kv_v, block(me), own_sem.at[0]),
           pltpu.make_async_copy(tab_v, tab_all.at[core], own_sem.at[1])]
    for c in own:
        c.start()

    ssq = jnp.zeros((rows, 1), F32)
    for k in range(nq):
        arrive(kchunks + k)
        q = jnp.dot(x_v[...], wq_v[k], preferred_element_type=F32)
        cq_f[:, k * nc:(k + 1) * nc] = q
        ssq = ssq + jnp.sum(q * q, axis=-1, keepdims=True)
    inv_q = lax.rsqrt(ssq / cq_f.shape[1] + NORM_EPS)
    cq_v[...] = (cq_f[...] * inv_q * gq_ref[...][None, :]).astype(BF16)
    cq_copy = remote(cq_v, cq_all.at[pl.ds(core * rows, rows)], pair_send.at[1], pair_recv.at[1], sib)
    cq_copy.start()
    own.append(pltpu.make_async_copy(cq_v, cq_all.at[pl.ds(core * rows, rows)], own_sem.at[2]))
    own[-1].start()

    to_right[0].wait_recv()
    half_right = remote(part(left, 0), part(left, 0), kv_send.at[5], kv_recv.at[5], right)
    half_right.start()
    to_left[1].wait_recv()
    half_left = remote(part(right, 1), part(right, 1), kv_send.at[6], kv_recv.at[6], left)
    half_left.start()

    depth = wide_v.shape[1] // 8
    groups = wide_v.shape[0]
    width = wide_v.shape[2]

    def up_relayout(t, out):
        arrive(kchunks + nq + t)

        def relayout(i, carry):
            base = pl.multiple_of(i * depth, depth)
            for g in range(groups):
                wide_v[g] = wu_v[t, pl.ds(base, depth), g * 8:(g + 1) * 8, :].astype(F32).reshape(depth * 8, width)
            for g in range(groups):
                for h in range(8):
                    col = (g * 8 + h) * width
                    wo_v[t, pl.ds(base, depth), col:col + width] = wide_v[g, pl.ds(h, depth, stride=8), :].astype(BF16)
            return carry

        lax.fori_loop(0, wu_v.shape[1] // depth, relayout, 0)
        own.append(pltpu.make_async_copy(wo_v.at[t], out, own_sem.at[3 + t]))
        own[-1].start()

    up_relayout(0, wk_out)
    to_right[1].wait_recv()
    sib_left = remote(block(left), block(left), kv_send.at[7], kv_recv.at[7], sib)
    sib_left.start()
    to_left[0].wait_recv()
    sib_right = remote(block(right), block(right), kv_send.at[8], kv_recv.at[8], sib)
    sib_right.start()
    up_relayout(1, wv_out)
    half_right.wait_recv()
    sib_across0 = remote(part(across, 0), part(across, 0), kv_send.at[9], kv_recv.at[9], sib)
    sib_across0.start()
    half_left.wait_recv()
    sib_across1 = remote(part(across, 1), part(across, 1), kv_send.at[10], kv_recv.at[10], sib)
    sib_across1.start()
    to_sib.wait()
    for c in to_right + to_left + [half_right, half_left]:
        c.wait_send()
    for c in (sib_left, sib_right, sib_across0, sib_across1, tab_copy, cq_copy):
        c.wait()
    for c in own:
        c.wait()


def shares(me, ranks, steps):
    chips = ranks // 2
    chip = me // 2
    give = jnp.maximum(chip - chips // 2 + 1, 0)
    take = jnp.maximum(chips // 2 - chip, 0)
    lead = jnp.where(take > 0, steps // 2 + take - 1, steps - give)
    return chip, lead, take, give


def weight_step(i, ranks, steps):
    _, lead, take, _ = shares(lax.axis_index("sp"), ranks, steps)
    far = steps - take + jnp.minimum(i - lead - 1, take - 1)
    late = jnp.where(i <= lead + take + 1, far, jnp.minimum(i - take - 2, steps - 1))
    return jnp.where((i <= lead) | (take == 0), jnp.minimum(i, lead - 1), late)


def attn_kernel(scale2, ranks, steps, cq_ref, kv_ref, tab_ref,
                wqa_ref, wqb_ref, wka_ref, wkb_ref, wva_ref, wvb_ref, oa_hbm, ob_hbm,
                cq_v, tab_v, k_v, v_a, v_b, q_v, s_a, s_b, m_a, m_b, l_a, l_b, o_a, o_b, cosq_ref, sinq_ref, oa_v, ob_v,
                lat_send, lat_recv, fwd_send, fwd_recv, o_sem, oa_send, ob_send, oa_recv, ob_recv):
    step = pl.program_id(0)
    final = pl.num_programs(0) - 1
    me = lax.axis_index("sp")
    core = lax.rem(me, 2)
    sib = me + 1 - 2 * core
    chip, lead, take, give = shares(me, ranks, steps)
    taker = take > 0
    far_chip = ranks // 2 - 1 - chip
    far = 2 * far_chip + core
    most = oa_recv.shape[0]
    is_far = (step > lead) & (step <= lead + take + 1) & taker
    qset = jnp.where(is_far, 1, 0)
    full = jnp.where(is_far, far_chip, chip)
    _, blocks, blk, kdim = k_v.shape
    kv_rank = wka_ref.shape[0]
    nope = wka_ref.shape[1] // 2
    half = cosq_ref.shape[1]
    rot = 2 * half
    sub = blk // 2
    everything = slice(None)
    my_rows = pl.ds(pl.multiple_of(core * sub, sub), sub)

    lat = [pltpu.make_async_remote_copy(src_ref=src, dst_ref=dst, send_sem=lat_send.at[k], recv_sem=lat_recv.at[k],
                                        device_id={"sp": far}, device_id_type=MESH)
           for k, (src, dst) in enumerate(((cq_ref.at[my_rows], cq_v.at[1, my_rows]), (tab_ref.at[core], tab_v.at[core])))]
    fwd = [pltpu.make_async_remote_copy(src_ref=ref, dst_ref=ref, send_sem=fwd_send.at[k], recv_sem=fwd_recv.at[k],
                                        device_id={"sp": sib}, device_id_type=MESH)
           for k, ref in enumerate((cq_v.at[1, my_rows], tab_v.at[core]))]

    def o_cols(at):
        return pl.ds(pl.multiple_of(at * 2 * nope, 2 * nope), 2 * nope)

    def o_local(part, s):
        src, dst = ((oa_v, oa_hbm), (ob_v, ob_hbm))[part]
        at = jnp.where(s <= lead, s - 1, s - take - 3)
        return pltpu.make_async_copy(src.at[most], dst.at[:, o_cols(at)], o_sem.at[part])

    def o_far(part, r):
        src, dst, send, recv = ((oa_v, oa_hbm, oa_send, oa_recv), (ob_v, ob_hbm, ob_send, ob_recv))[part]
        return pltpu.make_async_remote_copy(src_ref=src.at[r], dst_ref=dst.at[:, o_cols(steps - 1 - r)], send_sem=send.at[r], recv_sem=recv.at[r],
                                            device_id={"sp": far}, device_id_type=MESH)

    def left_own(s):
        return ((s >= 1) & (s <= lead)) | (taker & (s >= lead + take + 3) & (s <= steps + take + 2))

    def left_far(s):
        return taker & (s >= lead + 2) & (s <= lead + take + 1)

    far_slot = lead + take + 1 - step
    slot = jnp.where(left_far(step), far_slot, most)

    def emit(part):
        @pl.when(left_own(step))
        def _():
            o_local(part, step).start()

        @pl.when(left_far(step))
        def _():
            o_far(part, far_slot).start()

    def settle(part, s):
        @pl.when(left_own(s))
        def _():
            o_local(part, s).wait()

    @pl.when(step == 0)
    def _():
        barrier = pltpu.get_barrier_semaphore()
        for peer in (sib, far):
            pl.semaphore_signal(barrier, inc=1, device_id={"sp": peer}, device_id_type=MESH)
        for kb in range(blocks):
            pe = kv_ref[kb * blk:(kb + 1) * blk, kv_rank:]
            k_v[0, kb, :, nope:] = pe
            k_v[1, kb, :, nope:] = pe
        q_v[:, nope + rot:, :] = jnp.zeros((2, kdim - nope - rot, blk), BF16)
        for c in range(2):
            cosq_ref[0, :, c * sub:(c + 1) * sub] = tab_ref[c, :half, :]
            sinq_ref[0, :, c * sub:(c + 1) * sub] = tab_ref[c, half:, :]
        cq_v[0] = cq_ref[...]
        pl.semaphore_wait(barrier, 2)

        @pl.when(give > 0)
        def _():
            for c in lat:
                c.start()

    @pl.when(step > 0)
    def _():
        for part in range(2):
            settle(part, step - 1)

    @pl.when((step == lead) & taker)
    def _():
        for c in lat:
            c.wait_recv()
        for c in fwd:
            c.start()

    @pl.when((step == lead + 1) & taker)
    def _():
        for c in fwd:
            c.wait()
        for c in range(2):
            cosq_ref[1, :, c * sub:(c + 1) * sub] = tab_v[c, :half, :]
            sinq_ref[1, :, c * sub:(c + 1) * sub] = tab_v[c, half:, :]

    def q_proj(w_ref):
        w = jnp.concatenate([w_ref[0], w_ref[1]], axis=0)
        both = lax.dot_general(w, cq_v[qset], NT, preferred_element_type=F32)
        cos_t, sin_t = cosq_ref[qset], sinq_ref[qset]
        for h in range(2):
            u = both[h * (nope + rot):(h + 1) * (nope + rot)]
            q_v[h, :nope, :] = u[:nope].astype(BF16)
            z1 = u[nope:nope + half]
            z2 = u[nope + half:]
            q_v[h, nope:nope + half, :] = (z1 * cos_t - z2 * sin_t).astype(BF16)
            q_v[h, nope + half:nope + rot, :] = (z2 * cos_t + z1 * sin_t).astype(BF16)

    def kv_proj(kb, wk, wv, v_ref):
        c = kv_ref[pl.ds(pl.multiple_of(kb * blk, blk), blk), :kv_rank]
        k = jnp.dot(c, wk, preferred_element_type=F32).astype(BF16)
        v = lax.dot_general(wv, c, NT, preferred_element_type=F32).astype(BF16)
        for h in range(2):
            k_v[h, kb, :, :nope] = k[:, h * nope:(h + 1) * nope]
            v_ref[h, kb] = v[h * nope:(h + 1) * nope]

    def fold_max(m_ref, h, s, cols):
        t = jnp.max(s.reshape(s.shape[0] // 8, 8, s.shape[1]), axis=0)
        m_ref[h, :, cols] = jnp.maximum(m_ref[h, :, cols], t)

    def qk(h, kb, s_ref, m_ref):
        s = jnp.dot(k_v[h, kb], q_v[h], preferred_element_type=F32)
        s_ref[h, kb] = s
        fold_max(m_ref, h, s, everything)

    def qk_diag(h, kb, s_ref, m_ref):
        s0 = jnp.dot(k_v[h, kb, :sub, :], q_v[h], preferred_element_type=F32)
        s1 = jnp.dot(k_v[h, kb, sub:, :], q_v[h, :, sub:], preferred_element_type=F32)
        keep = lax.broadcasted_iota(jnp.int32, (sub, sub), 0) <= lax.broadcasted_iota(jnp.int32, (sub, sub), 1)
        s00 = jnp.where(keep, s0[:, :sub], -jnp.inf)
        s1 = jnp.where(keep, s1, -jnp.inf)
        s01 = s0[:, sub:]
        s_ref[h, kb, :sub, :sub] = s00
        s_ref[h, kb, :sub, sub:] = s01
        s_ref[h, kb, sub:, sub:] = s1
        fold_max(m_ref, h, s00, slice(0, sub))
        fold_max(m_ref, h, s01, slice(sub, blk))
        fold_max(m_ref, h, s1, slice(sub, blk))

    def fold_sum(l_ref, h, p, cols):
        l_ref[h, :, cols] += jnp.sum(p.reshape(p.shape[0] // 8, 8, p.shape[1]), axis=0)

    def top(m_ref):
        return [jnp.max(m_ref[h], axis=0, keepdims=True) for h in range(2)]

    def pv(h, kb, v_ref, s_ref, m, l_ref, o_ref):
        p = jnp.exp2((s_ref[h, kb] - m[h]) * scale2)
        fold_sum(l_ref, h, p, everything)
        o_ref[h] += jnp.dot(v_ref[h, kb], p.astype(BF16), preferred_element_type=F32)

    def pv_diag(h, kb, v_ref, s_ref, m, l_ref, o_ref):
        p0 = jnp.exp2((s_ref[h, kb, :sub, :] - m[h]) * scale2)
        p1 = jnp.exp2((s_ref[h, kb, sub:, sub:] - m[h][:, sub:]) * scale2)
        fold_sum(l_ref, h, p0, everything)
        fold_sum(l_ref, h, p1, slice(sub, blk))
        p0 = p0.astype(BF16)
        o_ref[h] += jnp.dot(v_ref[h, kb, :, :sub], p0, preferred_element_type=F32)
        o_ref[h, :, sub:] += jnp.dot(v_ref[h, kb, :, sub:], p1.astype(BF16), preferred_element_type=F32)

    def finish(l_ref, o_ref, out_ref):
        for h in range(2):
            l = jnp.sum(l_ref[h], axis=0, keepdims=True)
            out_ref[slot, :, h * nope:(h + 1) * nope] = (o_ref[h] / l).T.astype(BF16)

    def clear(l_ref, o_ref):
        l_ref[...] = jnp.zeros_like(l_ref)
        o_ref[...] = jnp.zeros_like(o_ref)

    def stage(wq_ref, wk_ref, wv_ref, new, old, done, done_out, part):
        s_n, m_n, v_n = new
        s_o, m_o, v_o, l_o, out_o = old
        m = top(m_o)
        q_proj(wq_ref)
        finish(done[0], done[1], done_out)
        emit(part)
        clear(l_o, out_o)
        m_n[...] = jnp.full_like(m_n, -jnp.inf)
        wk = wk_ref[...]
        wv = wv_ref[...].T

        def body(kb, carry):
            kv_proj(kb, wk, wv, v_n)
            for h in range(2):
                pv(h, kb, v_o, s_o, m, l_o, out_o)
                qk(h, kb, s_n, m_n)
            return carry

        lax.fori_loop(0, full, body, 0)
        kv_proj(full, wk, wv, v_n)
        for h in range(2):
            pv_diag(h, full, v_o, s_o, m, l_o, out_o)
            qk_diag(h, full, s_n, m_n)

    @pl.when((step < lead) | (taker & (step > lead) & (step != lead + take + 1) & (step < steps + take + 2)))
    def _():
        stage(wqa_ref, wka_ref, wva_ref, (s_a, m_a, v_a), (s_b, m_b, v_b, l_b, o_b), (l_a, o_a), oa_v, 0)
        stage(wqb_ref, wkb_ref, wvb_ref, (s_b, m_b, v_b), (s_a, m_a, v_a, l_a, o_a), (l_b, o_b), ob_v, 1)

    @pl.when((step == lead) | (taker & ((step == lead + take + 1) | (step == steps + take + 2))))
    def _():
        m = top(m_b)
        clear(l_b, o_b)
        finish(l_a, o_a, oa_v)
        emit(0)

        def body(kb, carry):
            for h in range(2):
                pv(h, kb, v_b, s_b, m, l_b, o_b)
            return carry

        lax.fori_loop(0, full, body, 0)
        for h in range(2):
            pv_diag(h, full, v_b, s_b, m, l_b, o_b)
        finish(l_b, o_b, ob_v)
        emit(1)

    @pl.when(step == final)
    def _():
        for part in range(2):
            settle(part, step)

        @pl.when(give > 0)
        def _():
            for c in lat:
                c.wait_send()

        for r in range(most):
            @pl.when(give > r)
            def _(r=r):
                for part in range(2):
                    o_far(part, r).wait_recv()

            @pl.when(take > r)
            def _(r=r):
                for part in range(2):
                    o_far(part, r).wait_send()


def out_kernel(oa_hbm, ob_hbm, wo_hbm, out_hbm, own_v, sib_v, w_v, acc_v, out_v,
               o_sem, lead_sem, w_sem, out_sem, swap_send, swap_recv, res_send, res_recv):
    me = lax.axis_index("sp")
    core = lax.rem(me, 2)
    sib = me + 1 - 2 * core
    wide = oa_hbm.shape[1]
    span = own_v.shape[1]
    rows = out_hbm.shape[0]
    bufs, _, nc = w_v.shape
    steps = acc_v.shape[0]

    def fetch(i):
        part = i // steps
        owner = core + part - 2 * core * part
        col = core * (steps * nc) + lax.rem(i, steps) * nc
        slot = lax.rem(i, bufs)
        return pltpu.make_async_copy(
            wo_hbm.at[pl.ds(pl.multiple_of(owner * span, span), span), pl.ds(pl.multiple_of(col, nc), nc)],
            w_v.at[slot], w_sem.at[slot])

    own = [pltpu.make_async_copy(h, own_v.at[:, pl.ds(k * wide, wide)], o_sem.at[k])
           for k, h in enumerate((oa_hbm, ob_hbm))]
    lead = [pltpu.make_async_copy(
        wo_hbm.at[pl.ds(pl.multiple_of(core * span + k * wide, wide), wide), pl.ds(pl.multiple_of(core * (steps * nc), nc), nc)],
        w_v.at[0, pl.ds(k * wide, wide)], lead_sem.at[k]) for k in range(2)]
    for k in range(2):
        own[k].start()
        lead[k].start()

    barrier = pltpu.get_barrier_semaphore()
    pl.semaphore_signal(barrier, inc=1, device_id={"sp": sib}, device_id_type=MESH)
    swap = [pltpu.make_async_remote_copy(
        src_ref=h, dst_ref=sib_v.at[:, pl.ds(k * wide, wide)],
        send_sem=swap_send.at[k], recv_sem=swap_recv.at[k], device_id={"sp": sib}, device_id_type=MESH)
        for k, h in enumerate((oa_hbm, ob_hbm))]
    own[0].wait()
    lead[0].wait()
    fetch(1).start()
    acc_v[0] = jnp.dot(own_v[:, :wide], w_v[0, :wide, :], preferred_element_type=F32)
    own[1].wait()
    lead[1].wait()
    fetch(2).start()
    pl.semaphore_wait(barrier, 1)
    for c in swap:
        c.start()
    acc_v[0] += jnp.dot(own_v[:, wide:], w_v[0, wide:, :], preferred_element_type=F32)

    def own_half(i, carry):
        fetch(i).wait()
        fetch(i + 2).start()
        acc_v[i] = jnp.dot(own_v[...], w_v[lax.rem(i, bufs)], preferred_element_type=F32)
        return carry

    lax.fori_loop(1, steps, own_half, 0)
    for c in swap:
        c.wait()

    def store(n):
        slot = lax.rem(n, 2)
        cols = pl.ds(pl.multiple_of(core * (steps * nc) + n * nc, nc), nc)
        keep = pltpu.make_async_copy(out_v.at[slot, pl.ds(pl.multiple_of(core * rows, rows), rows)],
                                     out_hbm.at[:, cols], out_sem.at[slot])
        give = pltpu.make_async_remote_copy(
            src_ref=out_v.at[slot, pl.ds(pl.multiple_of((1 - core) * rows, rows), rows)], dst_ref=out_hbm.at[:, cols],
            send_sem=res_send.at[n], recv_sem=res_recv.at[n], device_id={"sp": sib}, device_id_type=MESH)
        return keep, give

    def sib_half(n, carry):
        i = n + steps
        fetch(i).wait()

        @pl.when(i + 2 < 2 * steps)
        def _():
            fetch(i + 2).start()

        @pl.when(n >= 2)
        def _():
            keep, give = store(n - 2)
            keep.wait()
            give.wait_send()

        out_v[lax.rem(n, 2)] = (acc_v[n] + jnp.dot(sib_v[...], w_v[lax.rem(i, bufs)], preferred_element_type=F32)).astype(BF16)
        for c in store(n):
            c.start()
        return carry

    lax.fori_loop(0, steps, sib_half, 0)
    for n in range(steps - 2, steps):
        keep, give = store(n)
        keep.wait()
        give.wait_send()
    for n in range(steps):
        store(n)[1].wait_recv()


def result_kernel(res_hbm, kv_hbm, out_hbm, ckv_hbm, pe_hbm, res_v, kv_v, pe_v, in_sem, out_sem):
    me = lax.axis_index("sp")
    chunks, rows, width = res_v.shape
    kv_rank = ckv_hbm.shape[1]
    rot = pe_hbm.shape[0]
    take = [pltpu.make_async_copy(kv_hbm.at[pl.ds(pl.multiple_of(me * rows, rows), rows)], kv_v, in_sem.at[chunks])]
    take += [pltpu.make_async_copy(res_hbm.at[:, pl.ds(c * width, width)], res_v.at[c], in_sem.at[c]) for c in range(chunks)]
    for c in take:
        c.start()
    take[0].wait()
    pe_v[...] = kv_v[:, kv_rank:].astype(F32).T[:rot].astype(BF16)
    give = [pltpu.make_async_copy(kv_v.at[:, pl.ds(0, kv_rank)], ckv_hbm, out_sem.at[chunks]),
            pltpu.make_async_copy(pe_v, pe_hbm, out_sem.at[chunks + 1])]
    for c in give:
        c.start()
    for c in range(chunks):
        take[1 + c].wait()
        give.append(pltpu.make_async_copy(res_v.at[c], out_hbm.at[:, pl.ds(c * width, width)], out_sem.at[c]))
        give[-1].start()
    for c in give:
        c.wait()


def solution(mesh):
    ranks = mesh.shape["sp"]
    tok_spec = P(("dp", "sp"))
    rows_spec = P(("dp", "sp"), None)
    replicated = P()

    def local_step(tok_in, tok_pos, w_dq, g_q, w_uq, w_dkv, g_kv, w_uk, w_uv, w_o):
        rows, model = tok_in.shape
        num_heads = w_uq.shape[1]
        qk_dim = w_uq.shape[2]
        q_rank = w_dq.shape[1]
        kv_rank = g_kv.shape[0]
        rot = w_dkv.shape[1] - kv_rank
        nope = qk_dim - rot
        v_dim = w_uv.shape[2]
        seq = rows * ranks
        half = rot // 2
        mine = num_heads // 2
        pe_w = 128
        attn_scale = (0.1 * math.log(YARN_FACTOR) + 1.0) ** 2 / math.sqrt(qk_dim)
        kchunks, nq, depth = 4, 3, 64
        kv_w = kv_rank + pe_w
        any_spec = pl.BlockSpec(memory_space=pl.ANY)
        vmem_spec = pl.BlockSpec(memory_space=pltpu.VMEM)
        dma = pltpu.SemaphoreType.DMA
        kv_all, cq_all, tab_all, wk2, wv2 = pl.pallas_call(
            functools.partial(front_kernel, ranks, mine),
            out_shape=(
                jax.ShapeDtypeStruct((seq, kv_w), BF16),
                jax.ShapeDtypeStruct((2 * rows, q_rank), BF16),
                jax.ShapeDtypeStruct((2, rot, rows), F32),
                jax.ShapeDtypeStruct((kv_rank, mine * nope), BF16),
                jax.ShapeDtypeStruct((kv_rank, mine * v_dim), BF16),
            ),
            in_specs=[any_spec] * 5 + [vmem_spec] * 4,
            out_specs=(any_spec,) * 5,
            scratch_shapes=[
                pltpu.VMEM((rows, model), BF16),
                pltpu.VMEM((kchunks, kv_rank + rot, model // kchunks), BF16),
                pltpu.VMEM((nq, model, q_rank // nq), BF16),
                pltpu.VMEM((2, kv_rank, mine, nope), BF16),
                pltpu.VMEM((2, kv_rank, mine * nope), BF16),
                pltpu.VMEM((mine // 8, depth * 8, nope), F32),
                pltpu.VMEM((rows, q_rank), F32),
                pltpu.VMEM((rows, kv_w), BF16),
                pltpu.VMEM((rows, q_rank), BF16),
                pltpu.VMEM((rot, rows), F32),
                dma((2 * kchunks + nq + 2,)),
                dma((5,)),
                dma((11,)),
                dma((11,)),
                dma((2,)),
                dma((2,)),
            ],
            compiler_params=pltpu.CompilerParams(collective_id=0, has_side_effects=True, vmem_limit_bytes=60 << 20),
            cost_estimate=pl.CostEstimate(flops=2 * rows * model * (q_rank + kv_rank + rot), bytes_accessed=2 * model * (q_rank + kv_rank + rot), transcendentals=0),
        )(tok_in, w_dkv.T, w_dq, w_uk, w_uv, g_q, g_kv, tok_pos, rope_freqs(rot)[:, None])

        wuq_t = jnp.transpose(w_uq, (1, 2, 0))
        qn = 2 * rows
        nblk = seq // qn
        steps = mine // 4

        def whole(shape):
            return pl.BlockSpec(shape, lambda i: (0,) * len(shape))

        def up_spec(part):
            return pl.BlockSpec((2, qk_dim, q_rank), lambda i: (lax.rem(lax.axis_index("sp"), 2) * (mine // 2) + part * steps + weight_step(i, ranks, steps), 0, 0))

        def lat_spec(part):
            return pl.BlockSpec((kv_rank, 2 * nope), lambda i: (0, part * steps + weight_step(i, ranks, steps)))

        head_v = pltpu.VMEM((2, nblk, v_dim, qn), BF16)
        scores = pltpu.VMEM((2, nblk, qn, qn), F32)
        stat = pltpu.VMEM((2, 8, qn), F32)
        head_o = pltpu.VMEM((2, v_dim, qn), F32)
        rope_v = pltpu.VMEM((2, half, qn), F32)
        most = ranks // 4
        pair_o = pltpu.VMEM((most + 1, qn, 2 * v_dim), BF16)
        o_a, o_b = pl.pallas_call(
            functools.partial(attn_kernel, attn_scale * math.log2(math.e), ranks, steps),
            out_shape=(jax.ShapeDtypeStruct((qn, 2 * steps * v_dim), BF16),) * 2,
            grid=(steps + most + 3,),
            in_specs=[
                whole((qn, q_rank)),
                whole((seq, kv_w)),
                whole((2, rot, rows)),
                up_spec(0), up_spec(1), lat_spec(0), lat_spec(1), lat_spec(0), lat_spec(1),
            ],
            out_specs=(any_spec, any_spec),
            scratch_shapes=[pltpu.VMEM((2, qn, q_rank), BF16), pltpu.VMEM((2, rot, rows), F32),
                            pltpu.VMEM((2, nblk, qn, nope + pe_w), BF16), head_v, head_v, pltpu.VMEM((2, nope + pe_w, qn), BF16),
                            scores, scores, stat, stat, stat, stat, head_o, head_o, rope_v, rope_v, pair_o, pair_o,
                            dma((2,)), dma((2,)), dma((2,)), dma((2,)), dma((2,)), dma((most,)), dma((most,)), dma((most,)), dma((most,))],
            compiler_params=pltpu.CompilerParams(dimension_semantics=("arbitrary",), collective_id=2, has_side_effects=True, vmem_limit_bytes=62 << 20),
        )(cq_all, kv_all, tab_all, wuq_t, wuq_t, wk2, wk2, wv2, wv2)

        nc, bufs = 512, 3
        span = mine * v_dim
        pieces = model // 2 // nc
        res = pl.pallas_call(
            out_kernel,
            out_shape=jax.ShapeDtypeStruct((rows, model), BF16),
            in_specs=[any_spec] * 3,
            out_specs=any_spec,
            scratch_shapes=[
                pltpu.VMEM((qn, span), BF16),
                pltpu.VMEM((qn, span), BF16),
                pltpu.VMEM((bufs, span, nc), BF16),
                pltpu.VMEM((pieces, qn, nc), F32),
                pltpu.VMEM((2, qn, nc), BF16),
                dma((2,)),
                dma((2,)),
                dma((bufs,)),
                dma((2,)),
                dma((2,)),
                dma((2,)),
                dma((pieces,)),
                dma((pieces,)),
            ],
            compiler_params=pltpu.CompilerParams(collective_id=1, has_side_effects=True, vmem_limit_bytes=60 << 20),
        )(o_a, o_b, w_o.reshape(num_heads * v_dim, model))
        chunks = 8
        attn_out, cache_kv, pe_t = pl.pallas_call(
            result_kernel,
            out_shape=(
                jax.ShapeDtypeStruct((rows, model), BF16),
                jax.ShapeDtypeStruct((rows, kv_rank), BF16),
                jax.ShapeDtypeStruct((rot, rows), BF16),
            ),
            in_specs=[any_spec] * 2,
            out_specs=(any_spec,) * 3,
            scratch_shapes=[
                pltpu.VMEM((chunks, rows, model // chunks), BF16),
                pltpu.VMEM((rows, kv_w), BF16),
                pltpu.VMEM((rot, rows), BF16),
                dma((chunks + 1,)),
                dma((chunks + 2,)),
            ],
            compiler_params=pltpu.CompilerParams(vmem_limit_bytes=62 << 20),
        )(res, kv_all)
        return attn_out, cache_kv, pe_t.T

    return jax.shard_map(local_step, mesh=mesh,
                         in_specs=(rows_spec, tok_spec) + (replicated,) * 8,
                         out_specs=(rows_spec, rows_spec, rows_spec), check_vma=False)
```
